128 devices in a mesh: dy: 16 (over z, y), dx: 8 (over x, core).
Axes of the slice: x: 4, y: 4, z: 4, core: 2. Of those that a mesh axis runs over, the one named last changes fastest.
Arguments:
- tokens: bfloat16 [32768, 1024], P(('dy', 'dx'))
- targets: bfloat16 [32768, 1024], P(('dy', 'dx'))
- w_in: bfloat16 [4, 1024, 4096], replicated
- w_out: bfloat16 [4, 4096, 1024], replicated
Outputs:
- output 1: float32 [4, 1024, 4096], replicated
- output 2: float32 [4, 4096, 1024], replicated
All inputs are finite; a program needn't handle non-finite values.
Results may differ from the reference program's by a relative error of at most 0.00957852.
Values are sent between devices in bfloat16 or wider.
A program may use at most 1 GiB of HBM per device.

```python
import jax
import jax.numpy as jnp
from jax import lax

D = 1024
FF = 4096
TOK = 256
LAYERS = 4
SHARDS = 128


def setup_inputs(seed: int = 0) -> dict:
    total_tok = SHARDS * TOK
    rng_keys = jax.random.split(jax.random.key(seed), 4)
    targ_scale = 0.5 * total_tok ** 0.5
    tokens = jax.random.normal(rng_keys[0], (total_tok, D), jnp.float32)
    targets = jax.random.normal(rng_keys[1], (total_tok, D), jnp.float32) * targ_scale
    w_in = jax.random.normal(rng_keys[2], (LAYERS, D, FF), jnp.float32) * D ** -0.5
    w_out = jax.random.normal(rng_keys[3], (LAYERS, FF, D), jnp.float32) * FF ** -0.5
    return {'tokens': tokens.astype(jnp.bfloat16), 'targets': targets.astype(jnp.bfloat16), 'w_in': w_in.astype(jnp.bfloat16), 'w_out': w_out.astype(jnp.bfloat16)}


def shard_grads(tok_shard, tgt_shard, w_in, w_out):
    inv_total = 1.0 / (SHARDS * TOK)

    def forward_layer(hidden, layer_weights):
        w_first, w_second = layer_weights
        pre_act = jnp.dot(hidden, w_first, preferred_element_type=jnp.float32).astype(jnp.bfloat16)
        post_act = jax.nn.gelu(pre_act.astype(jnp.float32)).astype(jnp.bfloat16)
        branch = jnp.dot(post_act, w_second, preferred_element_type=jnp.float32)
        hidden_next = (hidden.astype(jnp.float32) + branch).astype(jnp.bfloat16)
        return hidden_next, (hidden, pre_act, post_act)

    final, saved = lax.scan(forward_layer, tok_shard, (w_in, w_out))
    grad_top = ((final.astype(jnp.float32) - tgt_shard.astype(jnp.float32)) * inv_total).astype(jnp.bfloat16)

    def backward_layer(grad_hid, layer_data):
        hidden, pre_act, post_act, w_first, w_second = layer_data
        grad_w_out = jnp.dot(post_act.T, grad_hid, preferred_element_type=jnp.float32)
        grad_post = jnp.dot(grad_hid, w_second.T, preferred_element_type=jnp.float32)
        gelu_vjp = jax.vjp(jax.nn.gelu, pre_act.astype(jnp.float32))[1]
        grad_pre = gelu_vjp(grad_post)[0].astype(jnp.bfloat16)
        grad_w_in = jnp.dot(hidden.T, grad_pre, preferred_element_type=jnp.float32)
        through_w = jnp.dot(grad_pre, w_first.T, preferred_element_type=jnp.float32)
        grad_below = (grad_hid.astype(jnp.float32) + through_w).astype(jnp.bfloat16)
        return grad_below, (grad_w_in, grad_w_out)

    hiddens, pre_acts, post_acts = saved
    layer_grads = lax.scan(backward_layer, grad_top, (hiddens, pre_acts, post_acts, w_in, w_out), reverse=True)[1]
    return layer_grads


def reference(tokens, targets, w_in, w_out):
    tok_shards = tokens.reshape(SHARDS, TOK, D)
    tgt_shards = targets.reshape(SHARDS, TOK, D)

    def accumulate(running, shard_pair):
        grad_w_in, grad_w_out = shard_grads(shard_pair[0], shard_pair[1], w_in, w_out)
        return (running[0] + grad_w_in, running[1] + grad_w_out), None

    zero_acc = (jnp.zeros((LAYERS, D, FF), jnp.float32), jnp.zeros((LAYERS, FF, D), jnp.float32))
    totals = lax.scan(accumulate, zero_acc, (tok_shards, tgt_shards))[0]
    return totals[0], totals[1]
```

```python
import jax
import jax.numpy as jnp
from jax import lax
from jax.sharding import Mesh
from jax.sharding import PartitionSpec as P

ROW = (((0,), (0,)), ((), ()))
COL = (((1,), (1,)), ((), ()))
AXES = ('z', 'y', 'x', 'c')
RING = {'x': ('z', 'y'), 'y': ('z', 'x'), 'z': ('y', 'x')}
GROUP_AXIS = ('x', 'x', 'x', 'x')
F32, BF16 = jnp.float32, jnp.bfloat16


def shift(value, axis, step):
    return lax.ppermute(value, axis, [(i, (i + step) % 4) for i in range(4)])


def swap_core(value):
    return lax.ppermute(value, 'c', [(0, 1), (1, 0)])


def gather_group(block, axis):
    half = block.shape[0] // 2
    from_left = shift(block, axis, 1)
    from_right = shift(block, axis, -1)
    opp_a = shift(from_left[:half], axis, 1)
    opp_b = shift(from_right[half:], axis, -1)
    mine = jnp.concatenate([block, from_left, from_right, opp_a, opp_b], axis=0)
    return jnp.concatenate([mine, swap_core(mine)], axis=0)


def gelu_pair(pre_act):
    return jax.vjp(jax.nn.gelu, pre_act.astype(F32))


def solution(mesh):
    mesh4 = Mesh(mesh.devices.reshape(4, 4, 4, 2), AXES)

    def local_step(tok, tgt, w_in, w_out):
        layers = w_in.shape[0]
        inv_total = 1.0 / (tok.shape[0] * mesh4.size)
        hidden = tok
        hiddens, pres, gathered_h, gathered_g = [], [], [], [None] * layers
        for l in range(layers):
            hiddens.append(hidden)
            pre = jnp.dot(hidden, w_in[l], preferred_element_type=F32).astype(BF16)
            pres.append(pre)
            post = jax.nn.gelu(pre.astype(F32)).astype(BF16)
            hidden = (hidden.astype(F32) + jnp.dot(post, w_out[l], preferred_element_type=F32)).astype(BF16)
        grad = ((hidden.astype(F32) - tgt.astype(F32)) * inv_total).astype(BF16)
        outs_in, outs_out = [None] * layers, [None] * layers
        for l in reversed(range(layers)):
            axis = GROUP_AXIS[l]
            other = RING[axis]
            width = w_in.shape[2] // 8
            start = (lax.axis_index(axis) * 2 + lax.axis_index('c')) * width
            hg = gather_group(hiddens[l], axis)
            gg = gather_group(grad, axis)
            wi = lax.dynamic_slice(w_in[l], (0, start), (w_in.shape[1], width))
            wo = lax.dynamic_slice(w_out[l], (start, 0), (width, w_out.shape[2]))
            pre = jnp.dot(hg, wi, preferred_element_type=F32).astype(BF16)
            post, vjp = gelu_pair(pre)
            e = lax.dot_general(gg, wo, COL, preferred_element_type=F32)
            p = vjp(e)[0].astype(BF16)
            d_in = lax.dot_general(p, hg, ROW, preferred_element_type=F32)
            d_out = lax.dot_general(post.astype(BF16), gg, ROW, preferred_element_type=F32)
            both = jnp.stack([d_in.reshape(16, width // 16, -1), d_out.reshape(16, width // 16, -1)], axis=1)
            part = lax.psum_scatter(both, other, scatter_dimension=0, tiled=True)
            full = lax.all_gather(part, AXES, axis=0, tiled=True)
            n = {'x': (2, 3, 0, 1), 'y': (1, 3, 0, 2), 'z': (0, 3, 1, 2)}[axis]
            blocks = full.reshape(4, 4, 4, 2, 2, width // 16, -1)
            fin = jnp.transpose(blocks[:, :, :, :, 0], n + (4, 5)).reshape(width * 8, -1)
            fout = jnp.transpose(blocks[:, :, :, :, 1], n + (4, 5)).reshape(width * 8, -1)
            outs_in[l] = fin.T
            outs_out[l] = fout
            if l > 0:
                e = lax.dot_general(grad, w_out[l], COL, preferred_element_type=F32)
                p = gelu_pair(pres[l])[1](e)[0].astype(BF16)
                through = lax.dot_general(p, w_in[l], COL, preferred_element_type=F32)
                grad = (grad.astype(F32) + through).astype(BF16)
        return jnp.stack(outs_in), jnp.stack(outs_out)

    spec = P(AXES, None)
    return jax.shard_map(local_step, mesh=mesh4, in_specs=(spec, spec, P(), P()), out_specs=(P(), P()), check_vma=False)
```

```python
import functools

import jax
import jax.numpy as jnp
from jax import lax
from jax.experimental import pallas as pl
from jax.experimental.pallas import tpu as pltpu
from jax.sharding import Mesh
from jax.sharding import PartitionSpec as P

AXES = ('z', 'y', 'x', 'c')
RING = 4
GROUP = 'x'
FIRST, SECOND = 'z', 'y'
F32, BF16 = jnp.float32, jnp.bfloat16
COL = (((1,), (1,)), ((), ()))
ROW = (((0,), (0,)), ((), ()))
GELU_S = 0.7978845608028654
GELU_C = 0.044715
MESH_ID = pl.DeviceIdType.MESH
MIB = 1 << 20


def place(axis, step):
    coords = [lax.axis_index(name) for name in AXES]
    which = AXES.index(axis)
    size = 2 if axis == 'c' else RING
    coords[which] = lax.rem(coords[which] + (step + size), size)
    return tuple(coords)


def remote(src, dst, sems, index, to):
    return pltpu.make_async_remote_copy(src_ref=src, dst_ref=dst, send_sem=sems[0].at[index], recv_sem=sems[1].at[index], device_id=to, device_id_type=MESH_ID)


def meet(neighbours):
    barrier = pltpu.get_barrier_semaphore()
    for axis, step in neighbours:
        pl.semaphore_signal(barrier, inc=1, device_id=place(axis, step), device_id_type=MESH_ID)
    pl.semaphore_wait(barrier, len(neighbours))


def gather_parts(src, out, sems, axis):
    right, left, other = place(axis, 1), place(axis, -1), place('c', 1)
    half = src.shape[0] // 2
    top, bottom = pl.ds(0, half), pl.ds(half, half)
    own = [remote(src, out.at[1], sems, 0, right), remote(src, out.at[2], sems, 1, left), remote(src, out.at[4], sems, 2, other)]
    onward = [
        remote(out.at[1, top], out.at[3, top], sems, 3, right),
        remote(out.at[2, bottom], out.at[3, bottom], sems, 4, left),
        remote(out.at[1], out.at[5], sems, 5, other),
        remote(out.at[2], out.at[6], sems, 6, other),
        remote(out.at[3], out.at[7], sems, 7, other),
    ]

    def begin():
        for copy in own:
            copy.start()
        out[0] = src[...]

    def middle():
        own[0].wait_recv()
        onward[0].start()
        onward[2].start()
        own[1].wait_recv()
        onward[1].start()
        onward[3].start()

    def late():
        onward[0].wait_recv()
        onward[1].wait_recv()
        onward[4].start()

    def finish():
        own[2].wait_recv()
        for copy in onward[2:]:
            copy.wait_recv()
        for copy in own + onward:
            copy.wait_send()

    return begin, middle, late, finish


def ring_sum_parts(parts, got, put, sems, axis):
    me = lax.axis_index(axis)
    right, left = place(axis, 1), place(axis, -1)
    nxt, prv, opp = lax.rem(me + 1, RING), lax.rem(me + 3, RING), lax.rem(me + 2, RING)
    half = parts.shape[1] // 2
    top, bottom = pl.ds(0, half), pl.ds(half, half)
    first = [
        remote(parts.at[opp, top], got.at[0], sems, 0, right),
        remote(parts.at[opp, bottom], got.at[3], sems, 3, left),
        remote(parts.at[nxt, bottom], got.at[1], sems, 1, right),
        remote(parts.at[prv, top], got.at[4], sems, 4, left),
    ]
    second = [remote(got.at[0], got.at[2], sems, 2, right), remote(got.at[3], got.at[5], sems, 5, left)]

    def begin():
        for copy in first:
            copy.start()

    def middle():
        first[0].wait_recv()
        got[0] = got[0] + parts[nxt, top]
        second[0].start()
        first[1].wait_recv()
        got[3] = got[3] + parts[prv, bottom]
        second[1].start()

    def finish():
        first[3].wait_recv()
        second[0].wait_recv()
        put(0, parts[me, top] + got[4] + got[2])
        first[2].wait_recv()
        second[1].wait_recv()
        put(1, parts[me, bottom] + got[1] + got[5])

    def drain():
        for copy in first + second:
            copy.wait_send()

    return begin, middle, finish, drain


def put_blocks(total, which, value):
    total[pl.ds(which * 2, 2)] = value.reshape((2,) + total.shape[1:])


def put_rows(total, which, value):
    total[pl.ds(which * value.shape[0], value.shape[0])] = value


def exchange_kernel(reduce, gathers, *refs):
    refs = list(refs)
    take = lambda count: [refs.pop(0) for _ in range(count)]
    sums_in = take(2) if reduce else []
    rows_in = take(gathers)
    sums_out = take(2) if reduce else []
    rows_out = take(gathers)
    gather_sems = [take(2) for _ in range(gathers)]
    meet([(GROUP, 1), (GROUP, -1), ('c', 1)] + ([(FIRST, 1), (FIRST, -1), (SECOND, 1), (SECOND, -1)] if reduce else []))
    moves = [gather_parts(src, out, sems, GROUP) for src, out, sems in zip(rows_in, rows_out, gather_sems)]
    for begin, _, _, _ in moves:
        begin()
    if reduce:
        stage_one, stage_two = [], []
        for color, (one, two) in enumerate(((FIRST, SECOND), (SECOND, FIRST))):
            got_one, mid, got_two, send_one, recv_one, send_two, recv_two = take(7)
            stage_one.append(ring_sum_parts(sums_in[color], got_one, functools.partial(put_blocks, mid), (send_one, recv_one), one))
            stage_two.append(ring_sum_parts(mid, got_two, functools.partial(put_rows, sums_out[color]), (send_two, recv_two), two))
        for begin, _, _, _ in stage_one:
            begin()
        for _, middle, _, _ in stage_one:
            middle()
        for (_, _, finish, _), (begin, _, _, _) in zip(stage_one, stage_two):
            finish()
            begin()
        for _, middle, _, _ in stage_two:
            middle()
        for _, _, finish, _ in stage_two:
            finish()
    for _, middle, _, _ in moves:
        middle()
    for _, _, late, _ in moves:
        late()
    for _, _, _, finish in moves:
        finish()
    if reduce:
        for _, _, _, drain in stage_one + stage_two:
            drain()


def exchange(sums, rows, collective_id):
    vmem = pl.BlockSpec(memory_space=pltpu.VMEM)
    out_shape, scratch = [], []
    for part in sums:
        out_shape.append(jax.ShapeDtypeStruct((part.shape[1] // RING, part.shape[2]), F32))
    for row in rows:
        out_shape.append(jax.ShapeDtypeStruct((2 * RING,) + row.shape, row.dtype))
        scratch += [pltpu.SemaphoreType.DMA((8,))] * 2
    for part in sums:
        _, n, w = part.shape
        scratch += [pltpu.VMEM((6, n // 2, w), F32), pltpu.VMEM((RING, n // RING, w), F32), pltpu.VMEM((6, n // 8, w), F32)]
        scratch += [pltpu.SemaphoreType.DMA((6,))] * 4
    return pl.pallas_call(
        functools.partial(exchange_kernel, bool(sums), len(rows)),
        out_shape=out_shape,
        in_specs=[vmem] * (len(sums) + len(rows)),
        out_specs=[vmem] * len(out_shape),
        scratch_shapes=scratch,
        compiler_params=pltpu.CompilerParams(collective_id=collective_id, has_side_effects=True, vmem_limit_bytes=48 * MIB),
        cost_estimate=pl.CostEstimate(flops=30_000_000_000, bytes_accessed=16 * MIB, transcendentals=0),
        name='exchange',
    )(*sums, *rows)


def gelu_terms(x):
    square = x * x
    t = jnp.tanh(x * (GELU_S + GELU_S * GELU_C * square))
    cdf = 0.5 + 0.5 * t
    slope = cdf + (0.5 * x) * (1.0 - t * t) * (GELU_S + 3.0 * GELU_S * GELU_C * square)
    return x * cdf, slope


def shard_grad_kernel(_, h_ref, g_ref, wi_ref, wo_ref, din_ref, dout_ref, post, pre_grad):
    rows = h_ref.shape[0]
    chunk = min(256, rows)

    @pl.loop(0, rows // chunk)
    def _(i):
        at = pl.ds(i * chunk, chunk)
        u = jnp.dot(h_ref[at], wi_ref[...], preferred_element_type=F32).astype(BF16)
        e = lax.dot_general(g_ref[at], wo_ref[...], COL, preferred_element_type=F32)
        act, slope = gelu_terms(u.astype(F32))
        post[at] = act.astype(BF16)
        pre_grad[at] = (e * slope).astype(BF16)

    din_ref[...] = lax.dot_general(pre_grad[...], h_ref[...], ROW, preferred_element_type=F32)
    dout_ref[...] = lax.dot_general(post[...], g_ref[...], ROW, preferred_element_type=F32)


def shard_grads(shard, rows_h, rows_g, w_in, w_out, layer):
    n, d = rows_h.shape
    width = w_in.shape[2] // (2 * RING)
    block = width // 2
    whole = pl.BlockSpec((n, d), lambda i, s: (0, 0))
    return pl.pallas_call(
        shard_grad_kernel,
        grid_spec=pltpu.PrefetchScalarGridSpec(
            num_scalar_prefetch=1,
            grid=(2,),
            in_specs=[
                whole,
                whole,
                pl.BlockSpec((None, d, block), lambda i, s: (layer, 0, s[0] * 2 + i)),
                pl.BlockSpec((None, block, d), lambda i, s: (layer, s[0] * 2 + i, 0)),
            ],
            out_specs=[pl.BlockSpec((block, d), lambda i, s: (i, 0))] * 2,
            scratch_shapes=[pltpu.VMEM((n, block), BF16)] * 2,
        ),
        out_shape=[jax.ShapeDtypeStruct((width, d), F32)] * 2,
        compiler_params=pltpu.CompilerParams(vmem_limit_bytes=48 * MIB),
        cost_estimate=pl.CostEstimate(flops=8 * n * d * width, bytes_accessed=16 * MIB, transcendentals=n * width),
        name='shard_grads',
    )(shard, rows_h, rows_g, w_in, w_out)


def place_kernel(weights, _, *refs):
    srcs, outs = refs[: len(weights)], refs[len(refs) - len(weights) :]
    for weight, src, out in zip(weights, srcs, outs):
        ring = src.shape[0]
        if weight == 0:
            out[...] = src[...].reshape(ring * src.shape[-2], src.shape[-1]).T
        else:
            size = src.shape[-2]
            for i in range(RING):
                for j in range(RING):
                    out[pl.ds((j * RING + i) * size, size)] = src[i * RING + j].reshape(size, src.shape[-1])


def place_blocks(core, blocks, weights, outs, layer, layers):
    _, _, size, d = blocks.shape
    width = RING * RING * size
    view = blocks.reshape(RING * RING, RING, len(weights), size, d)
    full = width * 2 * RING
    shapes = [jax.ShapeDtypeStruct((layers, d, full) if w == 0 else (layers, full, d), F32) for w in weights]
    src_specs = [pl.BlockSpec((RING * RING, None, None, size, d), functools.partial(lambda k, i, s: (0, i, k, 0, 0), k)) for k in range(len(weights))]
    out_specs = [
        pl.BlockSpec((None, d, width), lambda i, s: (layer, 0, i * 2 + s[0])) if w == 0 else pl.BlockSpec((None, width, d), lambda i, s: (layer, i * 2 + s[0], 0))
        for w in weights
    ]
    aliased = [o for o in outs if o is not None]
    return pl.pallas_call(
        functools.partial(place_kernel, weights),
        grid_spec=pltpu.PrefetchScalarGridSpec(
            num_scalar_prefetch=1,
            grid=(RING,),
            in_specs=src_specs + [pl.BlockSpec(memory_space=pl.ANY)] * len(aliased),
            out_specs=out_specs,
        ),
        out_shape=shapes,
        input_output_aliases={1 + len(weights) + k: k for k in range(len(aliased))},
        compiler_params=pltpu.CompilerParams(vmem_limit_bytes=63 * MIB),
        cost_estimate=pl.CostEstimate(flops=4_000_000_000, bytes_accessed=32 * MIB, transcendentals=0),
        name='place_blocks',
    )(core, *([view] * len(weights)), *aliased)


def solution(mesh):
    mesh4 = Mesh(mesh.devices.reshape(RING, RING, RING, 2), AXES)

    def local_step(tok, tgt, w_in, w_out):
        layers = w_in.shape[0]
        inv_total = 1.0 / (tok.shape[0] * mesh4.size)
        core = lax.axis_index('c')
        shard = (lax.axis_index(GROUP) * 2 + core).astype(jnp.int32).reshape(1)
        mine = core.astype(jnp.int32).reshape(1)
        hidden = tok
        hiddens, pres = [], []
        for l in range(layers):
            hiddens.append(hidden)
            pre = jnp.dot(hidden, w_in[l], preferred_element_type=F32).astype(BF16)
            pres.append(pre)
            post = jax.nn.gelu(pre.astype(F32)).astype(BF16)
            hidden = (hidden.astype(F32) + jnp.dot(post, w_out[l], preferred_element_type=F32)).astype(BF16)
        grad = ((hidden.astype(F32) - tgt.astype(F32)) * inv_total).astype(BF16)

        rows = exchange([], [hiddens[layers - 1], grad], layers)
        pieces = []
        for l in reversed(range(layers)):
            if l > 0:
                e = lax.dot_general(grad, w_out[l], COL, preferred_element_type=F32)
                p = jax.vjp(jax.nn.gelu, pres[l].astype(F32))[1](e)[0].astype(BF16)
                through = lax.dot_general(p, w_in[l], COL, preferred_element_type=F32)
                grad = (grad.astype(F32) + through).astype(BF16)
            flat = [r.reshape(-1, r.shape[-1]) for r in rows]
            sums = shard_grads(shard, flat[0], flat[1], w_in, w_out, l)
            sums = [s.reshape(RING, -1, s.shape[-1]) for s in sums]
            d_in, d_out, *rows = exchange(sums, [hiddens[l - 1], grad] if l > 0 else [], l)
            groups = [((0, 1), jnp.stack([d_in, d_out]))] if l > 0 else [((0,), d_in[None]), ((1,), d_out[None])]
            for weights, part in groups:
                own = lax.all_gather(part[None], ('z', 'y', 'x'), axis=0, tiled=True)
                pieces.append((l, weights, own))
        outs = [None, None]
        for l, weights, own in pieces:
            if outs[0] is not None:
                own, *outs = lax.optimization_barrier((own, *outs))
            away = lax.ppermute(own, 'c', [(0, 1), (1, 0)])
            for which, blocks in ((mine, own), (1 - mine, away)):
                new = place_blocks(which, blocks, weights, [outs[w] for w in weights], l, layers)
                for w, value in zip(weights, new):
                    outs[w] = value
        return outs[0], outs[1]

    spec = P(AXES, None)
    return jax.shard_map(local_step, mesh=mesh4, in_specs=(spec, spec, P(), P()), out_specs=(P(), P()), check_vma=False)
```

```python
import functools

import jax
import jax.numpy as jnp
from jax import lax
from jax.experimental import pallas as pl
from jax.experimental.pallas import tpu as pltpu
from jax.sharding import Mesh
from jax.sharding import PartitionSpec as P

AXES = ('z', 'y', 'x', 'c')
RING = 4
GROUP = 'x'
FIRST, SECOND = 'z', 'y'
ORDERS = (('x', 'y', 'z'), ('y', 'z', 'x'), ('z', 'x', 'y'))
KERNEL_GATHER_LAYERS = (0,)
F32, BF16 = jnp.float32, jnp.bfloat16
COL = (((1,), (1,)), ((), ()))
GELU_S = 0.7978845608028654
GELU_C = 0.044715
MESH_ID = pl.DeviceIdType.MESH
MIB = 1 << 20


def place(axis, step):
    coords = [lax.axis_index(name) for name in AXES]
    which = AXES.index(axis)
    size = 2 if axis == 'c' else RING
    coords[which] = lax.rem(coords[which] + (step + size), size)
    return tuple(coords)


def remote(src, dst, sems, index, to):
    return pltpu.make_async_remote_copy(src_ref=src, dst_ref=dst, send_sem=sems[0].at[index], recv_sem=sems[1].at[index], device_id=to, device_id_type=MESH_ID)


def meet(axes):
    barrier = pltpu.get_barrier_semaphore()
    neighbours = [(axis, step) for axis in axes for step in (1, -1)] + [('c', 1)]
    for axis, step in neighbours:
        pl.semaphore_signal(barrier, inc=1, device_id=place(axis, step), device_id_type=MESH_ID)
    pl.semaphore_wait(barrier, len(neighbours))


class RowGather:
    def __init__(self, src, out, sems, axis):
        right, left, other = place(axis, 1), place(axis, -1), place('c', 1)
        half = src.shape[0] // 2
        top, bottom = pl.ds(0, half), pl.ds(half, half)
        self.src, self.out = src, out
        self.own = [remote(src, out.at[1], sems, 0, right), remote(src, out.at[2], sems, 1, left), remote(src, out.at[4], sems, 2, other)]
        self.onward = [
            remote(out.at[1, top], out.at[3, top], sems, 3, right),
            remote(out.at[2, bottom], out.at[3, bottom], sems, 4, left),
            remote(out.at[1], out.at[5], sems, 5, other),
            remote(out.at[2], out.at[6], sems, 6, other),
            remote(out.at[3], out.at[7], sems, 7, other),
        ]

    def begin(self):
        for copy in self.own:
            copy.start()
        self.out[0] = self.src[...]

    def middle(self):
        for side in range(2):
            self.own[side].wait_recv()
            self.onward[side].start()
            self.onward[2 + side].start()

    def late(self):
        self.onward[0].wait_recv()
        self.onward[1].wait_recv()
        self.onward[4].start()

    def finish(self):
        self.own[2].wait_recv()
        for copy in self.onward[2:]:
            copy.wait_recv()
        for copy in self.own + self.onward:
            copy.wait_send()


class RingSum:
    def __init__(self, parts, got, put, sems, axis):
        self.parts, self.got, self.put = parts, got, put
        self.me = lax.axis_index(axis)
        right, left = place(axis, 1), place(axis, -1)
        self.nxt, self.prv, self.opp = lax.rem(self.me + 1, RING), lax.rem(self.me + 3, RING), lax.rem(self.me + 2, RING)
        half = parts.shape[1] // 2
        self.top, self.bottom = pl.ds(0, half), pl.ds(half, half)
        self.first = [
            remote(parts.at[self.opp, self.top], got.at[0], sems, 0, right),
            remote(parts.at[self.opp, self.bottom], got.at[3], sems, 3, left),
            remote(parts.at[self.nxt, self.bottom], got.at[1], sems, 1, right),
            remote(parts.at[self.prv, self.top], got.at[4], sems, 4, left),
        ]
        self.second = [remote(got.at[0], got.at[2], sems, 2, right), remote(got.at[3], got.at[5], sems, 5, left)]

    def begin_far(self):
        self.first[0].start()
        self.first[1].start()

    def begin_near(self):
        self.first[2].start()
        self.first[3].start()

    def middle(self):
        self.first[0].wait_recv()
        self.got[0] = self.got[0] + self.parts[self.nxt, self.top]
        self.second[0].start()
        self.first[1].wait_recv()
        self.got[3] = self.got[3] + self.parts[self.prv, self.bottom]
        self.second[1].start()

    def finish(self):
        self.first[3].wait_recv()
        self.second[0].wait_recv()
        self.put(0, self.parts[self.me, self.top] + self.got[4] + self.got[2])
        self.first[2].wait_recv()
        self.second[1].wait_recv()
        self.put(1, self.parts[self.me, self.bottom] + self.got[1] + self.got[5])

    def drain(self):
        for copy in self.first + self.second:
            copy.wait_send()


def put_blocks(total, which, value):
    total[pl.ds(which * 2, 2)] = value.reshape((2,) + total.shape[1:])


def put_rows(total, offset, which, value):
    total[pl.ds(offset + which * value.shape[0], value.shape[0])] = value


def gelu_terms(x):
    square = x * x
    t = jnp.tanh(x * (GELU_S + GELU_S * GELU_C * square))
    cdf = 0.5 + 0.5 * t
    slope = cdf + (0.5 * x) * (1.0 - t * t) * (GELU_S + 3.0 * GELU_S * GELU_C * square)
    return x * cdf, slope


def gather_kernel(count, *refs):
    srcs, outs, sems = refs[:count], refs[count : 2 * count], refs[2 * count :]
    meet((GROUP,))
    moves = [RowGather(srcs[i], outs[i], sems[2 * i : 2 * i + 2], GROUP) for i in range(count)]
    for stage in ('begin', 'middle', 'late', 'finish'):
        for move in moves:
            getattr(move, stage)()


def gather_rows(rows, collective_id):
    vmem = pl.BlockSpec(memory_space=pltpu.VMEM)
    return pl.pallas_call(
        functools.partial(gather_kernel, len(rows)),
        out_shape=[jax.ShapeDtypeStruct((2 * RING,) + row.shape, row.dtype) for row in rows],
        in_specs=[vmem] * len(rows),
        out_specs=[vmem] * len(rows),
        scratch_shapes=[pltpu.SemaphoreType.DMA((8,))] * (2 * len(rows)),
        compiler_params=pltpu.CompilerParams(collective_id=collective_id, has_side_effects=True, vmem_limit_bytes=24 * MIB),
        cost_estimate=pl.CostEstimate(flops=20_000_000_000, bytes_accessed=16 * MIB, transcendentals=0),
        name='gather_rows',
    )(*rows)


def layer_kernel(layer, gathers, hg, gg, w_in, w_out, *refs):
    refs = list(refs)
    take = lambda count: [refs.pop(0) for _ in range(count)]
    rows_in = take(gathers)
    (shard,) = take(1)
    rows_out = take(gathers)
    wi, wo, wi_t, act, slope_grad, w_sems = take(6)
    stage_one, stage_two = [], []
    for color, (one, two) in enumerate(((FIRST, SECOND), (SECOND, FIRST))):
        parts, got_one, mid, got_two, send_one, recv_one, send_two, recv_two = take(8)
        stage_one.append(RingSum(parts, got_one, functools.partial(put_blocks, mid), (send_one, recv_one), one))
        stage_two.append(RingSum(mid, got_two, functools.partial(put_rows, shard, color * mid.shape[1]), (send_two, recv_two), two))
    moves = [RowGather(src, out, take(2), GROUP) for src, out in zip(rows_in, rows_out)]

    width = wi.shape[1]
    start = (lax.axis_index(GROUP) * 2 + lax.axis_index('c')) * width
    start = pl.multiple_of(start, width)
    loads = [
        pltpu.make_async_copy(w_in.at[layer, :, pl.ds(start, width)], wi, w_sems.at[0]),
        pltpu.make_async_copy(w_out.at[layer, pl.ds(start, width), :], wo, w_sems.at[1]),
    ]
    for load in loads:
        load.start()
    meet((GROUP, FIRST, SECOND))
    for move in moves:
        move.begin()
    loads[0].wait()
    wi_t[...] = wi[...].T
    loads[1].wait()

    tokens = hg.shape[0]
    chunk = min(256, tokens)

    @pl.loop(0, tokens // chunk)
    def _(i):
        at = pl.ds(pl.multiple_of(i * chunk, chunk), chunk)
        u = lax.dot_general(wi_t[...], hg[at], COL, preferred_element_type=F32).astype(BF16)
        e = lax.dot_general(wo[...], gg[at], COL, preferred_element_type=F32)
        post, slope = gelu_terms(u.astype(F32))
        act[:, at] = post.astype(BF16)
        slope_grad[:, at] = (e * slope).astype(BF16)

    cols = stage_one[0].parts.shape[2]

    def fill(color, which):
        at = pl.ds(pl.multiple_of(which * cols, cols), cols)
        left, right = (slope_grad, hg) if color == 0 else (act, gg)
        stage_one[color].parts[which] = jnp.dot(left[...], right[:, at], preferred_element_type=F32)

    for color in range(2):
        fill(color, stage_one[color].opp)
        stage_one[color].begin_far()
    for color in range(2):
        fill(color, stage_one[color].nxt)
        fill(color, stage_one[color].prv)
        stage_one[color].begin_near()
    for color in range(2):
        fill(color, stage_one[color].me)
    if moves:
        moves[0].middle()
    for stage in stage_one:
        stage.middle()
    if moves:
        moves[1].middle()
    for one, two in zip(stage_one, stage_two):
        one.finish()
        two.begin_far()
        two.begin_near()
    if moves:
        moves[0].late()
    for stage in stage_two:
        stage.middle()
    for stage in stage_two:
        stage.finish()
    if moves:
        moves[1].late()
    for move in moves:
        move.finish()
    for stage in stage_one + stage_two:
        stage.drain()


def layer_grads(layer, hg, gg, w_in, w_out, rows):
    vmem, anywhere = pl.BlockSpec(memory_space=pltpu.VMEM), pl.BlockSpec(memory_space=pl.ANY)
    tokens, d = hg.shape
    width = w_in.shape[2] // (2 * RING)
    cols, n = d // RING, width // RING
    out_shape = [jax.ShapeDtypeStruct((2 * n, cols), F32)]
    out_shape += [jax.ShapeDtypeStruct((2 * RING,) + row.shape, row.dtype) for row in rows]
    scratch = [pltpu.VMEM((d, width), BF16), pltpu.VMEM((width, d), BF16), pltpu.VMEM((width, d), BF16)]
    scratch += [pltpu.VMEM((width, tokens), BF16)] * 2 + [pltpu.SemaphoreType.DMA((2,))]
    for _ in range(2):
        scratch += [pltpu.VMEM((RING, width, cols), F32), pltpu.VMEM((6, width // 2, cols), F32)]
        scratch += [pltpu.VMEM((RING, n, cols), F32), pltpu.VMEM((6, n // 2, cols), F32)]
        scratch += [pltpu.SemaphoreType.DMA((6,))] * 4
    scratch += [pltpu.SemaphoreType.DMA((8,))] * (2 * len(rows))
    return pl.pallas_call(
        functools.partial(layer_kernel, layer, len(rows)),
        out_shape=out_shape,
        in_specs=[vmem, vmem, anywhere, anywhere] + [vmem] * len(rows),
        out_specs=[vmem] * len(out_shape),
        scratch_shapes=scratch,
        compiler_params=pltpu.CompilerParams(collective_id=layer, has_side_effects=True, vmem_limit_bytes=48 * MIB),
        cost_estimate=pl.CostEstimate(flops=30_000_000_000, bytes_accessed=16 * MIB, transcendentals=0),
        name='layer_grads',
    )(hg, gg, w_in, w_out, *rows)


class BlockGather:
    def __init__(self, near, far, out_near, out_far, order, rows, sems, local_sems, base):
        self.near, self.far, self.outs = near, far, (out_near, out_far)
        self.order, self.rows, self.sems, self.local_sems = order, rows, sems, local_sems
        self.index = {axis: lax.axis_index(axis) for axis in 'xyz'}
        self.base, self.count, self.local_count = base, 0, 0
        self.other = place('c', 1)
        self.copies, self.cross, self.local = {}, [], []

    def at(self, phase, which, half=None):
        picks, rows = {}, self.rows
        for k, axis in enumerate(self.order):
            picks[axis] = pl.ds(0, RING) if k < phase else self.index[axis]
        if phase < 3:
            picks[self.order[phase]] = which
        if half is not None:
            if phase == 0:
                cut = (rows[1] // 16) * 8
                rows = (rows[0], cut) if half == 0 else (rows[0] + cut, rows[1] - cut)
            else:
                picks[self.order[phase - 1]] = pl.ds(half * 2, 2)
        return tuple(picks[axis] for axis in ('z', 'y', 'x')) + (pl.ds(*rows),)

    def send(self, where, to, dst=None):
        dst = self.near if dst is None else dst
        copy = remote(self.near.at[where], dst.at[where], self.sems, self.base + self.count, to)
        self.count += 1
        copy.start()
        return copy

    def cross_over(self, where):
        self.cross.append((self.send(where, self.other, self.far), where))
        self.keep(0, where)

    def keep(self, side, where):
        copy = pltpu.make_async_copy((self.near, self.far)[side].at[where], self.outs[side].at[where], self.local_sems.at[self.base + self.local_count])
        self.local_count += 1
        copy.start()
        self.local.append(copy)

    def begin(self, phase):
        axis = self.order[phase]
        me = self.index[axis]
        self.ends = (place(axis, 1), place(axis, -1))
        self.around = (lax.rem(me + 3, RING), lax.rem(me + 1, RING), lax.rem(me + 2, RING))
        whole = self.at(phase, me)
        self.near_copies = [self.send(whole, end) for end in self.ends]
        if phase == 2:
            self.cross_over(whole)

    def middle(self, phase):
        self.far_copies = []
        for side in range(2):
            self.near_copies[side].wait_recv()
            self.far_copies.append(self.send(self.at(phase, self.around[side], side), self.ends[side]))
            if phase == 2:
                self.cross_over(self.at(phase, self.around[side]))

    def finish(self, phase):
        for copy in self.far_copies:
            copy.wait_recv()
        for copy in self.near_copies + self.far_copies:
            self.copies[id(copy)] = copy
        if phase == 2:
            self.cross_over(self.at(phase, self.around[2]))

    def close(self):
        for copy, where in self.cross:
            copy.wait_recv()
            self.keep(1, where)
        for copy in list(self.copies.values()) + [c for c, _ in self.cross]:
            copy.wait_send()
        for copy in self.local:
            copy.wait()


BLOCK_SEMS = 16


def block_gather_kernel(shard, out_near, out_far, near, far, send, recv, local_sems):
    me = tuple(lax.axis_index(axis) for axis in ('z', 'y', 'x'))
    near[me] = shard[...]
    tiles = shard.shape[0] // 8
    cuts = [0, -(-tiles // 3), -(-2 * tiles // 3), tiles]
    meet(('x', 'y', 'z'))
    colors = [
        BlockGather(near, far, out_near, out_far, ORDERS[k], (8 * cuts[k], 8 * (cuts[k + 1] - cuts[k])), (send, recv), local_sems, k * BLOCK_SEMS) for k in range(3)
    ]
    for phase in range(3):
        for stage in ('begin', 'middle', 'finish'):
            for color in colors:
                getattr(color, stage)(phase)
    for color in colors:
        color.close()


def block_gather(shard, collective_id):
    vmem, anywhere = pl.BlockSpec(memory_space=pltpu.VMEM), pl.BlockSpec(memory_space=pl.ANY)
    shape = (RING, RING, RING) + shard.shape
    return pl.pallas_call(
        block_gather_kernel,
        out_shape=[jax.ShapeDtypeStruct(shape, F32)] * 2,
        in_specs=[vmem],
        out_specs=[anywhere] * 2,
        scratch_shapes=[pltpu.VMEM(shape, F32)] * 2 + [pltpu.SemaphoreType.DMA((3 * BLOCK_SEMS,))] * 3,
        compiler_params=pltpu.CompilerParams(collective_id=collective_id, has_side_effects=True, vmem_limit_bytes=48 * MIB),
        cost_estimate=pl.CostEstimate(flops=60_000_000_000, bytes_accessed=32 * MIB, transcendentals=0),
        name='block_gather',
    )(shard)


def place_kernel(_, src_in, src_out, *refs):
    out_in, out_out = refs[-2:]
    _, n, cols = src_in.shape
    for z in range(RING):
        for y in range(RING):
            out_in[z * cols : (z + 1) * cols, y * n : (y + 1) * n] = src_in[z * RING + y].T
            out_out[z * n : (z + 1) * n, y * cols : (y + 1) * cols] = src_out[z * RING + y]


def place_blocks(core, blocks, outs, layer, layers):
    n, cols = blocks.shape[-2] // 2, blocks.shape[-1]
    view = blocks.reshape(RING * RING, RING, 2 * n, cols)
    width, d = n * RING, cols * RING
    shapes = [jax.ShapeDtypeStruct((layers, d, width * 2 * RING), F32), jax.ShapeDtypeStruct((layers, width * 2 * RING, d), F32)]
    src_specs = [pl.BlockSpec((RING * RING, None, n, cols), functools.partial(lambda k, i, s: (0, i, k, 0), k)) for k in range(2)]
    return pl.pallas_call(
        place_kernel,
        grid_spec=pltpu.PrefetchScalarGridSpec(
            num_scalar_prefetch=1,
            grid=(RING,),
            in_specs=src_specs + [pl.BlockSpec(memory_space=pl.ANY)] * len(outs),
            out_specs=[
                pl.BlockSpec((None, d, width), lambda i, s: (layer, 0, i * 2 + s[0])),
                pl.BlockSpec((None, width, d), lambda i, s: (layer, i * 2 + s[0], 0)),
            ],
        ),
        out_shape=shapes,
        input_output_aliases={3 + k: k for k in range(len(outs))},
        compiler_params=pltpu.CompilerParams(vmem_limit_bytes=63 * MIB),
        cost_estimate=pl.CostEstimate(flops=10_000_000_000, bytes_accessed=32 * MIB, transcendentals=0),
        name='place_blocks',
    )(core, view, view, *outs)


def solution(mesh):
    mesh4 = Mesh(mesh.devices.reshape(RING, RING, RING, 2), AXES)

    def local_step(tok, tgt, w_in, w_out):
        layers = w_in.shape[0]
        inv_total = 1.0 / (tok.shape[0] * mesh4.size)
        mine = lax.axis_index('c').astype(jnp.int32).reshape(1)
        hidden = tok
        hiddens, pres = [], []
        for l in range(layers):
            hiddens.append(hidden)
            pre = jnp.dot(hidden, w_in[l], preferred_element_type=F32).astype(BF16)
            pres.append(pre)
            post = jax.nn.gelu(pre.astype(F32)).astype(BF16)
            hidden = (hidden.astype(F32) + jnp.dot(post, w_out[l], preferred_element_type=F32)).astype(BF16)
        grad = ((hidden.astype(F32) - tgt.astype(F32)) * inv_total).astype(BF16)

        rows = gather_rows([hiddens[layers - 1], grad], layers)
        sc_pieces, kernel_pieces = [], []
        for l in reversed(range(layers)):
            if l > 0:
                e = lax.dot_general(grad, w_out[l], COL, preferred_element_type=F32)
                p = jax.vjp(jax.nn.gelu, pres[l].astype(F32))[1](e)[0].astype(BF16)
                through = lax.dot_general(p, w_in[l], COL, preferred_element_type=F32)
                grad = (grad.astype(F32) + through).astype(BF16)
            flat = [r.reshape(-1, r.shape[-1]) for r in rows]
            shard, *rows = layer_grads(l, flat[0], flat[1], w_in, w_out, [hiddens[l - 1], grad] if l > 0 else [])
            if l in KERNEL_GATHER_LAYERS:
                kernel_pieces.append((l, block_gather(shard, layers + 1 + l)))
            else:
                if len(sc_pieces) >= 2:
                    before, blocks = sc_pieces[-2]
                    blocks, shard, *rows = lax.optimization_barrier((blocks, shard, *rows))
                    sc_pieces[-2] = (before, blocks)
                sc_pieces.append((l, lax.all_gather(shard[None], ('z', 'y', 'x'), axis=0, tiled=True)))

        outs = []
        first_layer, first_blocks = sc_pieces[0]
        last_layer, (near, far) = kernel_pieces[-1]
        first_blocks, far = lax.optimization_barrier((first_blocks, far))
        plan = [(first_layer, first_blocks)] + sc_pieces[1:-1] + kernel_pieces[:-1] + [(last_layer, (near, far))] + sc_pieces[-1:]
        for l, blocks in plan:
            if isinstance(blocks, (tuple, list)):
                own, away = blocks
            else:
                own = blocks
                if outs:
                    own, *outs = lax.optimization_barrier((own, *outs))
                away = lax.ppermute(own, 'c', [(0, 1), (1, 0)])
            outs = place_blocks(mine, own, outs, l, layers)
            outs = place_blocks(1 - mine, away, outs, l, layers)
        return outs[0], outs[1]

    spec = P(AXES, None)
    return jax.shard_map(local_step, mesh=mesh4, in_specs=(spec, spec, P(), P()), out_specs=(P(), P()), check_vma=False)
```

```python
import functools

import jax
import jax.numpy as jnp
from jax import lax
from jax.experimental import pallas as pl
from jax.experimental.pallas import tpu as pltpu
from jax.sharding import Mesh
from jax.sharding import PartitionSpec as P

AXES = ('z', 'y', 'x', 'c')
RING = 4
GROUPS = ('z', 'z', 'x', 'x')
OTHERS = {'x': ('z', 'y'), 'y': ('z', 'x'), 'z': ('y', 'x')}
CHUNK = 512
SLOTS = 4
ORDERS = (('x', 'y', 'z'), ('y', 'z', 'x'), ('z', 'x', 'y'))
GATHERED_TOGETHER = ((3,), (2, 1))
F32, BF16 = jnp.float32, jnp.bfloat16
COL = (((1,), (1,)), ((), ()))
GELU_S = 0.7978845608028654
GELU_C = 0.044715
MESH_ID = pl.DeviceIdType.MESH
MIB = 1 << 20


def place(axis, step):
    coords = [lax.axis_index(name) for name in AXES]
    which = AXES.index(axis)
    size = 2 if axis == 'c' else RING
    coords[which] = lax.rem(coords[which] + (step + size), size)
    return tuple(coords)


def remote(src, dst, sems, index, to):
    return pltpu.make_async_remote_copy(src_ref=src, dst_ref=dst, send_sem=sems[0].at[index], recv_sem=sems[1].at[index], device_id=to, device_id_type=MESH_ID)


def meet(axes):
    barrier = pltpu.get_barrier_semaphore()
    neighbours = [(axis, step) for axis in axes for step in (1, -1)] + [('c', 1)]
    for axis, step in neighbours:
        pl.semaphore_signal(barrier, inc=1, device_id=place(axis, step), device_id_type=MESH_ID)
    pl.semaphore_wait(barrier, len(neighbours))


class RowGather:
    def __init__(self, src, out, sems, axis):
        right, left, other = place(axis, 1), place(axis, -1), place('c', 1)
        half = src.shape[0] // 2
        top, bottom = pl.ds(0, half), pl.ds(half, half)
        self.src, self.out = src, out
        self.own = [remote(src, out.at[1], sems, 0, right), remote(src, out.at[2], sems, 1, left), remote(src, out.at[4], sems, 2, other)]
        self.onward = [
            remote(out.at[1, top], out.at[3, top], sems, 3, right),
            remote(out.at[2, bottom], out.at[3, bottom], sems, 4, left),
            remote(out.at[1], out.at[5], sems, 5, other),
            remote(out.at[2], out.at[6], sems, 6, other),
            remote(out.at[3], out.at[7], sems, 7, other),
        ]

    def begin(self):
        for copy in self.own:
            copy.start()
        self.out[0] = self.src[...]

    def middle(self):
        for side in range(2):
            self.own[side].wait_recv()
            self.onward[side].start()
            self.onward[2 + side].start()

    def late(self):
        self.onward[0].wait_recv()
        self.onward[1].wait_recv()
        self.onward[4].start()

    def finish(self):
        self.own[2].wait_recv()
        for copy in self.onward[2:]:
            copy.wait_recv()
        for copy in self.own + self.onward:
            copy.wait_send()


class RingSum:
    def __init__(self, parts, got, put, sems, axis):
        self.parts, self.got, self.put = parts, got, put
        self.me = lax.axis_index(axis)
        right, left = place(axis, 1), place(axis, -1)
        self.nxt, self.prv, self.opp = lax.rem(self.me + 1, RING), lax.rem(self.me + 3, RING), lax.rem(self.me + 2, RING)
        half = parts.shape[1] // 2
        self.top, self.bottom = pl.ds(0, half), pl.ds(half, half)
        self.first = [
            remote(parts.at[self.opp, self.top], got.at[0], sems, 0, right),
            remote(parts.at[self.opp, self.bottom], got.at[3], sems, 3, left),
            remote(parts.at[self.nxt, self.bottom], got.at[1], sems, 1, right),
            remote(parts.at[self.prv, self.top], got.at[4], sems, 4, left),
        ]
        self.second = [remote(got.at[0], got.at[2], sems, 2, right), remote(got.at[3], got.at[5], sems, 5, left)]

    def begin_far(self):
        self.first[0].start()
        self.first[1].start()

    def begin_near(self):
        self.first[2].start()
        self.first[3].start()

    def middle(self):
        self.first[0].wait_recv()
        self.got[0] = self.got[0] + self.parts[self.nxt, self.top]
        self.second[0].start()
        self.first[1].wait_recv()
        self.got[3] = self.got[3] + self.parts[self.prv, self.bottom]
        self.second[1].start()

    def finish(self):
        self.first[3].wait_recv()
        self.second[0].wait_recv()
        self.put(0, self.parts[self.me, self.top] + self.got[4] + self.got[2])
        self.first[2].wait_recv()
        self.second[1].wait_recv()
        self.put(1, self.parts[self.me, self.bottom] + self.got[1] + self.got[5])

    def drain(self):
        for copy in self.first + self.second:
            copy.wait_send()


def put_blocks(total, which, value):
    total[pl.ds(which * 2, 2)] = value.reshape((2,) + total.shape[1:])


def put_rows(total, offset, which, value):
    total[pl.ds(offset + which * value.shape[0], value.shape[0])] = value


def gelu_terms(x):
    square = x * x
    t = jnp.tanh(x * (GELU_S + GELU_S * GELU_C * square))
    cdf = 0.5 + 0.5 * t
    slope = cdf + (0.5 * x) * (1.0 - t * t) * (GELU_S + 3.0 * GELU_S * GELU_C * square)
    return x * cdf, slope


class Weights:
    def __init__(self, w_in, w_out, buf_in, buf_out, sems):
        self.w_in, self.w_out, self.buf_in, self.buf_out, self.sems = w_in, w_out, buf_in, buf_out, sems
        self.width = buf_in.shape[2]
        self.steps = w_in.shape[2] // self.width

    def copies(self, layer, chunk, slot):
        at = pl.ds(pl.multiple_of(chunk * self.width, self.width), self.width)
        return (
            pltpu.make_async_copy(self.w_in.at[layer, :, at], self.buf_in.at[slot], self.sems.at[0, slot]),
            pltpu.make_async_copy(self.w_out.at[layer, at, :], self.buf_out.at[slot], self.sems.at[1, slot]),
        )

    def start(self, layer, chunk, slot):
        for copy in self.copies(layer, chunk, slot):
            copy.start()

    def sweep(self, layer, base, following, body):
        def step(chunk, ahead):
            slot = lax.rem(base + chunk, SLOTS)
            for copy in self.copies(layer, chunk, slot):
                copy.wait()
            if ahead is not None:
                self.start(ahead[0], ahead[1], lax.rem(base + chunk + 2, SLOTS))
            body(chunk, self.buf_in.at[slot], self.buf_out.at[slot])

        @pl.loop(0, self.steps - 2)
        def _(chunk):
            step(chunk, (layer, chunk + 2))

        for last in range(2):
            step(self.steps - 2 + last, None if following is None else (following, last))


def forward_layer(weights, layer, base, following, hidden, pre, total, out):
    total[...] = jnp.zeros_like(total)
    half = weights.width // 2

    def body(chunk, wi, wo):
        posts = []
        for part in range(2):
            at = pl.ds(part * half, half)
            u = jnp.dot(hidden[...], wi[:, at], preferred_element_type=F32).astype(BF16)
            pre[:, pl.ds(pl.multiple_of(chunk * weights.width + part * half, half), half)] = u
            posts.append(gelu_terms(u.astype(F32))[0].astype(BF16))
        for part in range(2):
            total[...] += jnp.dot(posts[part], wo[pl.ds(part * half, half)], preferred_element_type=F32)

    weights.sweep(layer, base, following, body)
    out[...] = (hidden[...].astype(F32) + total[...]).astype(BF16)


def backward_layer(weights, layer, base, grad, pre, total, out):
    total[...] = jnp.zeros_like(total)
    half = weights.width // 2

    def body(chunk, wi, wo):
        grads = []
        for part in range(2):
            e = lax.dot_general(grad[...], wo[pl.ds(part * half, half)], COL, preferred_element_type=F32)
            u = pre[:, pl.ds(pl.multiple_of(chunk * weights.width + part * half, half), half)]
            grads.append((e * gelu_terms(u.astype(F32))[1]).astype(BF16))
        for part in range(2):
            total[...] += lax.dot_general(grads[part], wi[:, pl.ds(part * half, half)], COL, preferred_element_type=F32)

    weights.sweep(layer, base, None, body)
    out[...] = (grad[...].astype(F32) + total[...]).astype(BF16)


def forward_kernel(scale, tok, tgt, w_in, w_out, *refs):
    refs = list(refs)
    take = lambda count: [refs.pop(0) for _ in range(count)]
    kept_hidden, grad_below = take(2)
    gathered_out, pre_out = take(4), take(2)
    buf_in, buf_out, w_sems, pre, total, hid, grad, keep_sems = take(8)
    landing = take(4)
    sems = [take(2) for _ in range(4)]
    layers = w_in.shape[0]
    weights = Weights(w_in, w_out, buf_in, buf_out, w_sems)
    weights.start(0, 0, 0)
    weights.start(0, 1, 1)
    meet(('x', 'z'))
    moves = [
        RowGather(tok, landing[0], sems[0], GROUPS[0]),
        RowGather(hid.at[0], landing[1], sems[1], GROUPS[1]),
        RowGather(hid.at[2], landing[2], sems[2], GROUPS[3]),
        RowGather(grad, landing[3], sems[3], GROUPS[3]),
    ]
    stores = [pltpu.make_async_copy(landing[i], gathered_out[i], keep_sems.at[i]) for i in range(4)]
    stores += [pltpu.make_async_copy(pre.at[l], pre_out[l - 1], keep_sems.at[3 + l]) for l in (1, 2)]
    h = tok
    steps = weights.steps
    moves[0].begin()
    for l in range(layers):
        forward_layer(weights, l, l * steps, min(l + 1, layers - 1), h, pre.at[l], total, hid.at[l])
        h = hid.at[l]
        if l == 0:
            moves[1].begin()
        elif l == 1:
            stores[4].start()
            moves[0].middle()
        elif l == 2:
            stores[5].start()
            moves[2].begin()
            moves[1].middle()
            moves[0].late()
    grad[...] = ((h[...].astype(F32) - tgt[...].astype(F32)) * scale).astype(BF16)
    moves[3].begin()
    kept_hidden[...] = hid[1]
    backward_layer(weights, layers - 1, layers * steps, grad, pre.at[layers - 1], total, grad_below)
    moves[1].late()
    moves[0].finish()
    stores[0].start()
    moves[2].middle()
    moves[1].finish()
    stores[1].start()
    moves[3].middle()
    moves[2].late()
    moves[3].late()
    moves[2].finish()
    stores[2].start()
    moves[3].finish()
    stores[3].start()
    for store in stores:
        store.wait()


def forward(tok, tgt, w_in, w_out, total_rows, collective_id):
    vmem, anywhere = pl.BlockSpec(memory_space=pltpu.VMEM), pl.BlockSpec(memory_space=pl.ANY)
    n, d = tok.shape
    layers, _, full = w_in.shape
    row = jax.ShapeDtypeStruct((n, d), BF16)
    group = (2 * RING, n, d)
    width = min(CHUNK, full // 4)
    scratch = [pltpu.VMEM((SLOTS, d, width), BF16), pltpu.VMEM((SLOTS, width, d), BF16), pltpu.SemaphoreType.DMA((2, SLOTS))]
    scratch += [pltpu.VMEM((layers, n, full), BF16), pltpu.VMEM((n, d), F32), pltpu.VMEM((layers, n, d), BF16), pltpu.VMEM((n, d), BF16)]
    scratch += [pltpu.SemaphoreType.DMA((6,))] + [pltpu.VMEM(group, BF16)] * 4 + [pltpu.SemaphoreType.DMA((8,))] * 8
    return pl.pallas_call(
        functools.partial(forward_kernel, 1.0 / total_rows),
        out_shape=[row, row] + [jax.ShapeDtypeStruct(group, BF16)] * 4 + [jax.ShapeDtypeStruct((n, full), BF16)] * 2,
        in_specs=[vmem, vmem, anywhere, anywhere],
        out_specs=[vmem, vmem] + [anywhere] * 6,
        scratch_shapes=scratch,
        compiler_params=pltpu.CompilerParams(collective_id=collective_id, has_side_effects=True, vmem_limit_bytes=60 * MIB),
        cost_estimate=pl.CostEstimate(flops=30_000_000_000, bytes_accessed=96 * MIB, transcendentals=0),
        name='forward',
    )(tok, tgt, w_in, w_out)


def layer_kernel(layer, axes, gathers, chain, hg_in, gg_in, w_in, w_out, *refs):
    group, first, second = axes
    refs = list(refs)
    take = lambda count: [refs.pop(0) for _ in range(count)]
    rows_in = take(gathers)
    pre_in = take(1) if chain else []
    (shard,) = take(1)
    rows_out = take(gathers)
    below = take(1) if chain else []
    hg, gg, wi, wo, wi_t, act, slope_grad, w_sems, row_sems = take(9)
    stage_one, stage_two = [], []
    for color, (one, two) in enumerate(((first, second), (second, first))):
        parts, got_one, mid, got_two, send_one, recv_one, send_two, recv_two = take(8)
        stage_one.append(RingSum(parts, got_one, functools.partial(put_blocks, mid), (send_one, recv_one), one))
        stage_two.append(RingSum(mid, got_two, functools.partial(put_rows, shard, color * mid.shape[1]), (send_two, recv_two), two))
    landing = take(gathers)
    moves = [RowGather(src, out, take(2), GROUPS[layer - 1]) for src, out in zip(rows_in, landing)]
    if gathers:
        (keep_sems,) = take(1)
        stores = [pltpu.make_async_copy(landing[i], rows_out[i], keep_sems.at[i]) for i in range(gathers)]
    if chain:
        buf_in, buf_out, stream_sems, pre, total, pre_sem = take(6)
        weights = Weights(w_in, w_out, buf_in, buf_out, stream_sems)

    width = wi.shape[1]
    start = (lax.axis_index(group) * 2 + lax.axis_index('c')) * width
    start = pl.multiple_of(start, width)
    loads = [
        pltpu.make_async_copy(w_in.at[layer, :, pl.ds(start, width)], wi, w_sems.at[0]),
        pltpu.make_async_copy(w_out.at[layer, pl.ds(start, width), :], wo, w_sems.at[1]),
    ]
    for load in loads:
        load.start()
    tokens = hg.shape[0]
    chunk = min(256, tokens)

    def row_copies(i):
        at = pl.ds(pl.multiple_of(i * chunk, chunk), chunk)
        return [pltpu.make_async_copy(src.at[at], dst.at[at], row_sems.at[k, i]) for k, (src, dst) in enumerate(((hg_in, hg), (gg_in, gg)))]

    for i in range(tokens // chunk):
        for copy in row_copies(i):
            copy.start()
    if chain:
        weights.start(layer - 1, 0, 0)
        weights.start(layer - 1, 1, 1)
        pre_copy = pltpu.make_async_copy(pre_in[0], pre, pre_sem.at[0])
        pre_copy.start()
    meet(('x', 'y', 'z'))
    for move in moves:
        move.begin()
    loads[0].wait()
    wi_t[...] = wi[...].T
    loads[1].wait()

    @pl.loop(0, tokens // chunk)
    def _(i):
        for copy in row_copies(i):
            copy.wait()
        at = pl.ds(pl.multiple_of(i * chunk, chunk), chunk)
        u = lax.dot_general(wi_t[...], hg[at], COL, preferred_element_type=F32).astype(BF16)
        e = lax.dot_general(wo[...], gg[at], COL, preferred_element_type=F32)
        post, slope = gelu_terms(u.astype(F32))
        act[:, at] = post.astype(BF16)
        slope_grad[:, at] = (e * slope).astype(BF16)

    cols = stage_one[0].parts.shape[2]

    def fill(color, which):
        at = pl.ds(pl.multiple_of(which * cols, cols), cols)
        left, right = (slope_grad, hg) if color == 0 else (act, gg)
        stage_one[color].parts[which] = jnp.dot(left[...], right[:, at], preferred_element_type=F32)

    for color in range(2):
        fill(color, stage_one[color].opp)
        stage_one[color].begin_far()
    for color in range(2):
        fill(color, stage_one[color].nxt)
        fill(color, stage_one[color].prv)
        stage_one[color].begin_near()
    for color in range(2):
        fill(color, stage_one[color].me)
    if moves:
        moves[0].middle()
    for stage in stage_one:
        stage.middle()
    if chain:
        pre_copy.wait()
        backward_layer(weights, layer - 1, 0, rows_in[0], pre, total, below[0])
    for move in moves[1:]:
        move.middle()
    for one, two in zip(stage_one, stage_two):
        one.finish()
        two.begin_far()
        two.begin_near()
    if moves:
        moves[0].late()
    for stage in stage_two:
        stage.middle()
    for stage in stage_two:
        stage.finish()
    for move in moves[1:]:
        move.late()
    for i, move in enumerate(moves):
        move.finish()
        stores[i].start()
    for stage in stage_one + stage_two:
        stage.drain()
    for i in range(gathers):
        stores[i].wait()


def layer_grads(layer, hg, gg, w_in, w_out, rows, pre):
    vmem, anywhere = pl.BlockSpec(memory_space=pltpu.VMEM), pl.BlockSpec(memory_space=pl.ANY)
    tokens, d = hg.shape
    full = w_in.shape[2]
    width = full // (2 * RING)
    cols, n = d // RING, width // RING
    chain = pre is not None
    out_shape = [jax.ShapeDtypeStruct((2 * n, cols), F32)]
    out_shape += [jax.ShapeDtypeStruct((2 * RING,) + row.shape, row.dtype) for row in rows]
    scratch = [pltpu.VMEM((tokens, d), BF16)] * 2
    scratch += [pltpu.VMEM((d, width), BF16), pltpu.VMEM((width, d), BF16), pltpu.VMEM((width, d), BF16)]
    scratch += [pltpu.VMEM((width, tokens), BF16)] * 2 + [pltpu.SemaphoreType.DMA((2,)), pltpu.SemaphoreType.DMA((2, max(tokens // 256, 1)))]
    for _ in range(2):
        scratch += [pltpu.VMEM((RING, width, cols), F32), pltpu.VMEM((6, width // 2, cols), F32)]
        scratch += [pltpu.VMEM((RING, n, cols), F32), pltpu.VMEM((6, n // 2, cols), F32)]
        scratch += [pltpu.SemaphoreType.DMA((6,))] * 4
    scratch += [pltpu.VMEM((2 * RING,) + row.shape, row.dtype) for row in rows]
    scratch += [pltpu.SemaphoreType.DMA((8,))] * (2 * len(rows))
    if rows:
        scratch += [pltpu.SemaphoreType.DMA((len(rows),))]
    if chain:
        m = rows[0].shape[0]
        chunk = min(CHUNK, full // 4)
        out_shape.append(jax.ShapeDtypeStruct(rows[0].shape, BF16))
        scratch += [pltpu.VMEM((SLOTS, d, chunk), BF16), pltpu.VMEM((SLOTS, chunk, d), BF16), pltpu.SemaphoreType.DMA((2, SLOTS))]
        scratch += [pltpu.VMEM((m, full), BF16), pltpu.VMEM((m, d), F32), pltpu.SemaphoreType.DMA((1,))]
    group = GROUPS[layer]
    return pl.pallas_call(
        functools.partial(layer_kernel, layer, (group,) + OTHERS[group], len(rows), chain),
        out_shape=out_shape,
        in_specs=[anywhere] * 4 + [vmem] * len(rows) + [anywhere] * chain,
        out_specs=[vmem] + [anywhere] * len(rows) + [vmem] * chain,
        scratch_shapes=scratch,
        compiler_params=pltpu.CompilerParams(collective_id=layer, has_side_effects=True, vmem_limit_bytes=60 * MIB),
        cost_estimate=pl.CostEstimate(flops=30_000_000_000, bytes_accessed=16 * MIB, transcendentals=0),
        name='layer_grads',
    )(hg, gg, w_in, w_out, *rows, *([pre] if chain else []))


class BlockGather:
    def __init__(self, near, far, out, order, rows, sems, local_sems, base):
        self.near, self.far, self.out = near, far, out
        self.order, self.rows, self.sems, self.local_sems = order, rows, sems, local_sems
        self.index = {axis: lax.axis_index(axis) for axis in 'xyz'}
        self.base, self.count, self.local_count = base, 0, 0
        self.other = place('c', 1)
        self.copies, self.cross, self.local = {}, [], []

    def at(self, phase, which, half=None):
        picks, rows = {}, self.rows
        for k, axis in enumerate(self.order):
            picks[axis] = pl.ds(0, RING) if k < phase else self.index[axis]
        if phase < 3:
            picks[self.order[phase]] = which
        if half is not None:
            if phase == 0:
                cut = (rows[1] // 16) * 8
                rows = (rows[0], cut) if half == 0 else (rows[0] + cut, rows[1] - cut)
            else:
                picks[self.order[phase - 1]] = pl.ds(half * 2, 2)
        return tuple(picks[axis] for axis in ('z', 'y', 'x')) + (pl.ds(*rows),)

    def send(self, where, to, dst=None):
        dst = self.near if dst is None else dst
        copy = remote(self.near.at[where], dst.at[where], self.sems, self.base + self.count, to)
        self.count += 1
        copy.start()
        return copy

    def cross_over(self, where):
        self.cross.append((self.send(where, self.other, self.far), where))
        self.keep(0, where)

    def keep(self, side, where):
        core = lax.rem(lax.axis_index('c') + side, 2)
        copy = pltpu.make_async_copy((self.near, self.far)[side].at[where], self.out.at[where[:3] + (core,) + where[3:]], self.local_sems.at[self.base + self.local_count])
        self.local_count += 1
        copy.start()
        self.local.append(copy)

    def begin(self, phase):
        axis = self.order[phase]
        me = self.index[axis]
        self.ends = (place(axis, 1), place(axis, -1))
        self.around = (lax.rem(me + 3, RING), lax.rem(me + 1, RING), lax.rem(me + 2, RING))
        whole = self.at(phase, me)
        self.near_copies = [self.send(whole, end) for end in self.ends]
        if phase == 2:
            self.cross_over(whole)

    def middle(self, phase):
        self.far_copies = []
        for side in range(2):
            self.near_copies[side].wait_recv()
            self.far_copies.append(self.send(self.at(phase, self.around[side], side), self.ends[side]))
            if phase == 2:
                self.cross_over(self.at(phase, self.around[side]))

    def finish(self, phase):
        for copy in self.far_copies:
            copy.wait_recv()
        for copy in self.near_copies + self.far_copies:
            self.copies[id(copy)] = copy
        if phase == 2:
            self.cross_over(self.at(phase, self.around[2]))

    def close(self):
        for copy, where in self.cross:
            copy.wait_recv()
            self.keep(1, where)
        for copy in list(self.copies.values()) + [c for c, _ in self.cross]:
            copy.wait_send()
        for copy in self.local:
            copy.wait()


BLOCK_SEMS = 16


def block_gather_kernel(shard, out, near, far, send, recv, local_sems):
    me = tuple(lax.axis_index(axis) for axis in ('z', 'y', 'x'))
    near[me] = shard[...]
    tiles = shard.shape[0] // 8
    cuts = [0, -(-tiles // 3), -(-2 * tiles // 3), tiles]
    meet(('x', 'y', 'z'))
    colors = [
        BlockGather(near, far, out, ORDERS[k], (8 * cuts[k], 8 * (cuts[k + 1] - cuts[k])), (send, recv), local_sems, k * BLOCK_SEMS) for k in range(3)
    ]
    for phase in range(3):
        for stage in ('begin', 'middle', 'finish'):
            for color in colors:
                getattr(color, stage)(phase)
    for color in colors:
        color.close()


def block_gather(shard, collective_id):
    vmem, anywhere = pl.BlockSpec(memory_space=pltpu.VMEM), pl.BlockSpec(memory_space=pl.ANY)
    shape = (RING, RING, RING) + shard.shape
    return pl.pallas_call(
        block_gather_kernel,
        out_shape=jax.ShapeDtypeStruct((RING, RING, RING, 2) + shard.shape, F32),
        in_specs=[vmem],
        out_specs=anywhere,
        scratch_shapes=[pltpu.VMEM(shape, F32)] * 2 + [pltpu.SemaphoreType.DMA((3 * BLOCK_SEMS,))] * 3,
        compiler_params=pltpu.CompilerParams(collective_id=collective_id, has_side_effects=True, vmem_limit_bytes=48 * MIB),
        cost_estimate=pl.CostEstimate(flops=60_000_000_000, bytes_accessed=32 * MIB, transcendentals=0),
        name='block_gather',
    )(shard)


def place_kernel(src_in, src_out, *refs):
    out_in, out_out = refs[-2:]
    n, cols = src_in.shape[-2:]
    for a in range(RING):
        for b in range(RING):
            out_in[a * cols : (a + 1) * cols, b * n : (b + 1) * n] = src_in[a, b].T
            out_out[a * n : (a + 1) * n, b * cols : (b + 1) * cols] = src_out[a, b]


def place_blocks(blocks, which, outs, layer, layers):
    cols = blocks.shape[-1]
    n = cols // 2
    width, d = n * RING, cols * RING
    shapes = [jax.ShapeDtypeStruct((layers, d, width * 2 * RING), F32), jax.ShapeDtypeStruct((layers, width * 2 * RING, d), F32)]
    along = AXES.index(GROUPS[layer])
    picked = tuple(None if k == along else RING for k in range(3))
    src_specs = [
        pl.BlockSpec(picked + (None, n, cols), functools.partial(lambda k, i, c: tuple(i if dim == along else 0 for dim in range(3)) + (c, 2 * which + k, 0), k))
        for k in range(2)
    ]
    return pl.pallas_call(
        place_kernel,
        grid=(RING, 2),
        in_specs=src_specs + [pl.BlockSpec(memory_space=pl.ANY)] * len(outs),
        out_specs=[
            pl.BlockSpec((None, d, width), lambda i, c: (layer, 0, i * 2 + c)),
            pl.BlockSpec((None, width, d), lambda i, c: (layer, i * 2 + c, 0)),
        ],
        out_shape=shapes,
        input_output_aliases={2 + k: k for k in range(len(outs))},
        compiler_params=pltpu.CompilerParams(vmem_limit_bytes=63 * MIB),
        cost_estimate=pl.CostEstimate(flops=10_000_000_000, bytes_accessed=64 * MIB, transcendentals=0),
        name='place_blocks',
    )(blocks, blocks, *outs)


def solution(mesh):
    mesh4 = Mesh(mesh.devices.reshape(RING, RING, RING, 2), AXES)

    def local_step(tok, tgt, w_in, w_out):
        layers = w_in.shape[0]
        hidden, grad, h0, h1, h3, g4, pre1, pre2 = forward(tok, tgt, w_in, w_out, tok.shape[0] * mesh4.size, 2 * layers)
        flat = lambda r: r.reshape(-1, r.shape[-1])
        shards, gathered = {}, {}
        hg, gg = [h0, h1, None, h3], g4
        for l in reversed(range(layers)):
            if l == 3:
                shard, gg, hg[2], grad = layer_grads(l, flat(hg[l]), flat(gg), w_in, w_out, [grad, hidden], pre2)
            elif l == 2:
                shard, gg, grad = layer_grads(l, flat(hg[l]), flat(gg), w_in, w_out, [grad], pre1)
            elif l == 1:
                shard, gg = layer_grads(l, flat(hg[l]), flat(gg), w_in, w_out, [grad], None)
            else:
                (shard,) = layer_grads(l, flat(hg[l]), flat(gg), w_in, w_out, [], None)
            shards[l] = shard
            for part in GATHERED_TOGETHER:
                if part[-1] == l:
                    blocks = jnp.concatenate([shards[k] for k in part], axis=0)
                    full = lax.all_gather(blocks[None], AXES, axis=0, tiled=True)
                    gathered[part] = full.reshape((RING, RING, RING, 2) + blocks.shape)
        last = block_gather(shards[0], layers + 1)
        outs = []
        first, second = GATHERED_TOGETHER
        gathered[first], last = lax.optimization_barrier((gathered[first], last))
        for i, l in enumerate(first):
            outs = place_blocks(gathered[first], i, outs, l, layers)
        outs = place_blocks(last, 0, outs, 0, layers)
        blocks, *outs = lax.optimization_barrier((gathered[second], *outs))
        for i, l in enumerate(second):
            outs = place_blocks(blocks, i, outs, l, layers)
        return outs[0], outs[1]

    spec = P(AXES, None)
    return jax.shard_map(local_step, mesh=mesh4, in_specs=(spec, spec, P(), P()), out_specs=(P(), P()), check_vma=False)
```

```python
import functools

import jax
import jax.numpy as jnp
from jax import lax
from jax.experimental import pallas as pl
from jax.experimental.pallas import tpu as pltpu
from jax.sharding import Mesh
from jax.sharding import PartitionSpec as P

AXES = ('z', 'y', 'x', 'c')
RING = 4
GROUPS = ('z', 'z', 'x', 'x')
OTHERS = {'x': ('z', 'y'), 'y': ('z', 'x'), 'z': ('y', 'x')}
CHUNK = 512
SLOTS = 3
ORDERS = (('x', 'y', 'z'), ('y', 'z', 'x'), ('z', 'x', 'y'))
GATHERED_TOGETHER = ((3,), (2, 1))
F32, BF16 = jnp.float32, jnp.bfloat16
COL = (((1,), (1,)), ((), ()))
GELU_S = 0.7978845608028654
GELU_C = 0.044715
MESH_ID = pl.DeviceIdType.MESH
MIB = 1 << 20


def place(axis, step):
    coords = [lax.axis_index(name) for name in AXES]
    which = AXES.index(axis)
    size = 2 if axis == 'c' else RING
    coords[which] = lax.rem(coords[which] + (step + size), size)
    return tuple(coords)


def remote(src, dst, sems, index, to):
    return pltpu.make_async_remote_copy(src_ref=src, dst_ref=dst, send_sem=sems[0].at[index], recv_sem=sems[1].at[index], device_id=to, device_id_type=MESH_ID)


def meet(axes):
    barrier = pltpu.get_barrier_semaphore()
    neighbours = [(axis, step) for axis in axes for step in (1, -1)] + [('c', 1)]
    for axis, step in neighbours:
        pl.semaphore_signal(barrier, inc=1, device_id=place(axis, step), device_id_type=MESH_ID)
    pl.semaphore_wait(barrier, len(neighbours))


class RowGather:
    def __init__(self, src, out, sems, axis):
        right, left, other = place(axis, 1), place(axis, -1), place('c', 1)
        half = src.shape[0] // 2
        top, bottom = pl.ds(0, half), pl.ds(half, half)
        self.src, self.out, self.landed = src, out, set()
        self.own = [remote(src, out.at[1], sems, 0, right), remote(src, out.at[2], sems, 1, left), remote(src, out.at[4], sems, 2, other)]
        self.onward = [
            remote(out.at[1, top], out.at[3, top], sems, 3, right),
            remote(out.at[2, bottom], out.at[3, bottom], sems, 4, left),
            remote(out.at[1], out.at[5], sems, 5, other),
            remote(out.at[2], out.at[6], sems, 6, other),
            remote(out.at[3], out.at[7], sems, 7, other),
        ]
        self.brings = {1: self.own[:1], 2: self.own[1:2], 3: self.onward[:2], 4: self.own[2:], 5: self.onward[2:3], 6: self.onward[3:4], 7: self.onward[4:]}

    def arrive(self, *slots):
        for slot in slots:
            if slot and slot not in self.landed:
                self.landed.add(slot)
                for copy in self.brings[slot]:
                    copy.wait_recv()

    def begin(self):
        for copy in self.own:
            copy.start()
        self.out[0] = self.src[...]

    def middle(self):
        for side in range(2):
            self.arrive(1 + side)
            self.onward[side].start()
            self.onward[2 + side].start()

    def late(self):
        self.arrive(3)
        self.onward[4].start()

    def finish(self):
        self.arrive(4, 5, 6, 7)
        for copy in self.own + self.onward:
            copy.wait_send()


class RingSum:
    def __init__(self, parts, got, put, sems, axis):
        self.parts, self.got, self.put = parts, got, put
        self.me = lax.axis_index(axis)
        right, left = place(axis, 1), place(axis, -1)
        self.nxt, self.prv, self.opp = lax.rem(self.me + 1, RING), lax.rem(self.me + 3, RING), lax.rem(self.me + 2, RING)
        half = parts.shape[1] // 2
        self.top, self.bottom = pl.ds(0, half), pl.ds(half, half)
        self.first = [
            remote(parts.at[self.opp, self.top], got.at[0], sems, 0, right),
            remote(parts.at[self.opp, self.bottom], got.at[3], sems, 3, left),
            remote(parts.at[self.nxt, self.bottom], got.at[1], sems, 1, right),
            remote(parts.at[self.prv, self.top], got.at[4], sems, 4, left),
        ]
        self.second = [remote(got.at[0], got.at[2], sems, 2, right), remote(got.at[3], got.at[5], sems, 5, left)]

    def begin_far(self):
        self.first[0].start()
        self.first[1].start()

    def begin_near(self):
        self.first[2].start()
        self.first[3].start()

    def middle(self):
        self.first[0].wait_recv()
        self.got[0] = self.got[0] + self.parts[self.nxt, self.top]
        self.second[0].start()
        self.first[1].wait_recv()
        self.got[3] = self.got[3] + self.parts[self.prv, self.bottom]
        self.second[1].start()

    def finish(self):
        self.first[3].wait_recv()
        self.second[0].wait_recv()
        self.put(0, self.parts[self.me, self.top] + self.got[4] + self.got[2])
        self.first[2].wait_recv()
        self.second[1].wait_recv()
        self.put(1, self.parts[self.me, self.bottom] + self.got[1] + self.got[5])

    def drain(self):
        for copy in self.first + self.second:
            copy.wait_send()


def put_blocks(total, which, value):
    total[pl.ds(which * 2, 2)] = value.reshape((2,) + total.shape[1:])


def put_rows(total, offset, which, value):
    total[pl.ds(offset + which * value.shape[0], value.shape[0])] = value


def gelu_terms(x):
    square = x * x
    t = jnp.tanh(x * (GELU_S + GELU_S * GELU_C * square))
    cdf = 0.5 + 0.5 * t
    slope = cdf + (0.5 * x) * (1.0 - t * t) * (GELU_S + 3.0 * GELU_S * GELU_C * square)
    return x * cdf, slope


class Weights:
    def __init__(self, w_in, w_out, buf_in, buf_out, sems):
        self.w_in, self.w_out, self.buf_in, self.buf_out, self.sems = w_in, w_out, buf_in, buf_out, sems
        self.width = buf_in.shape[2]
        self.steps = w_in.shape[2] // self.width

    def copies(self, layer, chunk, slot):
        at = pl.ds(pl.multiple_of(chunk * self.width, self.width), self.width)
        return (
            pltpu.make_async_copy(self.w_in.at[layer, :, at], self.buf_in.at[slot], self.sems.at[0, slot]),
            pltpu.make_async_copy(self.w_out.at[layer, at, :], self.buf_out.at[slot], self.sems.at[1, slot]),
        )

    def start(self, layer, chunk, slot):
        for copy in self.copies(layer, chunk, slot):
            copy.start()

    def sweep(self, layer, base, following, body):
        def step(chunk, ahead):
            slot = lax.rem(base + chunk, SLOTS)
            for copy in self.copies(layer, chunk, slot):
                copy.wait()
            if ahead is not None:
                self.start(ahead[0], ahead[1], lax.rem(base + chunk + 2, SLOTS))
            body(chunk, self.buf_in.at[slot], self.buf_out.at[slot])

        @pl.loop(0, self.steps - 2)
        def _(chunk):
            step(chunk, (layer, chunk + 2))

        for last in range(2):
            step(self.steps - 2 + last, None if following is None else (following, last))


def forward_layer(weights, layer, base, following, hidden, pre, total, out):
    total[...] = jnp.zeros_like(total)
    half = weights.width // 2

    def body(chunk, wi, wo):
        posts = []
        for part in range(2):
            at = pl.ds(part * half, half)
            u = jnp.dot(hidden[...], wi[:, at], preferred_element_type=F32).astype(BF16)
            if pre is not None:
                pre[:, pl.ds(pl.multiple_of(chunk * weights.width + part * half, half), half)] = u
            posts.append(gelu_terms(u.astype(F32))[0].astype(BF16))
        for part in range(2):
            total[...] += jnp.dot(posts[part], wo[pl.ds(part * half, half)], preferred_element_type=F32)

    weights.sweep(layer, base, following, body)
    out[...] = (hidden[...].astype(F32) + total[...]).astype(BF16)


def backward_layer(weights, layer, base, following, grad, pre, total, out):
    total[...] = jnp.zeros_like(total)
    half = weights.width // 2

    def body(chunk, wi, wo):
        grads = []
        for part in range(2):
            e = lax.dot_general(grad[...], wo[pl.ds(part * half, half)], COL, preferred_element_type=F32)
            u = pre[:, pl.ds(pl.multiple_of(chunk * weights.width + part * half, half), half)]
            grads.append((e * gelu_terms(u.astype(F32))[1]).astype(BF16))
        for part in range(2):
            total[...] += lax.dot_general(grads[part], wi[:, pl.ds(part * half, half)], COL, preferred_element_type=F32)

    weights.sweep(layer, base, following, body)
    out[...] = (grad[...].astype(F32) + total[...]).astype(BF16)


class ShardWork:
    def __init__(self, layer, w_in, w_out, shard, take):
        group = GROUPS[layer]
        self.wi, self.wo, self.wi_t, self.act, self.slope, w_sems = take(6)
        self.stage_one, self.stage_two = [], []
        for color in range(2):
            one, two = OTHERS[group][color], OTHERS[group][1 - color]
            parts, got_one, mid, got_two, send_one, recv_one, send_two, recv_two = take(8)
            self.stage_one.append(RingSum(parts, got_one, functools.partial(put_blocks, mid), (send_one, recv_one), one))
            self.stage_two.append(RingSum(mid, got_two, functools.partial(put_rows, shard, color * mid.shape[1]), (send_two, recv_two), two))
        width = self.wi.shape[1]
        start = pl.multiple_of((lax.axis_index(group) * 2 + lax.axis_index('c')) * width, width)
        self.loads = [
            pltpu.make_async_copy(w_in.at[layer, :, pl.ds(start, width)], self.wi, w_sems.at[0]),
            pltpu.make_async_copy(w_out.at[layer, pl.ds(start, width), :], self.wo, w_sems.at[1]),
        ]

    def load(self):
        for load in self.loads:
            load.start()

    def ready(self):
        self.loads[0].wait()
        self.wi_t[...] = self.wi[...].T
        self.loads[1].wait()

    def rows(self, hg, gg, slot):
        n = hg.shape[1]
        at = pl.ds(pl.multiple_of(slot * n, n), n)
        u = lax.dot_general(self.wi_t[...], hg[slot], COL, preferred_element_type=F32).astype(BF16)
        e = lax.dot_general(self.wo[...], gg[slot], COL, preferred_element_type=F32)
        post, slope = gelu_terms(u.astype(F32))
        self.act[:, at] = post.astype(BF16)
        self.slope[:, at] = (e * slope).astype(BF16)

    def fill(self, color, which, hg, gg):
        cols = self.stage_one[color].parts.shape[2]
        at = pl.ds(pl.multiple_of(which * cols, cols), cols)
        left, right = (self.slope, hg) if color == 0 else (self.act, gg)
        self.stage_one[color].parts[which] = jnp.dot(left[...], right[:, :, at].reshape(-1, cols), preferred_element_type=F32)

    def multiply(self, hg, gg):
        for color in range(2):
            self.fill(color, self.stage_one[color].opp, hg, gg)
            self.stage_one[color].begin_far()
        for color in range(2):
            self.fill(color, self.stage_one[color].nxt, hg, gg)
            self.fill(color, self.stage_one[color].prv, hg, gg)
            self.stage_one[color].begin_near()
        for color in range(2):
            self.fill(color, self.stage_one[color].me, hg, gg)

    def middle_one(self):
        for stage in self.stage_one:
            stage.middle()

    def turn(self):
        for one, two in zip(self.stage_one, self.stage_two):
            one.finish()
            two.begin_far()
            two.begin_near()

    def finish_two(self):
        for stage in self.stage_two:
            stage.middle()
        for stage in self.stage_two:
            stage.finish()

    def drain(self):
        for stage in self.stage_one + self.stage_two:
            stage.drain()


def shard_scratch(tokens, d, width):
    cols, n = d // RING, width // RING
    scratch = [pltpu.VMEM((d, width), BF16), pltpu.VMEM((width, d), BF16), pltpu.VMEM((width, d), BF16)]
    scratch += [pltpu.VMEM((width, tokens), BF16)] * 2 + [pltpu.SemaphoreType.DMA((2,))]
    for _ in range(2):
        scratch += [pltpu.VMEM((RING, width, cols), F32), pltpu.VMEM((6, width // 2, cols), F32)]
        scratch += [pltpu.VMEM((RING, n, cols), F32), pltpu.VMEM((6, n // 2, cols), F32)]
        scratch += [pltpu.SemaphoreType.DMA((6,))] * 4
    return scratch


def stream_scratch(d, full):
    width = min(CHUNK, full // 4)
    return [pltpu.VMEM((SLOTS, d, width), BF16), pltpu.VMEM((SLOTS, width, d), BF16), pltpu.SemaphoreType.DMA((2, SLOTS))]


def first_kernel(scale, tok, tgt, w_in, w_out, *refs):
    refs = list(refs)
    take = lambda count: [refs.pop(0) for _ in range(count)]
    shard, below = take(2)
    gathered_out, pre_out = take(4), take(1)[0]
    buf_in, buf_out, w_sems, pre, total, hid, grads, keep_sems = take(8)
    landing = take(6)
    sems = [take(2) for _ in range(6)]
    layers = w_in.shape[0]
    top = layers - 1
    weights = Weights(w_in, w_out, buf_in, buf_out, w_sems)
    work = ShardWork(top, w_in, w_out, shard, take)
    weights.start(0, 0, 0)
    weights.start(0, 1, 1)
    work.load()
    meet(('x', 'y', 'z'))
    h0, h1 = RowGather(tok, landing[0], sems[0], GROUPS[0]), RowGather(hid.at[0], landing[1], sems[1], GROUPS[1])
    h3, g4 = RowGather(hid.at[2], landing[2], sems[2], GROUPS[3]), RowGather(grads.at[0], landing[3], sems[3], GROUPS[3])
    h2, g3 = RowGather(hid.at[1], landing[4], sems[4], GROUPS[2]), RowGather(grads.at[1], landing[5], sems[5], GROUPS[2])
    stores = [pltpu.make_async_copy(landing[k], gathered_out[i], keep_sems.at[i]) for i, k in enumerate((0, 1, 4, 5))]
    stores.append(pltpu.make_async_copy(pre.at[0], pre_out, keep_sems.at[4]))
    h = tok
    steps = weights.steps
    h0.begin()
    for l in range(layers):
        forward_layer(weights, l, l * steps, min(l + 1, top), h, pre.at[l - 1] if l else None, total, hid.at[l])
        h = hid.at[l]
        if l == 0:
            h1.begin()
        elif l == 1:
            stores[4].start()
            h0.middle()
            work.ready()
        elif l == 2:
            h3.begin()
            h1.middle()
            h0.late()
    grads[0] = ((h[...].astype(F32) - tgt[...].astype(F32)) * scale).astype(BF16)
    g4.begin()
    backward_layer(weights, top, layers * steps, top - 1, grads.at[0], pre.at[top - 1], total, grads.at[1])
    hg, gg = landing[2], landing[3]
    work.rows(hg, gg, 0)
    h1.late()
    h0.finish()
    stores[0].start()
    h3.middle()
    h3.arrive(4)
    g4.arrive(4)
    work.rows(hg, gg, 4)
    h1.finish()
    stores[1].start()
    g4.middle()
    g3.begin()
    h2.begin()

    def pair(first):
        @pl.loop(first, first + 2)
        def _(slot):
            work.rows(hg, gg, slot)

    pair(1)
    h3.late()
    h3.arrive(5, 6)
    g4.arrive(5, 6)
    pair(5)
    g4.late()
    work.rows(hg, gg, 3)
    h3.arrive(7)
    g4.arrive(7)
    work.rows(hg, gg, 7)
    work.multiply(hg, gg)
    g3.middle()
    work.middle_one()
    backward_layer(weights, top - 1, (layers + 1) * steps, None, grads.at[1], pre.at[top - 2], total, below)
    h2.middle()
    work.turn()
    g3.late()
    work.finish_two()
    h2.late()
    g3.finish()
    stores[3].start()
    h2.finish()
    stores[2].start()
    for move in (h3, g4):
        move.finish()
    work.drain()
    for store in stores:
        store.wait()


def first(tok, tgt, w_in, w_out, total_rows, collective_id):
    vmem, anywhere = pl.BlockSpec(memory_space=pltpu.VMEM), pl.BlockSpec(memory_space=pl.ANY)
    n, d = tok.shape
    layers, _, full = w_in.shape
    row = jax.ShapeDtypeStruct((n, d), BF16)
    group = (2 * RING, n, d)
    block = jax.ShapeDtypeStruct((full // (4 * RING), d // RING), F32)
    scratch = stream_scratch(d, full)
    scratch += [pltpu.VMEM((layers - 1, n, full), BF16), pltpu.VMEM((n, d), F32), pltpu.VMEM((layers, n, d), BF16), pltpu.VMEM((2, n, d), BF16)]
    scratch += [pltpu.SemaphoreType.DMA((5,))] + [pltpu.VMEM(group, BF16)] * 6 + [pltpu.SemaphoreType.DMA((8,))] * 12
    scratch += shard_scratch(2 * RING * n, d, full // (2 * RING))
    return pl.pallas_call(
        functools.partial(first_kernel, 1.0 / total_rows),
        out_shape=[block, row] + [jax.ShapeDtypeStruct(group, BF16)] * 4 + [jax.ShapeDtypeStruct((n, full), BF16)],
        in_specs=[vmem, vmem, anywhere, anywhere],
        out_specs=[vmem, vmem] + [anywhere] * 5,
        scratch_shapes=scratch,
        compiler_params=pltpu.CompilerParams(collective_id=collective_id, has_side_effects=True, vmem_limit_bytes=67_000_000),
        cost_estimate=pl.CostEstimate(flops=60_000_000_000, bytes_accessed=96 * MIB, transcendentals=0),
        name='first',
    )(tok, tgt, w_in, w_out)


def layer_kernel(layer, gathers, chain, hg_in, gg_in, w_in, w_out, *refs):
    refs = list(refs)
    take = lambda count: [refs.pop(0) for _ in range(count)]
    rows_in = take(gathers)
    pre_in = take(1) if chain else []
    (shard,) = take(1)
    rows_out = take(gathers)
    below = take(1) if chain else []
    hg, gg, row_sems = take(3)
    work = ShardWork(layer, w_in, w_out, shard, take)
    landing = take(gathers)
    moves = [RowGather(src, out, take(2), GROUPS[layer - 1]) for src, out in zip(rows_in, landing)]
    if gathers:
        (keep_sems,) = take(1)
        stores = [pltpu.make_async_copy(landing[i], rows_out[i], keep_sems.at[i]) for i in range(gathers)]
    if chain:
        buf_in, buf_out, stream_sems, pre, total, pre_sem = take(6)
        weights = Weights(w_in, w_out, buf_in, buf_out, stream_sems)
    work.load()

    def row_copies(i):
        return [pltpu.make_async_copy(src.at[i], dst.at[i], row_sems.at[k, i]) for k, (src, dst) in enumerate(((hg_in, hg), (gg_in, gg)))]

    for i in range(2 * RING):
        for copy in row_copies(i):
            copy.start()
    if chain:
        weights.start(layer - 1, 0, 0)
        weights.start(layer - 1, 1, 1)
        pre_copy = pltpu.make_async_copy(pre_in[0], pre, pre_sem.at[0])
        pre_copy.start()
    meet(('x', 'y', 'z'))
    for move in moves:
        move.begin()
    work.ready()

    @pl.loop(0, 2 * RING)
    def _(i):
        for copy in row_copies(i):
            copy.wait()
        work.rows(hg, gg, i)

    work.multiply(hg, gg)
    for move in moves:
        move.middle()
    work.middle_one()
    if chain:
        pre_copy.wait()
        backward_layer(weights, layer - 1, 0, None, rows_in[0], pre, total, below[0])
    work.turn()
    for move in moves:
        move.late()
    work.finish_two()
    for i, move in enumerate(moves):
        move.finish()
        stores[i].start()
    work.drain()
    for i in range(gathers):
        stores[i].wait()


def layer_grads(layer, hg, gg, w_in, w_out, rows, pre):
    vmem, anywhere = pl.BlockSpec(memory_space=pltpu.VMEM), pl.BlockSpec(memory_space=pl.ANY)
    _, m, d = hg.shape
    full = w_in.shape[2]
    chain = pre is not None
    out_shape = [jax.ShapeDtypeStruct((full // (4 * RING), d // RING), F32)]
    out_shape += [jax.ShapeDtypeStruct((2 * RING,) + row.shape, row.dtype) for row in rows]
    scratch = [pltpu.VMEM(hg.shape, BF16)] * 2 + [pltpu.SemaphoreType.DMA((2, 2 * RING))]
    scratch += shard_scratch(2 * RING * m, d, full // (2 * RING))
    scratch += [pltpu.VMEM((2 * RING,) + row.shape, row.dtype) for row in rows]
    scratch += [pltpu.SemaphoreType.DMA((8,))] * (2 * len(rows))
    if rows:
        scratch += [pltpu.SemaphoreType.DMA((len(rows),))]
    if chain:
        out_shape.append(jax.ShapeDtypeStruct(rows[0].shape, BF16))
        scratch += stream_scratch(d, full)
        scratch += [pltpu.VMEM((m, full), BF16), pltpu.VMEM((m, d), F32), pltpu.SemaphoreType.DMA((1,))]
    return pl.pallas_call(
        functools.partial(layer_kernel, layer, len(rows), chain),
        out_shape=out_shape,
        in_specs=[anywhere] * 4 + [vmem] * len(rows) + [anywhere] * chain,
        out_specs=[vmem] + [anywhere] * len(rows) + [vmem] * chain,
        scratch_shapes=scratch,
        compiler_params=pltpu.CompilerParams(collective_id=layer, has_side_effects=True, vmem_limit_bytes=60 * MIB),
        cost_estimate=pl.CostEstimate(flops=30_000_000_000, bytes_accessed=16 * MIB, transcendentals=0),
        name='layer_grads',
    )(hg, gg, w_in, w_out, *rows, *([pre] if chain else []))


class BlockGather:
    def __init__(self, near, far, order, rows, sems, base):
        self.near, self.far = near, far
        self.order, self.rows, self.sems = order, rows, sems
        self.index = {axis: lax.axis_index(axis) for axis in 'xyz'}
        self.base, self.count = base, 0
        self.other = place('c', 1)
        self.copies, self.cross = {}, []

    def at(self, phase, which, half=None):
        picks, rows = {}, self.rows
        for k, axis in enumerate(self.order):
            picks[axis] = pl.ds(0, RING) if k < phase else self.index[axis]
        if phase < 3:
            picks[self.order[phase]] = which
        if half is not None:
            if phase == 0:
                cut = (rows[1] // 16) * 8
                rows = (rows[0], cut) if half == 0 else (rows[0] + cut, rows[1] - cut)
            else:
                picks[self.order[phase - 1]] = pl.ds(half * 2, 2)
        return tuple(picks[axis] for axis in ('z', 'y', 'x')) + (pl.ds(*rows),)

    def send(self, where, to, dst=None):
        dst = self.near if dst is None else dst
        copy = remote(self.near.at[where], dst.at[where], self.sems, self.base + self.count, to)
        self.count += 1
        copy.start()
        return copy

    def cross_over(self, where):
        self.cross.append((self.send(where, self.other, self.far), where))

    def begin(self, phase):
        axis = self.order[phase]
        me = self.index[axis]
        self.ends = (place(axis, 1), place(axis, -1))
        self.around = (lax.rem(me + 3, RING), lax.rem(me + 1, RING), lax.rem(me + 2, RING))
        whole = self.at(phase, me)
        self.near_copies = [self.send(whole, end) for end in self.ends]
        if phase == 2:
            self.cross_over(whole)

    def middle(self, phase):
        self.far_copies = []
        for side in range(2):
            self.near_copies[side].wait_recv()
            self.far_copies.append(self.send(self.at(phase, self.around[side], side), self.ends[side]))
            if phase == 2:
                self.cross_over(self.at(phase, self.around[side]))

    def finish(self, phase):
        for copy in self.far_copies:
            copy.wait_recv()
        for copy in self.near_copies + self.far_copies:
            self.copies[id(copy)] = copy
        if phase == 2:
            self.cross_over(self.at(phase, self.around[2]))

    def close(self):
        for copy, where in self.cross:
            copy.wait_recv()
        for copy in list(self.copies.values()) + [c for c, _ in self.cross]:
            copy.wait_send()


BLOCK_SEMS = 16


def block_gather_kernel(shard, out, send, recv):
    near, far = out.at[0], out.at[1]
    me = tuple(lax.axis_index(axis) for axis in ('z', 'y', 'x'))
    near[me] = shard[...]
    tiles = shard.shape[0] // 8
    cuts = [0, -(-tiles // 3), -(-2 * tiles // 3), tiles]
    meet(('x', 'y', 'z'))
    colors = [BlockGather(near, far, ORDERS[k], (8 * cuts[k], 8 * (cuts[k + 1] - cuts[k])), (send, recv), k * BLOCK_SEMS) for k in range(3)]
    for phase in range(3):
        for stage in ('begin', 'middle', 'finish'):
            for color in colors:
                getattr(color, stage)(phase)
    for color in colors:
        color.close()


def block_gather(shard, collective_id):
    vmem = pl.BlockSpec(memory_space=pltpu.VMEM)
    return pl.pallas_call(
        block_gather_kernel,
        out_shape=pltpu.VMEM((2, RING, RING, RING) + shard.shape, F32),
        in_specs=[vmem],
        out_specs=vmem,
        scratch_shapes=[pltpu.SemaphoreType.DMA((3 * BLOCK_SEMS,))] * 2,
        compiler_params=pltpu.CompilerParams(collective_id=collective_id, has_side_effects=True, vmem_limit_bytes=16 * MIB),
        cost_estimate=pl.CostEstimate(flops=60_000_000_000, bytes_accessed=32 * MIB, transcendentals=0),
        name='block_gather',
    )(shard)


def place_held_kernel(along, _, blocks, out_in, out_out):
    i, k = pl.program_id(0), pl.program_id(1)
    n, cols = blocks.shape[-2] // 2, blocks.shape[-1]
    for a in range(RING):
        for b in range(RING):
            at = [a, b]
            at.insert(along, i)
            block = blocks[(k,) + tuple(at)]
            out_in[a * cols : (a + 1) * cols, b * n : (b + 1) * n] = block[:n].T
            out_out[a * n : (a + 1) * n, b * cols : (b + 1) * cols] = block[n:]


def place_held(core, blocks, layer, layers):
    cols = blocks.shape[-1]
    n = cols // 2
    width, d = n * RING, cols * RING
    return pl.pallas_call(
        functools.partial(place_held_kernel, AXES.index(GROUPS[layer])),
        grid_spec=pltpu.PrefetchScalarGridSpec(
            num_scalar_prefetch=1,
            grid=(RING, 2),
            in_specs=[pl.BlockSpec(memory_space=pltpu.VMEM)],
            out_specs=[
                pl.BlockSpec((None, d, width), lambda i, k, s: (layer, 0, i * 2 + (s[0] + k) % 2)),
                pl.BlockSpec((None, width, d), lambda i, k, s: (layer, i * 2 + (s[0] + k) % 2, 0)),
            ],
        ),
        out_shape=[jax.ShapeDtypeStruct((layers, d, width * 2 * RING), F32), jax.ShapeDtypeStruct((layers, width * 2 * RING, d), F32)],
        compiler_params=pltpu.CompilerParams(vmem_limit_bytes=24 * MIB),
        cost_estimate=pl.CostEstimate(flops=10_000_000_000, bytes_accessed=32 * MIB, transcendentals=0),
        name='place_held',
    )(core, pltpu.with_memory_space_constraint(blocks, pltpu.VMEM))


def place_kernel(src_in, src_out, *refs):
    out_in, out_out = refs[-2:]
    n, cols = src_in.shape[-2:]
    for a in range(RING):
        for b in range(RING):
            out_in[a * cols : (a + 1) * cols, b * n : (b + 1) * n] = src_in[a, b].T
            out_out[a * n : (a + 1) * n, b * cols : (b + 1) * cols] = src_out[a, b]


def place_blocks(blocks, which, outs, layer, layers):
    cols = blocks.shape[-1]
    n = cols // 2
    width, d = n * RING, cols * RING
    shapes = [jax.ShapeDtypeStruct((layers, d, width * 2 * RING), F32), jax.ShapeDtypeStruct((layers, width * 2 * RING, d), F32)]
    along = AXES.index(GROUPS[layer])
    picked = tuple(None if k == along else RING for k in range(3))
    src_specs = [
        pl.BlockSpec(picked + (None, n, cols), functools.partial(lambda k, i, c: tuple(i if dim == along else 0 for dim in range(3)) + (c, 2 * which + k, 0), k))
        for k in range(2)
    ]
    return pl.pallas_call(
        place_kernel,
        grid=(RING, 2),
        in_specs=src_specs + [pl.BlockSpec(memory_space=pl.ANY)] * len(outs),
        out_specs=[
            pl.BlockSpec((None, d, width), lambda i, c: (layer, 0, i * 2 + c)),
            pl.BlockSpec((None, width, d), lambda i, c: (layer, i * 2 + c, 0)),
        ],
        out_shape=shapes,
        input_output_aliases={2 + k: k for k in range(len(outs))},
        compiler_params=pltpu.CompilerParams(vmem_limit_bytes=63 * MIB),
        cost_estimate=pl.CostEstimate(flops=10_000_000_000, bytes_accessed=64 * MIB, transcendentals=0),
        name='place_blocks',
    )(blocks, blocks, *outs)


def solution(mesh):
    mesh4 = Mesh(mesh.devices.reshape(RING, RING, RING, 2), AXES)

    def local_step(tok, tgt, w_in, w_out):
        layers = w_in.shape[0]
        shard, grad, *hg, gg, pre = first(tok, tgt, w_in, w_out, tok.shape[0] * mesh4.size, 2 * layers)
        shards, gathered = {}, {}
        for l in reversed(range(layers)):
            if l == 2:
                shard, gg, grad = layer_grads(l, hg[l], gg, w_in, w_out, [grad], pre)
            elif l == 1:
                shard, gg = layer_grads(l, hg[l], gg, w_in, w_out, [grad], None)
            elif l == 0:
                (shard,) = layer_grads(l, hg[l], gg, w_in, w_out, [], None)
            shards[l] = shard
            for part in GATHERED_TOGETHER:
                if part[-1] == l:
                    blocks = jnp.concatenate([shards[k] for k in part], axis=0)
                    full = lax.all_gather(blocks[None], AXES, axis=0, tiled=True)
                    gathered[part] = full.reshape((RING, RING, RING, 2) + blocks.shape)
        last = block_gather(shards[0], layers + 1)
        early, late = GATHERED_TOGETHER
        outs = place_held(lax.axis_index('c').astype(jnp.int32).reshape(1), last, 0, layers)
        gathered[early], *outs = lax.optimization_barrier((gathered[early], *outs))
        for i, l in enumerate(early):
            outs = place_blocks(gathered[early], i, outs, l, layers)
        blocks, *outs = lax.optimization_barrier((gathered[late], *outs))
        for i, l in enumerate(late):
            outs = place_blocks(blocks, i, outs, l, layers)
        return outs[0], outs[1]

    spec = P(AXES, None)
    return jax.shard_map(local_step, mesh=mesh4, in_specs=(spec, spec, P(), P()), out_specs=(P(), P()), check_vma=False)
```

```python
import functools

import jax
import jax.numpy as jnp
from jax import lax
from jax.experimental import pallas as pl
from jax.experimental.pallas import tpu as pltpu
from jax.sharding import Mesh
from jax.sharding import PartitionSpec as P

AXES = ('z', 'y', 'x', 'c')
RING = 4
GROUPS = ('z', 'z', 'x', 'x')
OTHERS = {'x': ('z', 'y'), 'y': ('z', 'x'), 'z': ('y', 'x')}
CHUNK = 512
SLOTS = 3
ORDERS = (('x', 'y', 'z'), ('y', 'z', 'x'), ('z', 'x', 'y'))
SHARES = {3: (7, 15, 10), 2: (11, 11, 10), 1: (14, 9, 9), 0: (11, 11, 10)}
F32, BF16 = jnp.float32, jnp.bfloat16
COL = (((1,), (1,)), ((), ()))
GELU_S = 0.7978845608028654
GELU_C = 0.044715
MESH_ID = pl.DeviceIdType.MESH
MIB = 1 << 20


def place(axis, step):
    coords = [lax.axis_index(name) for name in AXES]
    which = AXES.index(axis)
    size = 2 if axis == 'c' else RING
    coords[which] = lax.rem(coords[which] + (step + size), size)
    return tuple(coords)


def remote(src, dst, sems, index, to):
    return pltpu.make_async_remote_copy(src_ref=src, dst_ref=dst, send_sem=sems[0].at[index], recv_sem=sems[1].at[index], device_id=to, device_id_type=MESH_ID)


def meet(axes):
    barrier = pltpu.get_barrier_semaphore()
    neighbours = [(axis, step) for axis in axes for step in (1, -1)] + [('c', 1)]
    for axis, step in neighbours:
        pl.semaphore_signal(barrier, inc=1, device_id=place(axis, step), device_id_type=MESH_ID)
    pl.semaphore_wait(barrier, len(neighbours))


class RowGather:
    def __init__(self, src, out, sems, axis):
        right, left, other = place(axis, 1), place(axis, -1), place('c', 1)
        half = src.shape[0] // 2
        top, bottom = pl.ds(0, half), pl.ds(half, half)
        self.src, self.out, self.landed = src, out, set()
        self.own = [remote(src, out.at[1], sems, 0, right), remote(src, out.at[2], sems, 1, left), remote(src, out.at[4], sems, 2, other)]
        self.onward = [
            remote(out.at[1, top], out.at[3, top], sems, 3, right),
            remote(out.at[2, bottom], out.at[3, bottom], sems, 4, left),
            remote(out.at[1], out.at[5], sems, 5, other),
            remote(out.at[2], out.at[6], sems, 6, other),
            remote(out.at[3], out.at[7], sems, 7, other),
        ]
        self.brings = {1: self.own[:1], 2: self.own[1:2], 3: self.onward[:2], 4: self.own[2:], 5: self.onward[2:3], 6: self.onward[3:4], 7: self.onward[4:]}

    def arrive(self, *slots):
        for slot in slots:
            if slot and slot not in self.landed:
                self.landed.add(slot)
                for copy in self.brings[slot]:
                    copy.wait_recv()

    def begin(self):
        for copy in self.own:
            copy.start()
        self.out[0] = self.src[...]

    def middle(self):
        for side in range(2):
            self.arrive(1 + side)
            self.onward[side].start()
            self.onward[2 + side].start()

    def late(self):
        self.arrive(3)
        self.onward[4].start()

    def finish(self):
        self.arrive(4, 5, 6, 7)
        for copy in self.own + self.onward:
            copy.wait_send()


class RingSum:
    def __init__(self, parts, got, put, sems, axis):
        self.parts, self.got, self.put = parts, got, put
        self.me = lax.axis_index(axis)
        right, left = place(axis, 1), place(axis, -1)
        self.nxt, self.prv, self.opp = lax.rem(self.me + 1, RING), lax.rem(self.me + 3, RING), lax.rem(self.me + 2, RING)
        half = parts.shape[1] // 2
        self.top, self.bottom = pl.ds(0, half), pl.ds(half, half)
        self.first = [
            remote(parts.at[self.opp, self.top], got.at[0], sems, 0, right),
            remote(parts.at[self.opp, self.bottom], got.at[3], sems, 3, left),
            remote(parts.at[self.nxt, self.bottom], got.at[1], sems, 1, right),
            remote(parts.at[self.prv, self.top], got.at[4], sems, 4, left),
        ]
        self.second = [remote(got.at[0], got.at[2], sems, 2, right), remote(got.at[3], got.at[5], sems, 5, left)]

    def begin_far(self):
        self.first[0].start()
        self.first[1].start()

    def begin_near(self):
        self.first[2].start()
        self.first[3].start()

    def middle(self):
        self.first[0].wait_recv()
        self.got[0] = self.got[0] + self.parts[self.nxt, self.top]
        self.second[0].start()
        self.first[1].wait_recv()
        self.got[3] = self.got[3] + self.parts[self.prv, self.bottom]
        self.second[1].start()

    def finish(self):
        self.first[3].wait_recv()
        self.second[0].wait_recv()
        self.put(0, self.parts[self.me, self.top] + self.got[4] + self.got[2])
        self.first[2].wait_recv()
        self.second[1].wait_recv()
        self.put(1, self.parts[self.me, self.bottom] + self.got[1] + self.got[5])

    def drain(self):
        for copy in self.first + self.second:
            copy.wait_send()


def put_blocks(total, which, value):
    total[pl.ds(which * 2, 2)] = value.reshape((2,) + total.shape[1:])


def put_rows(total, offset, which, value):
    total[pl.ds(offset + which * value.shape[0], value.shape[0])] = value


def gelu_terms(x):
    square = x * x
    t = jnp.tanh(x * (GELU_S + GELU_S * GELU_C * square))
    cdf = 0.5 + 0.5 * t
    slope = cdf + (0.5 * x) * (1.0 - t * t) * (GELU_S + 3.0 * GELU_S * GELU_C * square)
    return x * cdf, slope


class Weights:
    def __init__(self, w_in, w_out, buf_in, buf_out, sems):
        self.w_in, self.w_out, self.buf_in, self.buf_out, self.sems = w_in, w_out, buf_in, buf_out, sems
        self.width = buf_in.shape[2]
        self.steps = w_in.shape[2] // self.width

    def copies(self, layer, chunk, slot):
        at = pl.ds(pl.multiple_of(chunk * self.width, self.width), self.width)
        return (
            pltpu.make_async_copy(self.w_in.at[layer, :, at], self.buf_in.at[slot], self.sems.at[0, slot]),
            pltpu.make_async_copy(self.w_out.at[layer, at, :], self.buf_out.at[slot], self.sems.at[1, slot]),
        )

    def start(self, layer, chunk, slot):
        for copy in self.copies(layer, chunk, slot):
            copy.start()

    def sweep(self, layer, base, following, body):
        def step(chunk, ahead):
            slot = lax.rem(base + chunk, SLOTS)
            for copy in self.copies(layer, chunk, slot):
                copy.wait()
            if ahead is not None:
                self.start(ahead[0], ahead[1], lax.rem(base + chunk + 2, SLOTS))
            body(chunk, self.buf_in.at[slot], self.buf_out.at[slot])

        @pl.loop(0, self.steps - 2)
        def _(chunk):
            step(chunk, (layer, chunk + 2))

        for last in range(2):
            step(self.steps - 2 + last, None if following is None else (following, last))


def forward_layer(weights, layer, base, following, hidden, pre, total, out):
    total[...] = jnp.zeros_like(total)
    half = weights.width // 2

    def body(chunk, wi, wo):
        posts = []
        for part in range(2):
            at = pl.ds(part * half, half)
            u = jnp.dot(hidden[...], wi[:, at], preferred_element_type=F32).astype(BF16)
            if pre is not None:
                pre[:, pl.ds(pl.multiple_of(chunk * weights.width + part * half, half), half)] = u
            posts.append(gelu_terms(u.astype(F32))[0].astype(BF16))
        for part in range(2):
            total[...] += jnp.dot(posts[part], wo[pl.ds(part * half, half)], preferred_element_type=F32)

    weights.sweep(layer, base, following, body)
    out[...] = (hidden[...].astype(F32) + total[...]).astype(BF16)


def backward_layer(weights, layer, base, following, grad, pre, total, out):
    total[...] = jnp.zeros_like(total)
    half = weights.width // 2

    def body(chunk, wi, wo):
        grads = []
        for part in range(2):
            e = lax.dot_general(grad[...], wo[pl.ds(part * half, half)], COL, preferred_element_type=F32)
            u = pre[:, pl.ds(pl.multiple_of(chunk * weights.width + part * half, half), half)]
            grads.append((e * gelu_terms(u.astype(F32))[1]).astype(BF16))
        for part in range(2):
            total[...] += lax.dot_general(grads[part], wi[:, pl.ds(part * half, half)], COL, preferred_element_type=F32)

    weights.sweep(layer, base, following, body)
    out[...] = (grad[...].astype(F32) + total[...]).astype(BF16)


class ShardWork:
    def __init__(self, layer, w_in, w_out, shard, take):
        group = GROUPS[layer]
        self.wi, self.wo, self.wi_t, self.act, self.slope, w_sems = take(6)
        self.stage_one, self.stage_two = [], []
        for color in range(2):
            one, two = OTHERS[group][color], OTHERS[group][1 - color]
            parts, got_one, mid, got_two, send_one, recv_one, send_two, recv_two = take(8)
            self.stage_one.append(RingSum(parts, got_one, functools.partial(put_blocks, mid), (send_one, recv_one), one))
            self.stage_two.append(RingSum(mid, got_two, functools.partial(put_rows, shard, color * mid.shape[1]), (send_two, recv_two), two))
        width = self.wi.shape[1]
        start = pl.multiple_of((lax.axis_index(group) * 2 + lax.axis_index('c')) * width, width)
        self.loads = [
            pltpu.make_async_copy(w_in.at[layer, :, pl.ds(start, width)], self.wi, w_sems.at[0]),
            pltpu.make_async_copy(w_out.at[layer, pl.ds(start, width), :], self.wo, w_sems.at[1]),
        ]

    def load(self):
        for load in self.loads:
            load.start()

    def ready(self):
        self.loads[0].wait()
        self.wi_t[...] = self.wi[...].T
        self.loads[1].wait()

    def rows(self, hg, gg, slot):
        n = hg.shape[1]
        at = pl.ds(pl.multiple_of(slot * n, n), n)
        u = lax.dot_general(self.wi_t[...], hg[slot], COL, preferred_element_type=F32).astype(BF16)
        e = lax.dot_general(self.wo[...], gg[slot], COL, preferred_element_type=F32)
        post, slope = gelu_terms(u.astype(F32))
        self.act[:, at] = post.astype(BF16)
        self.slope[:, at] = (e * slope).astype(BF16)

    def fill(self, color, which, hg, gg):
        cols = self.stage_one[color].parts.shape[2]
        at = pl.ds(pl.multiple_of(which * cols, cols), cols)
        left, right = (self.slope, hg) if color == 0 else (self.act, gg)
        self.stage_one[color].parts[which] = jnp.dot(left[...], right[:, :, at].reshape(-1, cols), preferred_element_type=F32)

    def multiply_far(self, hg, gg):
        for color in range(2):
            self.fill(color, self.stage_one[color].opp, hg, gg)
            self.stage_one[color].begin_far()

    def multiply_near(self, hg, gg):
        for color in range(2):
            self.fill(color, self.stage_one[color].nxt, hg, gg)
            self.fill(color, self.stage_one[color].prv, hg, gg)
            self.stage_one[color].begin_near()

    def multiply_own(self, hg, gg):
        for color in range(2):
            self.fill(color, self.stage_one[color].me, hg, gg)

    def middle_one(self):
        for stage in self.stage_one:
            stage.middle()

    def turn(self):
        for one, two in zip(self.stage_one, self.stage_two):
            one.finish()
            two.begin_far()
            two.begin_near()

    def middle_two(self):
        for stage in self.stage_two:
            stage.middle()

    def finish_two(self):
        for stage in self.stage_two:
            stage.finish()

    def drain(self):
        for stage in self.stage_one + self.stage_two:
            stage.drain()


def shard_scratch(tokens, d, width):
    cols, n = d // RING, width // RING
    scratch = [pltpu.VMEM((d, width), BF16), pltpu.VMEM((width, d), BF16), pltpu.VMEM((width, d), BF16)]
    scratch += [pltpu.VMEM((width, tokens), BF16)] * 2 + [pltpu.SemaphoreType.DMA((2,))]
    for _ in range(2):
        scratch += [pltpu.VMEM((RING, width, cols), F32), pltpu.VMEM((6, width // 2, cols), F32)]
        scratch += [pltpu.VMEM((RING, n, cols), F32), pltpu.VMEM((6, n // 2, cols), F32)]
        scratch += [pltpu.SemaphoreType.DMA((6,))] * 4
    return scratch


def stream_scratch(d, full):
    width = min(CHUNK, full // 4)
    return [pltpu.VMEM((SLOTS, d, width), BF16), pltpu.VMEM((SLOTS, width, d), BF16), pltpu.SemaphoreType.DMA((2, SLOTS))]


def first_kernel(scale, tok, tgt, w_in, w_out, *refs):
    refs = list(refs)
    take = lambda count: [refs.pop(0) for _ in range(count)]
    shard, below, below_next = take(3)
    gathered_out = take(4)
    buf_in, buf_out, w_sems, pre, total, hid, grads, keep_sems = take(8)
    landing = take(6)
    sems = [take(2) for _ in range(6)]
    layers = w_in.shape[0]
    top = layers - 1
    weights = Weights(w_in, w_out, buf_in, buf_out, w_sems)
    work = ShardWork(top, w_in, w_out, shard, take)
    weights.start(0, 0, 0)
    weights.start(0, 1, 1)
    work.load()
    meet(('x', 'y', 'z'))
    h0, h1 = RowGather(tok, landing[0], sems[0], GROUPS[0]), RowGather(hid.at[0], landing[1], sems[1], GROUPS[1])
    h3, g4 = RowGather(hid.at[2], landing[2], sems[2], GROUPS[3]), RowGather(grads.at[0], landing[3], sems[3], GROUPS[3])
    h2, g3 = RowGather(hid.at[1], landing[4], sems[4], GROUPS[2]), RowGather(grads.at[1], landing[5], sems[5], GROUPS[2])
    stores = [pltpu.make_async_copy(landing[k], gathered_out[i], keep_sems.at[i]) for i, k in enumerate((0, 1, 4, 5))]
    h = tok
    steps = weights.steps
    h0.begin()
    for l in range(layers):
        forward_layer(weights, l, l * steps, min(l + 1, top), h, pre.at[l - 1] if l else None, total, hid.at[l])
        h = hid.at[l]
        if l == 0:
            h1.begin()
        elif l == 1:
            h0.middle()
            work.ready()
        elif l == 2:
            h3.begin()
            h1.middle()
            h0.late()
    grads[0] = ((h[...].astype(F32) - tgt[...].astype(F32)) * scale).astype(BF16)
    g4.begin()
    backward_layer(weights, top, layers * steps, top - 1, grads.at[0], pre.at[top - 1], total, grads.at[1])
    hg, gg = landing[2], landing[3]
    work.rows(hg, gg, 0)
    h1.late()
    h0.finish()
    stores[0].start()
    h3.middle()
    h3.arrive(4)
    g4.arrive(4)
    work.rows(hg, gg, 4)
    h1.finish()
    stores[1].start()
    g4.middle()
    g3.begin()
    h2.begin()

    def pair(first):
        @pl.loop(first, first + 2)
        def _(slot):
            work.rows(hg, gg, slot)

    pair(1)
    h3.late()
    h3.arrive(5, 6)
    g4.arrive(5, 6)
    pair(5)
    g4.late()
    work.rows(hg, gg, 3)
    h3.arrive(7)
    g4.arrive(7)
    work.rows(hg, gg, 7)
    work.multiply_far(hg, gg)
    work.multiply_near(hg, gg)
    work.multiply_own(hg, gg)
    g3.middle()
    work.middle_one()
    backward_layer(weights, top - 1, (layers + 1) * steps, top - 2, grads.at[1], pre.at[top - 2], total, below)
    h2.middle()
    work.turn()
    backward_layer(weights, top - 2, (layers + 2) * steps, None, below, pre.at[top - 3], total, below_next)
    g3.late()
    work.middle_two()
    work.finish_two()
    h2.late()
    g3.finish()
    stores[3].start()
    h2.finish()
    stores[2].start()
    for move in (h3, g4):
        move.finish()
    work.drain()
    for store in stores:
        store.wait()


def first(tok, tgt, w_in, w_out, total_rows, collective_id):
    vmem, anywhere = pl.BlockSpec(memory_space=pltpu.VMEM), pl.BlockSpec(memory_space=pl.ANY)
    n, d = tok.shape
    layers, _, full = w_in.shape
    row = jax.ShapeDtypeStruct((n, d), BF16)
    group = (2 * RING, n, d)
    block = jax.ShapeDtypeStruct((full // (4 * RING), d // RING), F32)
    scratch = stream_scratch(d, full)
    scratch += [pltpu.VMEM((layers - 1, n, full), BF16), pltpu.VMEM((n, d), F32), pltpu.VMEM((layers, n, d), BF16), pltpu.VMEM((2, n, d), BF16)]
    scratch += [pltpu.SemaphoreType.DMA((4,))] + [pltpu.VMEM(group, BF16)] * 6 + [pltpu.SemaphoreType.DMA((8,))] * 12
    scratch += shard_scratch(2 * RING * n, d, full // (2 * RING))
    return pl.pallas_call(
        functools.partial(first_kernel, 1.0 / total_rows),
        out_shape=[block, row, row] + [jax.ShapeDtypeStruct(group, BF16)] * 4,
        in_specs=[vmem, vmem, anywhere, anywhere],
        out_specs=[vmem] * 3 + [anywhere] * 4,
        scratch_shapes=scratch,
        compiler_params=pltpu.CompilerParams(collective_id=collective_id, has_side_effects=True, vmem_limit_bytes=67_000_000),
        cost_estimate=pl.CostEstimate(flops=60_000_000_000, bytes_accessed=96 * MIB, transcendentals=0),
        name='first',
    )(tok, tgt, w_in, w_out)


def layer_kernel(layer, gathers, hg_in, gg_in, w_in, w_out, above, *refs):
    refs = list(refs)
    take = lambda count: [refs.pop(0) for _ in range(count)]
    rows_in = take(gathers)
    shard, blocks = take(2)
    rows_out = take(gathers)
    hg, gg, row_sems, block_send, block_recv = take(5)
    work = ShardWork(layer, w_in, w_out, shard, take)
    landing = take(gathers)
    moves = [RowGather(src, out, take(2), GROUPS[layer - 1]) for src, out in zip(rows_in, landing)]
    if gathers:
        (keep_sems,) = take(1)
        stores = [pltpu.make_async_copy(landing[i], rows_out[i], keep_sems.at[i]) for i in range(gathers)]
    work.load()

    def row_copies(i):
        return [pltpu.make_async_copy(src.at[i], dst.at[i], row_sems.at[k, i]) for k, (src, dst) in enumerate(((hg_in, hg), (gg_in, gg)))]

    for i in range(2 * RING):
        for copy in row_copies(i):
            copy.start()
    colors = block_gather_colors(above, blocks, (block_send, block_recv), SHARES[layer + 1])
    meet(('x', 'y', 'z'))
    run = lambda stage, phase: [getattr(color, stage)(phase) for color in colors]
    run('begin', 0)
    for move in moves:
        move.begin()
    work.ready()

    def quarter(first):
        @pl.loop(first, first + 2)
        def _(i):
            for copy in row_copies(i):
                copy.wait()
            work.rows(hg, gg, i)

    quarter(0)
    run('middle', 0)
    quarter(2)
    run('finish', 0)
    run('begin', 1)
    quarter(4)
    quarter(6)
    work.multiply_far(hg, gg)
    run('middle', 1)
    work.multiply_near(hg, gg)
    work.multiply_own(hg, gg)
    for move in moves:
        move.middle()
    run('finish', 1)
    work.middle_one()
    run('begin', 2)
    work.turn()
    for move in moves:
        move.late()
    work.middle_two()
    run('middle', 2)
    work.finish_two()
    for i, move in enumerate(moves):
        move.finish()
        stores[i].start()
    run('finish', 2)
    for color in colors:
        color.close()
    work.drain()
    for i in range(gathers):
        stores[i].wait()


def layer_grads(layer, hg, gg, w_in, w_out, rows, above):
    vmem, anywhere = pl.BlockSpec(memory_space=pltpu.VMEM), pl.BlockSpec(memory_space=pl.ANY)
    _, m, d = hg.shape
    full = w_in.shape[2]
    out_shape = [jax.ShapeDtypeStruct(above.shape, F32), pltpu.VMEM((2, RING, RING, RING) + above.shape, F32)]
    out_shape += [jax.ShapeDtypeStruct((2 * RING,) + row.shape, row.dtype) for row in rows]
    scratch = [pltpu.VMEM(hg.shape, BF16)] * 2 + [pltpu.SemaphoreType.DMA((2, 2 * RING))] + [pltpu.SemaphoreType.DMA((3 * BLOCK_SEMS,))] * 2
    scratch += shard_scratch(2 * RING * m, d, full // (2 * RING))
    scratch += [pltpu.VMEM((2 * RING,) + row.shape, row.dtype) for row in rows]
    scratch += [pltpu.SemaphoreType.DMA((8,))] * (2 * len(rows))
    if rows:
        scratch += [pltpu.SemaphoreType.DMA((len(rows),))]
    return pl.pallas_call(
        functools.partial(layer_kernel, layer, len(rows)),
        out_shape=out_shape,
        in_specs=[anywhere] * 4 + [vmem] * (1 + len(rows)),
        out_specs=[vmem, vmem] + [anywhere] * len(rows),
        scratch_shapes=scratch,
        compiler_params=pltpu.CompilerParams(collective_id=layer, has_side_effects=True, vmem_limit_bytes=32_900_000),
        cost_estimate=pl.CostEstimate(flops=30_000_000_000, bytes_accessed=16 * MIB, transcendentals=0),
        name='layer_grads',
    )(hg, gg, w_in, w_out, above, *rows)


class BlockGather:
    def __init__(self, near, far, order, rows, sems, base):
        self.near, self.far = near, far
        self.order, self.rows, self.sems = order, rows, sems
        self.index = {axis: lax.axis_index(axis) for axis in 'xyz'}
        self.base, self.count = base, 0
        self.other = place('c', 1)
        self.copies, self.cross = {}, []

    def at(self, phase, which, half=None):
        picks, rows = {}, self.rows
        for k, axis in enumerate(self.order):
            picks[axis] = pl.ds(0, RING) if k < phase else self.index[axis]
        if phase < 3:
            picks[self.order[phase]] = which
        if half is not None:
            if phase == 0:
                cut = (rows[1] // 16) * 8
                rows = (rows[0], cut) if half == 0 else (rows[0] + cut, rows[1] - cut)
            else:
                picks[self.order[phase - 1]] = pl.ds(half * 2, 2)
        return tuple(picks[axis] for axis in ('z', 'y', 'x')) + (pl.ds(*rows),)

    def send(self, where, to, dst=None):
        dst = self.near if dst is None else dst
        copy = remote(self.near.at[where], dst.at[where], self.sems, self.base + self.count, to)
        self.count += 1
        copy.start()
        return copy

    def cross_over(self, where):
        self.cross.append((self.send(where, self.other, self.far), where))

    def begin(self, phase):
        axis = self.order[phase]
        me = self.index[axis]
        self.ends = (place(axis, 1), place(axis, -1))
        self.around = (lax.rem(me + 3, RING), lax.rem(me + 1, RING), lax.rem(me + 2, RING))
        whole = self.at(phase, me)
        self.near_copies = [self.send(whole, end) for end in self.ends]
        if phase == 2:
            self.cross_over(whole)

    def middle(self, phase):
        self.far_copies = []
        for side in range(2):
            self.near_copies[side].wait_recv()
            self.far_copies.append(self.send(self.at(phase, self.around[side], side), self.ends[side]))
            if phase == 2:
                self.cross_over(self.at(phase, self.around[side]))

    def finish(self, phase):
        for copy in self.far_copies:
            copy.wait_recv()
        for copy in self.near_copies + self.far_copies:
            self.copies[id(copy)] = copy
        if phase == 2:
            self.cross_over(self.at(phase, self.around[2]))

    def close(self):
        for copy, where in self.cross:
            copy.wait_recv()
        for copy in list(self.copies.values()) + [c for c, _ in self.cross]:
            copy.wait_send()


BLOCK_SEMS = 16


def block_gather_colors(shard, out, sems, shares):
    near, far = out.at[0], out.at[1]
    me = tuple(lax.axis_index(axis) for axis in ('z', 'y', 'x'))
    near[me] = shard[...]
    starts = [8 * sum(shares[:k]) for k in range(3)]
    return [BlockGather(near, far, ORDERS[k], (starts[k], 8 * shares[k]), sems, k * BLOCK_SEMS) for k in range(3)]


def block_gather_kernel(shard, out, send, recv):
    colors = block_gather_colors(shard, out, (send, recv), SHARES[0])
    meet(('x', 'y', 'z'))
    for phase in range(3):
        for stage in ('begin', 'middle', 'finish'):
            for color in colors:
                getattr(color, stage)(phase)
    for color in colors:
        color.close()


def block_gather(shard, collective_id):
    vmem = pl.BlockSpec(memory_space=pltpu.VMEM)
    return pl.pallas_call(
        block_gather_kernel,
        out_shape=pltpu.VMEM((2, RING, RING, RING) + shard.shape, F32),
        in_specs=[vmem],
        out_specs=vmem,
        scratch_shapes=[pltpu.SemaphoreType.DMA((3 * BLOCK_SEMS,))] * 2,
        compiler_params=pltpu.CompilerParams(collective_id=collective_id, has_side_effects=True, vmem_limit_bytes=16 * MIB),
        cost_estimate=pl.CostEstimate(flops=60_000_000_000, bytes_accessed=32 * MIB, transcendentals=0),
        name='block_gather',
    )(shard)


def place_kernel(along, _, blocks, *refs):
    out_in, out_out = refs[-2:]
    i, k = pl.program_id(0), pl.program_id(1)
    n, cols = blocks.shape[-2] // 2, blocks.shape[-1]
    for a in range(RING):
        for b in range(RING):
            at = [a, b]
            at.insert(along, i)
            block = blocks[(k,) + tuple(at)]
            out_in[a * cols : (a + 1) * cols, b * n : (b + 1) * n] = block[:n].T
            out_out[a * n : (a + 1) * n, b * cols : (b + 1) * cols] = block[n:]


def place_blocks(core, blocks, outs, layer, layers):
    cols = blocks.shape[-1]
    n = cols // 2
    width, d = n * RING, cols * RING
    return pl.pallas_call(
        functools.partial(place_kernel, AXES.index(GROUPS[layer])),
        grid_spec=pltpu.PrefetchScalarGridSpec(
            num_scalar_prefetch=1,
            grid=(RING, 2),
            in_specs=[pl.BlockSpec(memory_space=pltpu.VMEM)] + [pl.BlockSpec(memory_space=pl.ANY)] * len(outs),
            out_specs=[
                pl.BlockSpec((None, d, width), lambda i, k, s: (layer, 0, i * 2 + (s[0] + k) % 2)),
                pl.BlockSpec((None, width, d), lambda i, k, s: (layer, i * 2 + (s[0] + k) % 2, 0)),
            ],
        ),
        out_shape=[jax.ShapeDtypeStruct((layers, d, width * 2 * RING), F32), jax.ShapeDtypeStruct((layers, width * 2 * RING, d), F32)],
        input_output_aliases={2 + k: k for k in range(len(outs))},
        compiler_params=pltpu.CompilerParams(vmem_limit_bytes=24 * MIB),
        cost_estimate=pl.CostEstimate(flops=10_000_000_000, bytes_accessed=32 * MIB, transcendentals=0),
        name='place_blocks',
    )(core, pltpu.with_memory_space_constraint(blocks, pltpu.VMEM), *outs)


def solution(mesh):
    mesh4 = Mesh(mesh.devices.reshape(RING, RING, RING, 2), AXES)

    def local_step(tok, tgt, w_in, w_out):
        layers = w_in.shape[0]
        core = lax.axis_index('c').astype(jnp.int32).reshape(1)
        above, *grads, h0, h1, h2, gg = first(tok, tgt, w_in, w_out, tok.shape[0] * mesh4.size, 2 * layers)
        hg = [h0, h1, h2]
        outs = []
        for l in reversed(range(layers - 1)):
            if outs:
                above, *outs = lax.optimization_barrier((above, *outs))
            shard, blocks, *rows = layer_grads(l, hg[l], gg, w_in, w_out, grads[:1] if l else [], above)
            outs = place_blocks(core, blocks, outs, l + 1, layers)
            above, grads = shard, grads[1:]
            gg = rows[0] if rows else None
        above, *outs = lax.optimization_barrier((above, *outs))
        outs = place_blocks(core, block_gather(above, layers + 1), outs, 0, layers)
        return outs[0], outs[1]

    spec = P(AXES, None)
    return jax.shard_map(local_step, mesh=mesh4, in_specs=(spec, spec, P(), P()), out_specs=(P(), P()), check_vma=False)
```

```python
import functools
import math

import jax
import jax.numpy as jnp
from jax import lax
from jax.experimental import pallas as pl
from jax.experimental.pallas import tpu as pltpu
from jax.sharding import Mesh
from jax.sharding import PartitionSpec as P

AXES = ('z', 'y', 'x', 'c')
RING = 4
GROUPS = ('z', 'z', 'x', 'x')
OTHERS = {'x': ('z', 'y'), 'y': ('z', 'x'), 'z': ('y', 'x')}
CHUNK = 512
SLOTS = 3
ORDERS = (('x', 'y', 'z'), ('y', 'z', 'x'), ('z', 'x', 'y'))
SHARES = {3: (6, 14, 12), 2: (12, 10, 10), 1: (14, 9, 9), 0: (10, 11, 11)}
SUM_PRIORITY = {2: 35, 1: 0, 0: 15}
F32, BF16 = jnp.float32, jnp.bfloat16
COL = (((1,), (1,)), ((), ()))
GELU_S = 0.7978845608028654
GELU_C = 0.044715
MESH_ID = pl.DeviceIdType.MESH
MIB = 1 << 20
HOP_US, CHIP_US = 2.0, 1.1
LINK_RATE, CHIP_RATE = 46.65e3, 600e3
ROW_SENDS, SUM_SENDS, BLOCK_SENDS = 10, 24, 123


def place(axis, step):
    coords = [lax.axis_index(name) for name in AXES]
    which = AXES.index(axis)
    size = 2 if axis == 'c' else RING
    coords[which] = lax.rem(coords[which] + (step + size), size)
    return tuple(coords)


def meet():
    barrier = pltpu.get_barrier_semaphore()
    neighbours = [(axis, step) for axis in 'xyz' for step in (1, -1)] + [('c', 1)]
    for axis, step in neighbours:
        pl.semaphore_signal(barrier, inc=1, device_id=place(axis, step), device_id_type=MESH_ID)
    pl.semaphore_wait(barrier, len(neighbours))


def around(axis):
    me = lax.axis_index(axis)
    return {'m': me, 'p': lax.rem(me + 3, RING), 'n': lax.rem(me + 1, RING), 'o': lax.rem(me + 2, RING)}


class Plan:
    def __init__(self, sems, backlog=2.0):
        self.sems, self.backlog, self.items, self.copies = sems, backlog, {}, {}

    def send(self, name, axis, step, src, dst, needs, priority):
        index = len(self.copies)
        self.copies[name] = pltpu.make_async_remote_copy(
            src_ref=src, dst_ref=dst, send_sem=self.sems[0].at[index], recv_sem=self.sems[1].at[index], device_id=place(axis, step), device_id_type=MESH_ID
        )
        size = math.prod(src.shape) * jnp.dtype(src.dtype).itemsize
        self.items[name] = ((axis, step), size, tuple(needs), priority)

    def work(self, name, cost, run, needs, priority):
        self.items[name] = (run, cost, tuple(needs), priority)

    def order(self, now):
        free, done, todo, order = {}, {}, dict(self.items), []
        while todo:
            due, soonest = None, math.inf
            for name, (what, size, needs, priority) in todo.items():
                if any(need not in done for need in needs):
                    continue
                when = max([done[need] for need in needs], default=0.0)
                if name in self.copies:
                    when = max(when, free.get(what, 0.0) - self.backlog)
                if when <= now + 1e-9:
                    key = (name not in self.copies, priority)
                    due = min(due, (key, len(order), name), key=lambda d: d[0]) if due else (key, len(order), name)
                soonest = min(soonest, when)
            if due is None:
                now = max(now, soonest)
                continue
            name = due[2]
            what, size, _, _ = todo.pop(name)
            order.append(name)
            if name in self.copies:
                inside = what[0] == 'c'
                free[what] = max(now, free.get(what, 0.0)) + size / (CHIP_RATE if inside else LINK_RATE)
                done[name] = free[what] + (CHIP_US if inside else HOP_US)
                now += 0.03
            else:
                now += size
                done[name] = now
        return order

    def run(self, start=3.0):
        landed = set()

        def arrive(name):
            if name in self.copies and name not in landed:
                landed.add(name)
                self.copies[name].wait_recv()

        for name in self.order(start):
            what, _, needs, _ = self.items[name]
            for need in needs:
                arrive(need)
            if name in self.copies:
                self.copies[name].start()
            else:
                what()
        for name, copy in self.copies.items():
            arrive(name)
            copy.wait_send()


def plan_rows(plan, key, out, axis, after, priority):
    half = out.shape[1] // 2
    top, bottom = pl.ds(0, half), pl.ds(half, half)

    def send(name, axis, step, src, dst, needs, late=0):
        plan.send((key,) + name, axis, step, out.at[src], out.at[dst], needs, priority + late)
        return (key,) + name

    right_top = send(('own', 'right', 'top'), axis, 1, (0, top), (1, top), after)
    left_bottom = send(('own', 'left', 'bottom'), axis, -1, (0, bottom), (2, bottom), after)
    right_bottom = send(('own', 'right', 'bottom'), axis, 1, (0, bottom), (1, bottom), after, 2)
    left_top = send(('own', 'left', 'top'), axis, -1, (0, top), (2, top), after, 2)
    ahead = send(('on', 'right'), axis, 1, (1, top), (3, top), [right_top], 1)
    behind = send(('on', 'left'), axis, -1, (2, bottom), (3, bottom), [left_bottom], 1)
    slots = [list(after), [right_top, right_bottom], [left_top, left_bottom], [ahead, behind]]
    return slots + [[send(('core', slot), 'c', 1, (slot,), (4 + slot,), slots[slot])] for slot in range(4)]


def plan_sums(plan, key, parts, filled, got, put, axis, after, costs, priority):
    at = around(axis)
    half = parts.shape[1] // 2
    top, bottom = pl.ds(0, half), pl.ds(half, half)
    send = lambda name, step, src, dst, needs, late: plan.send((key, name), axis, step, src, got.at[dst], list(after) + needs, priority + late)
    send('far right', 1, parts.at[at['o'], top], 0, filled['o'], 0)
    send('far left', -1, parts.at[at['o'], bottom], 3, filled['o'], 0)
    send('near right', 1, parts.at[at['n'], bottom], 1, filled['n'], 3)
    send('near left', -1, parts.at[at['p'], top], 4, filled['p'], 3)

    def add(slot, which, rows):
        got[slot] = got[slot] + parts[at[which], rows]

    plan.work((key, 'add right'), costs[0], lambda: add(0, 'n', top), [(key, 'far right')] + filled['n'], 1)
    plan.work((key, 'add left'), costs[0], lambda: add(3, 'p', bottom), [(key, 'far left')] + filled['p'], 1)
    send('on right', 1, got.at[0], 2, [(key, 'add right')], 1)
    send('on left', -1, got.at[3], 5, [(key, 'add left')], 1)

    def total(which, rows, one, two):
        put(which, parts[at['m'], rows] + got[one] + got[two])

    plan.work((key, 'sum 0'), costs[1], lambda: total(0, top, 4, 2), [(key, 'near left'), (key, 'on right')] + filled['m'], 2)
    plan.work((key, 'sum 1'), costs[1], lambda: total(1, bottom, 1, 5), [(key, 'near right'), (key, 'on left')] + filled['m'], 2)
    return [(key, 'sum 0'), (key, 'sum 1')]


def put_blocks(total, which, value):
    total[pl.ds(which * 2, 2)] = value.reshape((2,) + total.shape[1:])


def put_rows(total, offset, which, value):
    total[pl.ds(offset + which * value.shape[0], value.shape[0])] = value


def plan_blocks(plan, key, out, order, rows, after):
    near, far = out.at[0], out.at[1]
    at = {axis: around(axis) for axis in order}
    every = pl.ds(0, RING)
    onward = {'m': 1, 'o': 1, 'p': -1, 'n': -1}

    def where(picks, part=rows):
        chosen = dict(zip(order, picks))
        return tuple(every if chosen[axis] == 'all' else at[axis][chosen[axis]] for axis in ('z', 'y', 'x')) + (pl.ds(*part),)

    def send(name, axis, step, picks, needs, priority, part=rows, dst=near):
        spot = where(picks, part)
        plan.send((key,) + name, axis, step, near.at[spot], dst.at[spot], needs, priority)
        return [(key,) + name]

    cut = (rows[1] // 16) * 8
    halves = (rows[0], cut), (rows[0] + cut, rows[1] - cut)
    ready = {'m': list(after)}
    for side, step, half in (('p', 1, 0), ('n', -1, 1)):
        ready[side] = send((1, 'own', side), order[0], step, 'mmm', after, 10)
    ready['o'] = []
    for side, step, half in (('p', 1, 0), ('n', -1, 1)):
        ready['o'] = ready['o'] + send((1, 'on', side), order[0], step, (side, 'm', 'm'), ready[side], 9, halves[half])
    for phase in (2, 3):
        spread = {'m': sum([ready[i] for i in 'mpno'], []), 'p': [], 'n': [], 'o': []}
        arrived = {}
        for i in 'mpno':
            picks = {side: (i, side, 'm') if phase == 2 else ('all', i, side) for side in 'mpno'}
            for side, step in (('p', 1), ('n', -1)):
                first = onward[i] == step
                arrived[i, side] = send((phase, 'own', side, i), order[phase - 1], step, picks['m'], ready[i], (12 if first else 14) if phase == 2 else (30 if first else 50))
            side = 'p' if onward[i] == 1 else 'n'
            arrived[i, 'o'] = send((phase, 'on', side, i), order[phase - 1], onward[i], picks[side], arrived[i, side], 11 if phase == 2 else 40)
            for side in 'pno':
                spread[side] = spread[side] + arrived[i, side]
                if phase == 3:
                    send(('core', side, i), 'c', 1, picks[side], arrived[i, side], 60, dst=far)
        if phase == 2:
            ready = spread
            send(('core', 'm'), 'c', 1, ('all', 'all', 'm'), sum([ready[i] for i in 'mpno'], []), 60, dst=far)


def gelu_terms(x):
    square = x * x
    t = jnp.tanh(x * (GELU_S + GELU_S * GELU_C * square))
    cdf = 0.5 + 0.5 * t
    slope = cdf + (0.5 * x) * (1.0 - t * t) * (GELU_S + 3.0 * GELU_S * GELU_C * square)
    return x * cdf, slope


class Weights:
    def __init__(self, w_in, w_out, buf_in, buf_out, sems):
        self.w_in, self.w_out, self.buf_in, self.buf_out, self.sems = w_in, w_out, buf_in, buf_out, sems
        self.width = buf_in.shape[2]
        self.steps = w_in.shape[2] // self.width

    def copies(self, layer, chunk, slot):
        at = pl.ds(pl.multiple_of(chunk * self.width, self.width), self.width)
        return (
            pltpu.make_async_copy(self.w_in.at[layer, :, at], self.buf_in.at[slot], self.sems.at[0, slot]),
            pltpu.make_async_copy(self.w_out.at[layer, at, :], self.buf_out.at[slot], self.sems.at[1, slot]),
        )

    def start(self, layer, chunk, slot):
        for copy in self.copies(layer, chunk, slot):
            copy.start()

    def sweep(self, layer, base, following, body):
        def step(chunk, ahead):
            slot = lax.rem(base + chunk, SLOTS)
            for copy in self.copies(layer, chunk, slot):
                copy.wait()
            if ahead is not None:
                self.start(ahead[0], ahead[1], lax.rem(base + chunk + 2, SLOTS))
            body(chunk, self.buf_in.at[slot], self.buf_out.at[slot])

        def loop(first, last):
            @pl.loop(first, last)
            def _(chunk):
                step(chunk, (layer, chunk + 2))

        def end():
            loop(self.steps // 2, self.steps - 2)
            for last in range(2):
                step(self.steps - 2 + last, None if following is None else (following, last))

        return lambda: loop(0, self.steps // 2), end


def forward_layer(weights, layer, base, following, hidden, pre, total, out):
    half = weights.width // 2

    def body(chunk, wi, wo):
        posts = []
        for part in range(2):
            at = pl.ds(part * half, half)
            u = jnp.dot(hidden[...], wi[:, at], preferred_element_type=F32).astype(BF16)
            if pre is not None:
                pre[:, pl.ds(pl.multiple_of(chunk * weights.width + part * half, half), half)] = u
            posts.append(gelu_terms(u.astype(F32))[0].astype(BF16))
        for part in range(2):
            total[...] += jnp.dot(posts[part], wo[pl.ds(part * half, half)], preferred_element_type=F32)

    begin, end = weights.sweep(layer, base, following, body)

    def run():
        total[...] = jnp.zeros_like(total)
        begin()
        end()
        out((hidden[...].astype(F32) + total[...]).astype(BF16))

    return run


def backward_layer(weights, layer, base, following, grad, pre, total, out):
    half = weights.width // 2

    def body(chunk, wi, wo):
        grads = []
        for part in range(2):
            e = lax.dot_general(grad[...], wo[pl.ds(part * half, half)], COL, preferred_element_type=F32)
            u = pre[:, pl.ds(pl.multiple_of(chunk * weights.width + part * half, half), half)]
            grads.append((e * gelu_terms(u.astype(F32))[1]).astype(BF16))
        for part in range(2):
            total[...] += lax.dot_general(grads[part], wi[:, pl.ds(part * half, half)], COL, preferred_element_type=F32)

    begin, end = weights.sweep(layer, base, following, body)

    def first_piece():
        total[...] = jnp.zeros_like(total)
        begin()

    def second_piece():
        end()
        out[...] = (grad[...].astype(F32) + total[...]).astype(BF16)

    return first_piece, second_piece


class ShardWork:
    def __init__(self, layer, w_in, w_out, shard, take):
        self.group, self.shard = GROUPS[layer], shard
        self.wi, self.wo, self.wi_t, self.act, self.slope, w_sems = take(6)
        self.buffers = [take(4), take(4)]
        width = self.wi.shape[1]
        start = pl.multiple_of((lax.axis_index(self.group) * 2 + lax.axis_index('c')) * width, width)
        self.loads = [
            pltpu.make_async_copy(w_in.at[layer, :, pl.ds(start, width)], self.wi, w_sems.at[0]),
            pltpu.make_async_copy(w_out.at[layer, pl.ds(start, width), :], self.wo, w_sems.at[1]),
        ]

    def load(self):
        for load in self.loads:
            load.start()

    def ready(self):
        self.loads[0].wait()
        self.wi_t[...] = self.wi[...].T
        self.loads[1].wait()

    def rows(self, hg, gg, slot):
        n = hg.shape[1]
        at = pl.ds(pl.multiple_of(slot * n, n), n)
        u = lax.dot_general(self.wi_t[...], hg[slot], COL, preferred_element_type=F32).astype(BF16)
        e = lax.dot_general(self.wo[...], gg[slot], COL, preferred_element_type=F32)
        post, slope = gelu_terms(u.astype(F32))
        self.act[:, at] = post.astype(BF16)
        self.slope[:, at] = (e * slope).astype(BF16)

    def fill(self, color, which, hg, gg):
        parts = self.buffers[color][0]
        cols = parts.shape[2]
        at = pl.ds(pl.multiple_of(which * cols, cols), cols)
        left, right = (self.slope, hg) if color == 0 else (self.act, gg)
        parts[which] = jnp.dot(left[...], right[:, :, at].reshape(-1, cols), preferred_element_type=F32)

    def plan(self, plan, hg, gg, ready, priority):
        for color in range(2):
            parts, got_one, mid, got_two = self.buffers[color]
            one, two = OTHERS[self.group][color], OTHERS[self.group][1 - color]
            at = around(one)
            filled = {}
            for rank, which in enumerate('onpm'):
                filled[which] = [('fill', color, which)]
                plan.work(filled[which][0], 0.7, functools.partial(self.fill, color, at[which], hg, gg), ready, (10, 21, 22, 40)[rank] + 0.5 * color)
            sums = plan_sums(plan, ('sum', 1, color), parts, filled, got_one, functools.partial(put_blocks, mid), one, [], (0.12, 0.15), priority)
            filled = dict.fromkeys('mpno', sums)
            put = functools.partial(put_rows, self.shard, color * mid.shape[1])
            plan_sums(plan, ('sum', 2, color), mid, filled, got_two, put, two, [], (0.05, 0.05), priority - 4)


def shard_scratch(tokens, d, width):
    cols, n = d // RING, width // RING
    scratch = [pltpu.VMEM((d, width), BF16), pltpu.VMEM((width, d), BF16), pltpu.VMEM((width, d), BF16)]
    scratch += [pltpu.VMEM((width, tokens), BF16)] * 2 + [pltpu.SemaphoreType.DMA((2,))]
    for _ in range(2):
        scratch += [pltpu.VMEM((RING, width, cols), F32), pltpu.VMEM((6, width // 2, cols), F32)]
        scratch += [pltpu.VMEM((RING, n, cols), F32), pltpu.VMEM((6, n // 2, cols), F32)]
    return scratch


def send_sems(count):
    return [pltpu.SemaphoreType.DMA((count,))] * 2


def stream_scratch(d, full):
    width = min(CHUNK, full // 4)
    return [pltpu.VMEM((SLOTS, d, width), BF16), pltpu.VMEM((SLOTS, width, d), BF16), pltpu.SemaphoreType.DMA((2, SLOTS))]


def first_kernel(scale, tok, tgt, w_in, w_out, *refs):
    refs = list(refs)
    take = lambda count: [refs.pop(0) for _ in range(count)]
    shard, below, below_next = take(3)
    gathered_out = take(4)
    buf_in, buf_out, w_sems, pre, total, keep_sems = take(6)
    h0, h1, h2, h3, g4, g3 = take(6)
    sems = take(2)
    layers = w_in.shape[0]
    top = layers - 1
    weights = Weights(w_in, w_out, buf_in, buf_out, w_sems)
    work = ShardWork(top, w_in, w_out, shard, take)
    weights.start(0, 0, 0)
    weights.start(0, 1, 1)
    work.load()
    h0[0] = tok[...]
    meet()
    plan = Plan(sems)
    stores = [pltpu.make_async_copy(src, dst, keep_sems.at[i]) for i, (src, dst) in enumerate(zip((h0, h1, h2, g3), gathered_out))]

    def to(ref):
        def out(value):
            ref[0] = value

        return out

    def last(value):
        g4[0] = ((value.astype(F32) - tgt[...].astype(F32)) * scale).astype(BF16)

    steps = weights.steps
    hiddens, outs = [tok, h1.at[0], h2.at[0], h3.at[0]], [to(h1), to(h2), to(h3), last]
    for l in range(layers):
        run = forward_layer(weights, l, l * steps, min(l + 1, top), hiddens[l], pre.at[l - 1] if l else None, total, outs[l])
        plan.work(('forward', l), 5.5, run, [('forward', l - 1)] if l else [], 1)
    plan.work('ready', 1.0, work.ready, [('forward', 1)], 3)
    done = ('forward', top)
    for i, (l, grad, out) in enumerate(((top, g4.at[0], g3.at[0]), (top - 1, g3.at[0], below), (top - 2, below, below_next))):
        pieces = backward_layer(weights, l, (layers + i) * steps, l - 1 if i < 2 else None, grad, pre.at[l - 1], total, out)
        for k, piece in enumerate(pieces):
            plan.work(('backward', l, k), 3.2, piece, [done], (6, 45, 46)[i])
            done = ('backward', l, k)
    kept = [
        plan_rows(plan, 'h0', h0, GROUPS[0], [], 22),
        plan_rows(plan, 'h1', h1, GROUPS[1], [('forward', 0)], 22),
        plan_rows(plan, 'h2', h2, GROUPS[2], [('forward', 1)], 10),
        plan_rows(plan, 'g3', g3, GROUPS[2], [('backward', top, 1)], 30),
    ]
    for i, slots in enumerate(kept):
        plan.work(('store', i), 0.02, stores[i].start, sum(slots, []), 50)
    h3_slots = plan_rows(plan, 'h3', h3, GROUPS[top], [('forward', top - 1)], 0)
    g4_slots = plan_rows(plan, 'g4', g4, GROUPS[top], [('forward', top)], 5)
    for slot in range(2 * RING):
        plan.work(('rows', slot), 0.75, functools.partial(work.rows, h3, g4, slot), ['ready'] + h3_slots[slot] + g4_slots[slot], 5)
    work.plan(plan, h3, g4, [('rows', slot) for slot in range(2 * RING)], -10)
    plan.run()
    for store in stores:
        store.wait()


def first(tok, tgt, w_in, w_out, total_rows, collective_id):
    vmem, anywhere = pl.BlockSpec(memory_space=pltpu.VMEM), pl.BlockSpec(memory_space=pl.ANY)
    n, d = tok.shape
    layers, _, full = w_in.shape
    row = jax.ShapeDtypeStruct((n, d), BF16)
    group = (2 * RING, n, d)
    block = jax.ShapeDtypeStruct((full // (4 * RING), d // RING), F32)
    scratch = stream_scratch(d, full)
    scratch += [pltpu.VMEM((layers - 1, n, full), BF16), pltpu.VMEM((n, d), F32)]
    scratch += [pltpu.SemaphoreType.DMA((4,))] + [pltpu.VMEM(group, BF16)] * 6 + send_sems(6 * ROW_SENDS + SUM_SENDS)
    scratch += shard_scratch(2 * RING * n, d, full // (2 * RING))
    return pl.pallas_call(
        functools.partial(first_kernel, 1.0 / total_rows),
        out_shape=[block, row, row] + [jax.ShapeDtypeStruct(group, BF16)] * 4,
        in_specs=[vmem, vmem, anywhere, anywhere],
        out_specs=[vmem] * 3 + [anywhere] * 4,
        scratch_shapes=scratch,
        compiler_params=pltpu.CompilerParams(collective_id=collective_id, has_side_effects=True, vmem_limit_bytes=67_000_000),
        cost_estimate=pl.CostEstimate(flops=60_000_000_000, bytes_accessed=96 * MIB, transcendentals=0),
        name='first',
    )(tok, tgt, w_in, w_out)


def layer_kernel(layer, gathers, hg_in, gg_in, w_in, w_out, above, *refs):
    refs = list(refs)
    take = lambda count: [refs.pop(0) for _ in range(count)]
    rows_in = take(gathers)
    shard, blocks = take(2)
    rows_out = take(gathers)
    hg, gg, row_sems = take(3)
    sems = take(2)
    work = ShardWork(layer, w_in, w_out, shard, take)
    landing = take(gathers)
    if gathers:
        (keep_sems,) = take(1)
    work.load()

    def row_copies(i):
        return [pltpu.make_async_copy(src.at[i], dst.at[i], row_sems.at[k, i]) for k, (src, dst) in enumerate(((hg_in, hg), (gg_in, gg)))]

    for i in range(2 * RING):
        for copy in row_copies(i):
            copy.start()
    for src, out in zip(rows_in, landing):
        out[0] = src[...]
    hold_block(above, blocks)
    meet()
    plan = Plan(sems)
    plan.work('ready', 1.0, work.ready, [], 5)

    def quarter(first):
        @pl.loop(first, first + 2)
        def _(i):
            for copy in row_copies(i):
                copy.wait()
            work.rows(hg, gg, i)

    for i in range(RING):
        plan.work(('rows', i), 1.5, functools.partial(quarter, 2 * i), ['ready'], 6)
    plan_all_blocks(plan, blocks, SHARES[layer + 1])
    stores = []
    for i in range(gathers):
        slots = plan_rows(plan, ('rows in', i), landing[i], GROUPS[layer - 1], [], 20)
        stores.append(pltpu.make_async_copy(landing[i], rows_out[i], keep_sems.at[i]))
        plan.work(('store', i), 0.02, stores[i].start, sum(slots, []), 50)
    work.plan(plan, hg, gg, [('rows', i) for i in range(RING)], SUM_PRIORITY[layer])
    plan.run()
    for store in stores:
        store.wait()


def layer_grads(layer, hg, gg, w_in, w_out, rows, above):
    vmem, anywhere = pl.BlockSpec(memory_space=pltpu.VMEM), pl.BlockSpec(memory_space=pl.ANY)
    _, m, d = hg.shape
    full = w_in.shape[2]
    out_shape = [jax.ShapeDtypeStruct(above.shape, F32), pltpu.VMEM((2, RING, RING, RING) + above.shape, F32)]
    out_shape += [jax.ShapeDtypeStruct((2 * RING,) + row.shape, row.dtype) for row in rows]
    scratch = [pltpu.VMEM(hg.shape, BF16)] * 2 + [pltpu.SemaphoreType.DMA((2, 2 * RING))]
    scratch += send_sems(BLOCK_SENDS + SUM_SENDS + len(rows) * ROW_SENDS)
    scratch += shard_scratch(2 * RING * m, d, full // (2 * RING))
    scratch += [pltpu.VMEM((2 * RING,) + row.shape, row.dtype) for row in rows]
    if rows:
        scratch += [pltpu.SemaphoreType.DMA((len(rows),))]
    return pl.pallas_call(
        functools.partial(layer_kernel, layer, len(rows)),
        out_shape=out_shape,
        in_specs=[anywhere] * 4 + [vmem] * (1 + len(rows)),
        out_specs=[vmem, vmem] + [anywhere] * len(rows),
        scratch_shapes=scratch,
        compiler_params=pltpu.CompilerParams(collective_id=layer, has_side_effects=True, vmem_limit_bytes=32_900_000),
        cost_estimate=pl.CostEstimate(flops=30_000_000_000, bytes_accessed=16 * MIB, transcendentals=0),
        name='layer_grads',
    )(hg, gg, w_in, w_out, above, *rows)


def hold_block(shard, out):
    out[(0,) + tuple(lax.axis_index(axis) for axis in ('z', 'y', 'x'))] = shard[...]


def plan_all_blocks(plan, out, shares):
    unit = out.shape[-2] // sum(shares)
    for k, order in enumerate(ORDERS):
        plan_blocks(plan, ('blocks', k), out, order, (unit * sum(shares[:k]), unit * shares[k]), [])


def block_gather_kernel(shard, out, send, recv):
    hold_block(shard, out)
    meet()
    plan = Plan((send, recv))
    plan_all_blocks(plan, out, SHARES[0])
    plan.run()


def block_gather(shard, collective_id):
    vmem = pl.BlockSpec(memory_space=pltpu.VMEM)
    return pl.pallas_call(
        block_gather_kernel,
        out_shape=pltpu.VMEM((2, RING, RING, RING) + shard.shape, F32),
        in_specs=[vmem],
        out_specs=vmem,
        scratch_shapes=send_sems(BLOCK_SENDS),
        compiler_params=pltpu.CompilerParams(collective_id=collective_id, has_side_effects=True, vmem_limit_bytes=16 * MIB),
        cost_estimate=pl.CostEstimate(flops=60_000_000_000, bytes_accessed=32 * MIB, transcendentals=0),
        name='block_gather',
    )(shard)


def place_kernel(along, _, blocks, *refs):
    out_in, out_out = refs[-2:]
    i, k = pl.program_id(0), pl.program_id(1)
    n, cols = blocks.shape[-2] // 2, blocks.shape[-1]
    for a in range(RING):
        for b in range(RING):
            at = [a, b]
            at.insert(along, i)
            block = blocks[(k,) + tuple(at)]
            out_in[a * cols : (a + 1) * cols, b * n : (b + 1) * n] = block[:n].T
            out_out[a * n : (a + 1) * n, b * cols : (b + 1) * cols] = block[n:]


def place_blocks(core, blocks, outs, layer, layers):
    cols = blocks.shape[-1]
    n = cols // 2
    width, d = n * RING, cols * RING
    return pl.pallas_call(
        functools.partial(place_kernel, AXES.index(GROUPS[layer])),
        grid_spec=pltpu.PrefetchScalarGridSpec(
            num_scalar_prefetch=1,
            grid=(RING, 2),
            in_specs=[pl.BlockSpec(memory_space=pltpu.VMEM)] + [pl.BlockSpec(memory_space=pl.ANY)] * len(outs),
            out_specs=[
                pl.BlockSpec((None, d, width), lambda i, k, s: (layer, 0, i * 2 + (s[0] + k) % 2)),
                pl.BlockSpec((None, width, d), lambda i, k, s: (layer, i * 2 + (s[0] + k) % 2, 0)),
            ],
        ),
        out_shape=[jax.ShapeDtypeStruct((layers, d, width * 2 * RING), F32), jax.ShapeDtypeStruct((layers, width * 2 * RING, d), F32)],
        input_output_aliases={2 + k: k for k in range(len(outs))},
        compiler_params=pltpu.CompilerParams(vmem_limit_bytes=24 * MIB),
        cost_estimate=pl.CostEstimate(flops=10_000_000_000, bytes_accessed=32 * MIB, transcendentals=0),
        name='place_blocks',
    )(core, pltpu.with_memory_space_constraint(blocks, pltpu.VMEM), *outs)


def solution(mesh):
    mesh4 = Mesh(mesh.devices.reshape(RING, RING, RING, 2), AXES)

    def local_step(tok, tgt, w_in, w_out):
        layers = w_in.shape[0]
        core = lax.axis_index('c').astype(jnp.int32).reshape(1)
        above, *grads, h0, h1, h2, gg = first(tok, tgt, w_in, w_out, tok.shape[0] * mesh4.size, 2 * layers)
        hg = [h0, h1, h2]
        outs = []
        for l in reversed(range(layers - 1)):
            if outs:
                above, *outs = lax.optimization_barrier((above, *outs))
            shard, blocks, *rows = layer_grads(l, hg[l], gg, w_in, w_out, grads[:1] if l else [], above)
            outs = place_blocks(core, blocks, outs, l + 1, layers)
            above, grads = shard, grads[1:]
            gg = rows[0] if rows else None
        above, *outs = lax.optimization_barrier((above, *outs))
        outs = place_blocks(core, block_gather(above, layers + 1), outs, 0, layers)
        return outs[0], outs[1]

    spec = P(AXES, None)
    return jax.shard_map(local_step, mesh=mesh4, in_specs=(spec, spec, P(), P()), out_specs=(P(), P()), check_vma=False)
```

```python
import functools
import math

import jax
import jax.numpy as jnp
from jax import lax
from jax.experimental import pallas as pl
from jax.experimental.pallas import tpu as pltpu
from jax.sharding import Mesh
from jax.sharding import PartitionSpec as P

AXES = ('z', 'y', 'x', 'c')
RING = 4
GROUPS = ('x', 'z', 'y', 'x')
OTHERS = {'x': ('z', 'y'), 'y': ('z', 'x'), 'z': ('y', 'x')}
CHUNK = 512
SLOTS = 4
ORDERS = (('x', 'y', 'z'), ('y', 'z', 'x'), ('z', 'x', 'y'))
SHARES = {3: (10, 8, 14), 2: (14, 10, 8), 1: (8, 14, 10), 0: (10, 11, 11)}
F32, BF16 = jnp.float32, jnp.bfloat16
COL = (((1,), (1,)), ((), ()))
GELU_S = 0.7978845608028654
GELU_C = 0.044715
MESH_ID = pl.DeviceIdType.MESH
MIB = 1 << 20
HOP_US, CHIP_US = 2.0, 1.1
LINK_RATE, CHIP_RATE = 45.7e3, 600e3
ROW_SENDS, SUM_SENDS, BLOCK_SENDS = 10, 24, 123


def place(axis, step):
    coords = [lax.axis_index(name) for name in AXES]
    which = AXES.index(axis)
    size = 2 if axis == 'c' else RING
    coords[which] = lax.rem(coords[which] + (step + size), size)
    return tuple(coords)


def meet():
    barrier = pltpu.get_barrier_semaphore()
    neighbours = [(axis, step) for axis in 'xyz' for step in (1, -1)] + [('c', 1)]
    for axis, step in neighbours:
        pl.semaphore_signal(barrier, inc=1, device_id=place(axis, step), device_id_type=MESH_ID)
    pl.semaphore_wait(barrier, len(neighbours))


def around(axis):
    me = lax.axis_index(axis)
    return {'m': me, 'p': lax.rem(me + 3, RING), 'n': lax.rem(me + 1, RING), 'o': lax.rem(me + 2, RING)}


class Plan:
    def __init__(self, sems, backlog):
        self.sems, self.backlog, self.items, self.copies = sems, backlog, {}, {}

    def send(self, name, axis, step, src, dst, needs, priority):
        index = len(self.copies)
        self.copies[name] = pltpu.make_async_remote_copy(
            src_ref=src, dst_ref=dst, send_sem=self.sems[0].at[index], recv_sem=self.sems[1].at[index], device_id=place(axis, step), device_id_type=MESH_ID
        )
        size = math.prod(src.shape) * jnp.dtype(src.dtype).itemsize
        self.items[name] = ((axis, step), size, tuple(needs), priority)

    def work(self, name, cost, run, needs, priority):
        self.items[name] = (run, cost, tuple(needs), priority)

    def order(self, now):
        free, done, todo, order = {}, {}, dict(self.items), []
        while todo:
            due, soonest = None, math.inf
            for name, (what, size, needs, priority) in todo.items():
                if any(need not in done for need in needs):
                    continue
                when = max([done[need] for need in needs], default=0.0)
                if name in self.copies:
                    when = max(when, free.get(what, 0.0) - self.backlog)
                if when <= now + 1e-9:
                    key = (name not in self.copies, priority)
                    due = min(due, (key, len(order), name), key=lambda d: d[0]) if due else (key, len(order), name)
                soonest = min(soonest, when)
            if due is None:
                now = max(now, soonest)
                continue
            name = due[2]
            what, size, _, _ = todo.pop(name)
            order.append(name)
            if name in self.copies:
                inside = what[0] == 'c'
                free[what] = max(now, free.get(what, 0.0)) + size / (CHIP_RATE if inside else LINK_RATE)
                done[name] = free[what] + (CHIP_US if inside else HOP_US)
                now += 0.03
            else:
                now += size
                done[name] = now
        return order

    def run(self, start):
        landed = set()

        def arrive(name):
            if name in self.copies and name not in landed:
                landed.add(name)
                self.copies[name].wait_recv()

        for name in self.order(start):
            what, _, needs, _ = self.items[name]
            for need in needs:
                arrive(need)
            if name in self.copies:
                self.copies[name].start()
            else:
                what()
        for name, copy in self.copies.items():
            arrive(name)
            copy.wait_send()


def plan_rows(plan, key, own, out, axis, after, priority):
    half = out.shape[1] // 2
    top, bottom = pl.ds(0, half), pl.ds(half, half)

    def send(name, axis, step, src, dst, needs, late=0):
        plan.send((key,) + name, axis, step, src, out.at[dst], needs, priority + late)
        return (key,) + name

    right_top = send(('own', 'right', 'top'), axis, 1, own.at[top], (1, top), after)
    left_bottom = send(('own', 'left', 'bottom'), axis, -1, own.at[bottom], (2, bottom), after)
    right_bottom = send(('own', 'right', 'bottom'), axis, 1, own.at[bottom], (1, bottom), after, 2)
    left_top = send(('own', 'left', 'top'), axis, -1, own.at[top], (2, top), after, 2)
    ahead = send(('on', 'right'), axis, 1, out.at[1, top], (3, top), [right_top], 1)
    behind = send(('on', 'left'), axis, -1, out.at[2, bottom], (3, bottom), [left_bottom], 1)
    slots = [list(after), [right_top, right_bottom], [left_top, left_bottom], [ahead, behind]]
    return slots + [[send(('core', slot), 'c', 1, out.at[slot] if slot else own, (4 + slot,), slots[slot])] for slot in range(4)]


def plan_sums(plan, key, parts, filled, got, put, axis, after, costs, priority):
    at = around(axis)
    half = parts.shape[1] // 2
    top, bottom = pl.ds(0, half), pl.ds(half, half)
    send = lambda name, step, src, dst, needs, late: plan.send((key, name), axis, step, src, got.at[dst], list(after) + needs, priority + late)
    send('far right', 1, parts.at[at['o'], top], 0, filled['o'], 0)
    send('far left', -1, parts.at[at['o'], bottom], 3, filled['o'], 0)
    send('near right', 1, parts.at[at['n'], bottom], 1, filled['n'], 3)
    send('near left', -1, parts.at[at['p'], top], 4, filled['p'], 3)

    def add(slot, which, rows):
        got[slot] = got[slot] + parts[at[which], rows]

    plan.work((key, 'add right'), costs[0], lambda: add(0, 'n', top), [(key, 'far right')] + filled['n'], 1)
    plan.work((key, 'add left'), costs[0], lambda: add(3, 'p', bottom), [(key, 'far left')] + filled['p'], 1)
    send('on right', 1, got.at[0], 2, [(key, 'add right')], 1)
    send('on left', -1, got.at[3], 5, [(key, 'add left')], 1)

    def total(which, rows, one, two):
        put(which, parts[at['m'], rows] + got[one] + got[two])

    plan.work((key, 'sum 0'), costs[1], lambda: total(0, top, 4, 2), [(key, 'near left'), (key, 'on right')] + filled['m'], 2)
    plan.work((key, 'sum 1'), costs[1], lambda: total(1, bottom, 1, 5), [(key, 'near right'), (key, 'on left')] + filled['m'], 2)
    return [(key, 'sum 0'), (key, 'sum 1')]


def put_blocks(total, which, value):
    total[pl.ds(which * 2, 2)] = value.reshape((2,) + total.shape[1:])


def put_rows(total, offset, which, value):
    total[pl.ds(offset + which * value.shape[0], value.shape[0])] = value


def plan_blocks(plan, key, out, order, rows, after):
    near, far = out.at[0], out.at[1]
    at = {axis: around(axis) for axis in order}
    every = pl.ds(0, RING)
    onward = {'m': 1, 'o': 1, 'p': -1, 'n': -1}

    def where(picks, part=rows):
        chosen = dict(zip(order, picks))
        return tuple(every if chosen[axis] == 'all' else at[axis][chosen[axis]] for axis in ('z', 'y', 'x')) + (pl.ds(*part),)

    def send(name, axis, step, picks, needs, priority, part=rows, dst=near):
        spot = where(picks, part)
        plan.send((key,) + name, axis, step, near.at[spot], dst.at[spot], needs, priority)
        return [(key,) + name]

    cut = (rows[1] // 16) * 8
    halves = (rows[0], cut), (rows[0] + cut, rows[1] - cut)
    ready = {'m': list(after)}
    for side, step, half in (('p', 1, 0), ('n', -1, 1)):
        ready[side] = send((1, 'own', side), order[0], step, 'mmm', after, 10)
    ready['o'] = []
    for side, step, half in (('p', 1, 0), ('n', -1, 1)):
        ready['o'] = ready['o'] + send((1, 'on', side), order[0], step, (side, 'm', 'm'), ready[side], 9, halves[half])
    for phase in (2, 3):
        spread = {'m': sum([ready[i] for i in 'mpno'], []), 'p': [], 'n': [], 'o': []}
        arrived = {}
        for i in 'mpno':
            picks = {side: (i, side, 'm') if phase == 2 else ('all', i, side) for side in 'mpno'}
            for side, step in (('p', 1), ('n', -1)):
                first = onward[i] == step
                arrived[i, side] = send((phase, 'own', side, i), order[phase - 1], step, picks['m'], ready[i], (12 if first else 14) if phase == 2 else (30 if first else 50))
            side = 'p' if onward[i] == 1 else 'n'
            arrived[i, 'o'] = send((phase, 'on', side, i), order[phase - 1], onward[i], picks[side], arrived[i, side], 11 if phase == 2 else 40)
            for side in 'pno':
                spread[side] = spread[side] + arrived[i, side]
                if phase == 3:
                    send(('core', side, i), 'c', 1, picks[side], arrived[i, side], 60, dst=far)
        if phase == 2:
            ready = spread
            send(('core', 'm'), 'c', 1, ('all', 'all', 'm'), sum([ready[i] for i in 'mpno'], []), 60, dst=far)


def gelu_terms(x):
    square = x * x
    t = jnp.tanh(x * (GELU_S + GELU_S * GELU_C * square))
    cdf = 0.5 + 0.5 * t
    slope = cdf + (0.5 * x) * (1.0 - t * t) * (GELU_S + 3.0 * GELU_S * GELU_C * square)
    return x * cdf, slope


class Weights:
    def __init__(self, w_in, w_out, buf_in, buf_out, sems):
        self.w_in, self.w_out, self.buf_in, self.buf_out, self.sems = w_in, w_out, buf_in, buf_out, sems
        self.width = buf_in.shape[2]
        self.steps = w_in.shape[2] // self.width

    def copies(self, layer, chunk, slot):
        at = pl.ds(pl.multiple_of(chunk * self.width, self.width), self.width)
        return (
            pltpu.make_async_copy(self.w_in.at[layer, :, at], self.buf_in.at[slot], self.sems.at[0, slot]),
            pltpu.make_async_copy(self.w_out.at[layer, at, :], self.buf_out.at[slot], self.sems.at[1, slot]),
        )

    def start(self, layer, chunk, slot):
        for copy in self.copies(layer, chunk, slot):
            copy.start()

    def sweep(self, layer, base, following, body):
        def step(chunk):
            slot = lax.rem(base + chunk, SLOTS)
            for copy in self.copies(layer, chunk, slot):
                copy.wait()
            ahead = chunk + SLOTS - 1
            over = lax.div(ahead, self.steps)

            def load():
                self.start(layer + over * ((layer if following is None else following) - layer), ahead - over * self.steps, lax.rem(base + ahead, SLOTS))

            if following is None:
                pl.when(ahead < self.steps)(load)
            else:
                load()
            body(chunk, self.buf_in.at[slot], self.buf_out.at[slot])

        return lambda first, last: pl.loop(first, last)(step)


def forward_layer(weights, layer, base, following, hidden, pre, total, out):
    half = weights.width // 2

    def body(chunk, wi, wo):
        posts = []
        for part in range(2):
            at = pl.ds(part * half, half)
            u = jnp.dot(hidden[...], wi[:, at], preferred_element_type=F32).astype(BF16)
            if pre is not None:
                pre[:, pl.ds(pl.multiple_of(chunk * weights.width + part * half, half), half)] = u
            posts.append(gelu_terms(u.astype(F32))[0].astype(BF16))
        for part in range(2):
            total[...] += jnp.dot(posts[part], wo[pl.ds(part * half, half)], preferred_element_type=F32)

    sweep = weights.sweep(layer, base, following, body)

    def run():
        total[...] = jnp.zeros_like(total)
        sweep(0, weights.steps)
        out((hidden[...].astype(F32) + total[...]).astype(BF16))

    return run


def backward_layer(weights, layer, base, following, grad, pre, total, out):
    half = weights.width // 2

    def body(chunk, wi, wo):
        grads = []
        for part in range(2):
            e = lax.dot_general(grad[...], wo[pl.ds(part * half, half)], COL, preferred_element_type=F32)
            u = pre[:, pl.ds(pl.multiple_of(chunk * weights.width + part * half, half), half)]
            grads.append((e * gelu_terms(u.astype(F32))[1]).astype(BF16))
        for part in range(2):
            total[...] += lax.dot_general(grads[part], wi[:, pl.ds(part * half, half)], COL, preferred_element_type=F32)

    sweep = weights.sweep(layer, base, following, body)
    middle = weights.steps // 2

    def first_piece():
        total[...] = jnp.zeros_like(total)
        sweep(0, middle)

    def second_piece():
        sweep(middle, weights.steps)
        out[...] = (grad[...].astype(F32) + total[...]).astype(BF16)

    return first_piece, second_piece


class ShardWork:
    def __init__(self, layer, w_in, w_out, shard, take):
        self.group, self.shard = GROUPS[layer], shard
        self.wi, self.wo, self.wi_t, self.act, self.slope, w_sems = take(6)
        self.buffers = [take(4), take(4)]
        width = self.wi.shape[1]
        start = pl.multiple_of((lax.axis_index(self.group) * 2 + lax.axis_index('c')) * width, width)
        self.loads = [
            pltpu.make_async_copy(w_in.at[layer, :, pl.ds(start, width)], self.wi, w_sems.at[0]),
            pltpu.make_async_copy(w_out.at[layer, pl.ds(start, width), :], self.wo, w_sems.at[1]),
        ]

    def load(self):
        for load in self.loads:
            load.start()

    def ready(self):
        self.loads[0].wait()
        self.wi_t[...] = self.wi[...].T
        self.loads[1].wait()

    def rows(self, hg, gg, slot):
        n = hg.shape[1]
        at = pl.ds(pl.multiple_of(slot * n, n), n)
        u = lax.dot_general(self.wi_t[...], hg[slot], COL, preferred_element_type=F32).astype(BF16)
        e = lax.dot_general(self.wo[...], gg[slot], COL, preferred_element_type=F32)
        post, slope = gelu_terms(u.astype(F32))
        self.act[:, at] = post.astype(BF16)
        self.slope[:, at] = (e * slope).astype(BF16)

    def fill(self, color, which, hg, gg):
        parts = self.buffers[color][0]
        cols = parts.shape[2]
        at = pl.ds(pl.multiple_of(which * cols, cols), cols)
        left, right = (self.slope, hg) if color == 0 else (self.act, gg)
        parts[which] = jnp.dot(left[...], right[:, :, at].reshape(-1, cols), preferred_element_type=F32)

    def plan(self, plan, hg, gg, ready, priority):
        for color in range(2):
            parts, got_one, mid, got_two = self.buffers[color]
            one, two = OTHERS[self.group][color], OTHERS[self.group][1 - color]
            at = around(one)
            filled = {}
            for rank, which in enumerate('onpm'):
                filled[which] = [('fill', color, which)]
                plan.work(filled[which][0], 0.7, functools.partial(self.fill, color, at[which], hg, gg), ready, (10, 21, 22, 40)[rank] + 0.5 * color)
            sums = plan_sums(plan, ('sum', 1, color), parts, filled, got_one, functools.partial(put_blocks, mid), one, [], (0.12, 0.15), priority)
            filled = dict.fromkeys('mpno', sums)
            put = functools.partial(put_rows, self.shard, color * mid.shape[1])
            plan_sums(plan, ('sum', 2, color), mid, filled, got_two, put, two, [], (0.05, 0.05), priority - 4)


def shard_scratch(tokens, d, width):
    cols, n = d // RING, width // RING
    scratch = [pltpu.VMEM((d, width), BF16), pltpu.VMEM((width, d), BF16), pltpu.VMEM((width, d), BF16)]
    scratch += [pltpu.VMEM((width, tokens), BF16)] * 2 + [pltpu.SemaphoreType.DMA((2,))]
    for _ in range(2):
        scratch += [pltpu.VMEM((RING, width, cols), F32), pltpu.VMEM((6, width // 2, cols), F32)]
        scratch += [pltpu.VMEM((RING, n, cols), F32), pltpu.VMEM((6, n // 2, cols), F32)]
    return scratch


def send_sems(count):
    return [pltpu.SemaphoreType.DMA((count,))] * 2


def stream_scratch(d, full):
    width = min(CHUNK, full // 4)
    return [pltpu.VMEM((SLOTS, d, width), BF16), pltpu.VMEM((SLOTS, width, d), BF16), pltpu.SemaphoreType.DMA((2, SLOTS))]


def first_kernel(scale, tok, tgt, w_in, w_out, *refs):
    refs = list(refs)
    take = lambda count: [refs.pop(0) for _ in range(count)]
    (shard,) = take(1)
    hg_out, gg_out = take(3), take(3)
    buf_in, buf_out, w_sems, pre, total, mine, keep_sems, h3, g4 = take(9)
    sems = take(2)
    layers = w_in.shape[0]
    top = layers - 1
    weights = Weights(w_in, w_out, buf_in, buf_out, w_sems)
    work = ShardWork(top, w_in, w_out, shard, take)
    for chunk in range(SLOTS - 1):
        weights.start(0, chunk, chunk)
    work.load()
    meet()
    plan = Plan(sems, 3.0)
    hiddens = [tok, mine.at[0], mine.at[1], h3.at[0]]
    grads = [g4.at[0], mine.at[2], mine.at[3], mine.at[4]]

    def to(ref):
        def out(value):
            ref[...] = value

        return out

    def last(value):
        g4[0] = ((value.astype(F32) - tgt[...].astype(F32)) * scale).astype(BF16)

    steps = weights.steps
    outs = [to(hiddens[1]), to(hiddens[2]), to(hiddens[3]), last]
    for l in range(layers):
        run = forward_layer(weights, l, l * steps, min(l + 1, top), hiddens[l], pre.at[l - 1] if l else None, total, outs[l])
        plan.work(('forward', l), 6.5, run, [('forward', l - 1)] if l else [], 1)
    plan.work('ready', 2.0, work.ready, [('forward', 1)], 3)
    done = ('forward', top)
    for i in range(layers - 1):
        l = top - i
        pieces = backward_layer(weights, l, (layers + i) * steps, l - 1 if l > 1 else None, grads[i], pre.at[l - 1], total, grads[i + 1])
        for k, piece in enumerate(pieces):
            plan.work(('backward', l, k), 3.5, piece, [done], 6 + i)
            done = ('backward', l, k)
    stores = []

    def keep(name, own, out, axis, after, priority):
        plan_rows(plan, name, own, out, axis, after, priority)
        stores.append(pltpu.make_async_copy(own, out.at[0], keep_sems.at[len(stores)]))
        plan.work((name, 'store'), 0.02, stores[-1].start, after, 50)

    for l in range(top):
        keep(('h', l), hiddens[l], hg_out[l], GROUPS[l], [('forward', l - 1)] if l else [], (22, 22, 10)[l])
    for l in range(top):
        keep(('g', l), grads[top - l], gg_out[l], GROUPS[l], [('backward', l + 1, 1)], (32, 31, 10)[l])
    h3_slots = plan_rows(plan, 'h3', hiddens[top], h3, GROUPS[top], [('forward', top - 1)], 0)
    g4_slots = plan_rows(plan, 'g4', grads[0], g4, GROUPS[top], [('forward', top)], 5)
    rows = []
    for slots in ((0,), (4,), (1, 2), (5, 6), (3,), (7,)):
        if len(slots) == 1:
            run = functools.partial(work.rows, h3, g4, slots[0])
        else:
            run = functools.partial(pl.loop(slots[0], slots[-1] + 1), functools.partial(work.rows, h3, g4))
        rows.append(('rows', slots))
        plan.work(rows[-1], 0.85 * len(slots), run, sum([h3_slots[slot] + g4_slots[slot] for slot in slots], ['ready']), 5)
    work.plan(plan, h3, g4, rows, -10)
    plan.run(5.0)
    for store in stores:
        store.wait()


def first(tok, tgt, w_in, w_out, total_rows, collective_id):
    vmem, anywhere = pl.BlockSpec(memory_space=pltpu.VMEM), pl.BlockSpec(memory_space=pl.ANY)
    n, d = tok.shape
    layers, _, full = w_in.shape
    group = (2 * RING, n, d)
    kept = 2 * (layers - 1)
    scratch = stream_scratch(d, full)
    scratch += [pltpu.VMEM((layers - 1, n, full), BF16), pltpu.VMEM((n, d), F32), pltpu.VMEM((5, n, d), BF16)]
    scratch += [pltpu.SemaphoreType.DMA((kept,))] + [pltpu.VMEM(group, BF16)] * 2 + send_sems((kept + 2) * ROW_SENDS + SUM_SENDS)
    scratch += shard_scratch(2 * RING * n, d, full // (2 * RING))
    return pl.pallas_call(
        functools.partial(first_kernel, 1.0 / total_rows),
        out_shape=[pltpu.VMEM((full // (4 * RING), d // RING), F32)] + [jax.ShapeDtypeStruct(group, BF16)] * kept,
        in_specs=[vmem, vmem, anywhere, anywhere],
        out_specs=[vmem] + [anywhere] * kept,
        scratch_shapes=scratch,
        compiler_params=pltpu.CompilerParams(collective_id=collective_id, has_side_effects=True, vmem_limit_bytes=60 * MIB),
        cost_estimate=pl.CostEstimate(flops=60_000_000_000, bytes_accessed=96 * MIB, transcendentals=0),
        name='first',
    )(tok, tgt, w_in, w_out)


def layer_kernel(layer, hg_in, gg_in, w_in, w_out, above, shard, blocks, hg, gg, row_sems, *refs):
    refs = list(refs)
    take = lambda count: [refs.pop(0) for _ in range(count)]
    sems = take(2)
    work = ShardWork(layer, w_in, w_out, shard, take)
    work.load()

    def row_copies(i):
        return [pltpu.make_async_copy(src.at[i], dst.at[i], row_sems.at[k, i]) for k, (src, dst) in enumerate(((hg_in, hg), (gg_in, gg)))]

    for i in range(2 * RING):
        for copy in row_copies(i):
            copy.start()
    hold_block(above, blocks)
    meet()
    plan = Plan(sems, 2.0)
    plan.work('ready', 2.0, work.ready, [], 5)

    def quarter(first):
        @pl.loop(first, first + 2)
        def _(i):
            for copy in row_copies(i):
                copy.wait()
            work.rows(hg, gg, i)

    for i in range(RING):
        plan.work(('rows', i), 1.7, functools.partial(quarter, 2 * i), ['ready'], 6)
    plan_all_blocks(plan, blocks, SHARES[layer + 1])
    work.plan(plan, hg, gg, [('rows', i) for i in range(RING)], 45)
    plan.run(4.0)


def layer_grads(layer, hg, gg, w_in, w_out, above):
    vmem, anywhere = pl.BlockSpec(memory_space=pltpu.VMEM), pl.BlockSpec(memory_space=pl.ANY)
    _, m, d = hg.shape
    scratch = [pltpu.VMEM(hg.shape, BF16)] * 2 + [pltpu.SemaphoreType.DMA((2, 2 * RING))]
    scratch += send_sems(BLOCK_SENDS + SUM_SENDS)
    scratch += shard_scratch(2 * RING * m, d, w_in.shape[2] // (2 * RING))
    return pl.pallas_call(
        functools.partial(layer_kernel, layer),
        out_shape=[pltpu.VMEM(above.shape, F32), pltpu.VMEM((2, RING, RING, RING) + above.shape, F32)],
        in_specs=[anywhere] * 4 + [vmem],
        out_specs=[vmem, vmem],
        scratch_shapes=scratch,
        compiler_params=pltpu.CompilerParams(collective_id=layer, has_side_effects=True, vmem_limit_bytes=31_000_000),
        cost_estimate=pl.CostEstimate(flops=30_000_000_000, bytes_accessed=16 * MIB, transcendentals=0),
        name='layer_grads',
    )(hg, gg, w_in, w_out, in_vmem(above))


def in_vmem(value):
    return pltpu.with_memory_space_constraint(value, pltpu.VMEM)


def hold_block(shard, out):
    out[(0,) + tuple(lax.axis_index(axis) for axis in ('z', 'y', 'x'))] = shard[...]


def plan_all_blocks(plan, out, shares):
    unit = out.shape[-2] // sum(shares)
    for k, order in enumerate(ORDERS):
        plan_blocks(plan, ('blocks', k), out, order, (unit * sum(shares[:k]), unit * shares[k]), [])


def block_gather_kernel(shard, out, send, recv):
    hold_block(shard, out)
    meet()
    plan = Plan((send, recv), 2.0)
    plan_all_blocks(plan, out, SHARES[0])
    plan.run(3.0)


def block_gather(shard, collective_id):
    vmem = pl.BlockSpec(memory_space=pltpu.VMEM)
    return pl.pallas_call(
        block_gather_kernel,
        out_shape=pltpu.VMEM((2, RING, RING, RING) + shard.shape, F32),
        in_specs=[vmem],
        out_specs=vmem,
        scratch_shapes=send_sems(BLOCK_SENDS),
        compiler_params=pltpu.CompilerParams(collective_id=collective_id, has_side_effects=True, vmem_limit_bytes=16 * MIB),
        cost_estimate=pl.CostEstimate(flops=60_000_000_000, bytes_accessed=32 * MIB, transcendentals=0),
        name='block_gather',
    )(in_vmem(shard))


def place_kernel(along, _, blocks, *refs):
    out_in, out_out = refs[-2:]
    i, k = pl.program_id(0), pl.program_id(1)
    n, cols = blocks.shape[-2] // 2, blocks.shape[-1]
    for a in range(RING):
        for b in range(RING):
            at = [a, b]
            at.insert(along, i)
            block = blocks[(k,) + tuple(at)]
            out_in[a * cols : (a + 1) * cols, b * n : (b + 1) * n] = block[:n].T
            out_out[a * n : (a + 1) * n, b * cols : (b + 1) * cols] = block[n:]


def place_blocks(core, blocks, outs, layer, layers):
    cols = blocks.shape[-1]
    n = cols // 2
    width, d = n * RING, cols * RING
    return pl.pallas_call(
        functools.partial(place_kernel, AXES.index(GROUPS[layer])),
        grid_spec=pltpu.PrefetchScalarGridSpec(
            num_scalar_prefetch=1,
            grid=(RING, 2),
            in_specs=[pl.BlockSpec(memory_space=pltpu.VMEM)] + [pl.BlockSpec(memory_space=pl.ANY)] * len(outs),
            out_specs=[
                pl.BlockSpec((None, d, width), lambda i, k, s: (layer, 0, i * 2 + (s[0] + k) % 2)),
                pl.BlockSpec((None, width, d), lambda i, k, s: (layer, i * 2 + (s[0] + k) % 2, 0)),
            ],
        ),
        out_shape=[jax.ShapeDtypeStruct((layers, d, width * 2 * RING), F32), jax.ShapeDtypeStruct((layers, width * 2 * RING, d), F32)],
        input_output_aliases={2 + k: k for k in range(len(outs))},
        compiler_params=pltpu.CompilerParams(vmem_limit_bytes=24 * MIB),
        cost_estimate=pl.CostEstimate(flops=10_000_000_000, bytes_accessed=32 * MIB, transcendentals=0),
        name='place_blocks',
    )(core, in_vmem(blocks), *outs)


def solution(mesh):
    mesh4 = Mesh(mesh.devices.reshape(RING, RING, RING, 2), AXES)

    def local_step(tok, tgt, w_in, w_out):
        layers = w_in.shape[0]
        core = lax.axis_index('c').astype(jnp.int32).reshape(1)
        above, *rows = first(tok, tgt, w_in, w_out, tok.shape[0] * mesh4.size, 2 * layers)
        hg, gg = rows[: layers - 1], rows[layers - 1 :]
        outs = []
        for l in reversed(range(layers - 1)):
            if outs:
                above, *outs = lax.optimization_barrier((above, *outs))
            shard, blocks = layer_grads(l, hg[l], gg[l], w_in, w_out, above)
            outs = place_blocks(core, blocks, outs, l + 1, layers)
            above = shard
        above, *outs = lax.optimization_barrier((above, *outs))
        outs = place_blocks(core, block_gather(above, layers + 1), outs, 0, layers)
        return outs[0], outs[1]

    spec = P(AXES, None)
    return jax.shard_map(local_step, mesh=mesh4, in_specs=(spec, spec, P(), P()), out_specs=(P(), P()), check_vma=False)
```

```python
import functools
import math

import jax
import jax.numpy as jnp
from jax import lax
from jax.experimental import pallas as pl
from jax.experimental.pallas import tpu as pltpu
from jax.sharding import Mesh
from jax.sharding import PartitionSpec as P

AXES = ('z', 'y', 'x', 'c')
RING = 4
GROUPS = ('x', 'z', 'y', 'x')
OTHERS = {'x': ('z', 'y'), 'y': ('z', 'x'), 'z': ('y', 'x')}
CHUNK = 512
SLOTS = 6
COLORS = (('yzx', 5), ('zxy', 8), ('xyz', 12), ('yxz', 3), ('zyx', 4))
LAST_COLORS = (('xyz', 10), ('zxy', 8), ('xzy', 3), ('yzx', 11))
F32, BF16 = jnp.float32, jnp.bfloat16
COL = (((1,), (1,)), ((), ()))
GELU_S = 0.7978845608028654
GELU_C = 0.044715
MESH_ID = pl.DeviceIdType.MESH
MIB = 1 << 20
HOP_US, CHIP_US = 2.0, 1.1
LINK_RATE, CHIP_RATE = 45.7e3, 600e3
ROW_SENDS, SUM_SENDS, BLOCK_SENDS = 10, 24, 41


def place(axis, step):
    coords = [lax.axis_index(name) for name in AXES]
    which = AXES.index(axis)
    size = 2 if axis == 'c' else RING
    coords[which] = lax.rem(coords[which] + (step + size), size)
    return tuple(coords)


def greet():
    barrier = pltpu.get_barrier_semaphore()
    neighbours = [(axis, step) for axis in 'xyz' for step in (1, -1)] + [('c', 1)]
    for axis, step in neighbours:
        pl.semaphore_signal(barrier, inc=1, device_id=place(axis, step), device_id_type=MESH_ID)
    return lambda: pl.semaphore_wait(barrier, len(neighbours))


def around(axis):
    me = lax.axis_index(axis)
    return {'m': me, 'p': lax.rem(me + 3, RING), 'n': lax.rem(me + 1, RING), 'o': lax.rem(me + 2, RING)}


class Plan:
    def __init__(self, sems, backlog):
        self.sems, self.backlog, self.items, self.copies = sems, backlog, {}, {}

    def send(self, name, axis, step, src, dst, needs, priority):
        index = len(self.copies)
        self.copies[name] = pltpu.make_async_remote_copy(
            src_ref=src, dst_ref=dst, send_sem=self.sems[0].at[index], recv_sem=self.sems[1].at[index], device_id=place(axis, step), device_id_type=MESH_ID
        )
        size = math.prod(src.shape) * jnp.dtype(src.dtype).itemsize
        self.items[name] = ((axis, step), size, tuple(needs), priority)

    def work(self, name, cost, run, needs, priority):
        self.items[name] = (run, cost, tuple(needs), priority)

    def order(self, now):
        free, done, todo, order = {}, {}, dict(self.items), []
        while todo:
            due, soonest = None, math.inf
            for name, (what, size, needs, priority) in todo.items():
                if any(need not in done for need in needs):
                    continue
                when = max([done[need] for need in needs], default=0.0)
                if name in self.copies:
                    when = max(when, free.get(what, 0.0) - self.backlog)
                if when <= now + 1e-9:
                    key = (name not in self.copies, priority)
                    due = min(due, (key, len(order), name), key=lambda d: d[0]) if due else (key, len(order), name)
                soonest = min(soonest, when)
            if due is None:
                now = max(now, soonest)
                continue
            name = due[2]
            what, size, _, _ = todo.pop(name)
            order.append(name)
            if name in self.copies:
                inside = what[0] == 'c'
                free[what] = max(now, free.get(what, 0.0)) + size / (CHIP_RATE if inside else LINK_RATE)
                done[name] = free[what] + (CHIP_US if inside else HOP_US)
                now += 0.03
            else:
                now += size
                done[name] = now
        return order

    def run(self, start):
        landed = set()

        def arrive(name):
            if name in self.copies and name not in landed:
                landed.add(name)
                self.copies[name].wait_recv()

        for name in self.order(start):
            what, _, needs, _ = self.items[name]
            for need in needs:
                arrive(need)
            if name in self.copies:
                self.copies[name].start()
            else:
                what()
        for name, copy in self.copies.items():
            arrive(name)
            copy.wait_send()


def plan_rows(plan, key, own, out, axis, after, priority):
    half = out.shape[1] // 2
    top, bottom = pl.ds(0, half), pl.ds(half, half)

    def send(name, axis, step, src, dst, needs, late=0):
        plan.send((key,) + name, axis, step, src, out.at[dst], needs, priority + late)
        return (key,) + name

    right_top = send(('own', 'right', 'top'), axis, 1, own.at[top], (1, top), after)
    left_bottom = send(('own', 'left', 'bottom'), axis, -1, own.at[bottom], (2, bottom), after)
    right_bottom = send(('own', 'right', 'bottom'), axis, 1, own.at[bottom], (1, bottom), after, 2)
    left_top = send(('own', 'left', 'top'), axis, -1, own.at[top], (2, top), after, 2)
    ahead = send(('on', 'right'), axis, 1, out.at[1, top], (3, top), [right_top], 1)
    behind = send(('on', 'left'), axis, -1, out.at[2, bottom], (3, bottom), [left_bottom], 1)
    slots = [list(after), [right_top, right_bottom], [left_top, left_bottom], [ahead, behind]]
    return slots + [[send(('core', slot), 'c', 1, out.at[slot] if slot else own, (4 + slot,), slots[slot])] for slot in range(4)]


def plan_sums(plan, key, parts, filled, got, put, axis, after, costs, priority):
    at = around(axis)
    half = parts.shape[1] // 2
    top, bottom = pl.ds(0, half), pl.ds(half, half)
    send = lambda name, step, src, dst, needs, late: plan.send((key, name), axis, step, src, got.at[dst], list(after) + needs, priority + late)
    send('far right', 1, parts.at[at['o'], top], 0, filled['o'], 0)
    send('far left', -1, parts.at[at['o'], bottom], 3, filled['o'], 0)
    send('near right', 1, parts.at[at['n'], bottom], 1, filled['n'], 3)
    send('near left', -1, parts.at[at['p'], top], 4, filled['p'], 3)

    def add(slot, which, rows):
        got[slot] = got[slot] + parts[at[which], rows]

    plan.work((key, 'add right'), costs[0], lambda: add(0, 'n', top), [(key, 'far right')] + filled['n'], 1)
    plan.work((key, 'add left'), costs[0], lambda: add(3, 'p', bottom), [(key, 'far left')] + filled['p'], 1)
    send('on right', 1, got.at[0], 2, [(key, 'add right')], 1)
    send('on left', -1, got.at[3], 5, [(key, 'add left')], 1)

    def total(which, rows, one, two):
        put(which, parts[at['m'], rows] + got[one] + got[two])

    plan.work((key, 'sum 0'), costs[1], lambda: total(0, top, 4, 2), [(key, 'near left'), (key, 'on right')] + filled['m'], 2)
    plan.work((key, 'sum 1'), costs[1], lambda: total(1, bottom, 1, 5), [(key, 'near right'), (key, 'on left')] + filled['m'], 2)
    return [(key, 'sum 0'), (key, 'sum 1')]


def put_blocks(total, which, value):
    total[pl.ds(which * 2, 2)] = value.reshape((2,) + total.shape[1:])


def put_rows(total, offset, which, value):
    total[pl.ds(offset + which * value.shape[0], value.shape[0])] = value


def plan_blocks(plan, key, out, order, rows, after):
    near, far = out.at[0], out.at[1]
    at = {axis: around(axis) for axis in order}
    every = pl.ds(0, RING)
    onward = {'m': 1, 'o': 1, 'p': -1, 'n': -1}

    def where(picks, part=rows):
        chosen = dict(zip(order, picks))
        return tuple(every if chosen[axis] == 'all' else at[axis][chosen[axis]] for axis in ('z', 'y', 'x')) + (pl.ds(*part),)

    def send(name, axis, step, picks, needs, priority, part=rows, dst=near):
        spot = where(picks, part)
        plan.send((key,) + name, axis, step, near.at[spot], dst.at[spot], needs, priority)
        return [(key,) + name]

    cut = (rows[1] // 16) * 8
    halves = (rows[0], cut), (rows[0] + cut, rows[1] - cut)
    ready = {'m': list(after)}
    for side, step, half in (('p', 1, 0), ('n', -1, 1)):
        ready[side] = send((1, 'own', side), order[0], step, 'mmm', after, 10)
    ready['o'] = []
    for side, step, half in (('p', 1, 0), ('n', -1, 1)):
        ready['o'] = ready['o'] + send((1, 'on', side), order[0], step, (side, 'm', 'm'), ready[side], 9, halves[half])
    for phase in (2, 3):
        spread = {'m': sum([ready[i] for i in 'mpno'], []), 'p': [], 'n': [], 'o': []}
        arrived = {}
        for i in 'mpno':
            picks = {side: (i, side, 'm') if phase == 2 else ('all', i, side) for side in 'mpno'}
            for side, step in (('p', 1), ('n', -1)):
                first = onward[i] == step
                arrived[i, side] = send((phase, 'own', side, i), order[phase - 1], step, picks['m'], ready[i], (12 if first else 14) if phase == 2 else (30 if first else 50))
            side = 'p' if onward[i] == 1 else 'n'
            arrived[i, 'o'] = send((phase, 'on', side, i), order[phase - 1], onward[i], picks[side], arrived[i, side], 11 if phase == 2 else 40)
            for side in 'pno':
                spread[side] = spread[side] + arrived[i, side]
                if phase == 3:
                    send(('core', side, i), 'c', 1, picks[side], arrived[i, side], 60, dst=far)
        if phase == 2:
            ready = spread
            send(('core', 'm'), 'c', 1, ('all', 'all', 'm'), sum([ready[i] for i in 'mpno'], []), 60, dst=far)


def gelu_terms(x):
    square = x * x
    t = jnp.tanh(x * (GELU_S + GELU_S * GELU_C * square))
    cdf = 0.5 + 0.5 * t
    slope = cdf + (0.5 * x) * (1.0 - t * t) * (GELU_S + 3.0 * GELU_S * GELU_C * square)
    return x * cdf, slope


class Weights:
    def __init__(self, w_in, w_out, buf_in, buf_out, sems):
        self.w_in, self.w_out, self.buf_in, self.buf_out, self.sems = w_in, w_out, buf_in, buf_out, sems
        self.width = buf_in.shape[2]
        self.steps = w_in.shape[2] // self.width

    def copies(self, layer, chunk, slot):
        at = pl.ds(pl.multiple_of(chunk * self.width, self.width), self.width)
        return (
            pltpu.make_async_copy(self.w_in.at[layer, :, at], self.buf_in.at[slot], self.sems.at[0, slot]),
            pltpu.make_async_copy(self.w_out.at[layer, at, :], self.buf_out.at[slot], self.sems.at[1, slot]),
        )

    def start(self, layer, chunk, slot):
        for copy in self.copies(layer, chunk, slot):
            copy.start()

    def sweep(self, layer, base, following, body):
        def step(chunk):
            slot = lax.rem(base + chunk, SLOTS)
            for copy in self.copies(layer, chunk, slot):
                copy.wait()
            ahead = chunk + SLOTS - 1
            over = lax.div(ahead, self.steps)

            def load():
                self.start(layer + over * ((layer if following is None else following) - layer), ahead - over * self.steps, lax.rem(base + ahead, SLOTS))

            if following is None:
                pl.when(ahead < self.steps)(load)
            else:
                load()
            body(chunk, self.buf_in.at[slot], self.buf_out.at[slot])

        return lambda first, last: pl.loop(first, last)(step)


def forward_layer(weights, layer, base, following, hidden, pre, total, out):
    half = weights.width // 2

    def body(chunk, wi, wo):
        posts = []
        for part in range(2):
            at = pl.ds(part * half, half)
            u = jnp.dot(hidden[...], wi[:, at], preferred_element_type=F32).astype(BF16)
            if pre is not None:
                pre[:, pl.ds(pl.multiple_of(chunk * weights.width + part * half, half), half)] = u
            posts.append(gelu_terms(u.astype(F32))[0].astype(BF16))
        for part in range(2):
            total[...] += jnp.dot(posts[part], wo[pl.ds(part * half, half)], preferred_element_type=F32)

    sweep = weights.sweep(layer, base, following, body)

    def run():
        total[...] = jnp.zeros_like(total)
        sweep(0, weights.steps)
        out((hidden[...].astype(F32) + total[...]).astype(BF16))

    return run


def backward_layer(weights, layer, base, following, grad, pre, total, out):
    half = weights.width // 2

    def body(chunk, wi, wo):
        grads = []
        for part in range(2):
            e = lax.dot_general(grad[...], wo[pl.ds(part * half, half)], COL, preferred_element_type=F32)
            u = pre[:, pl.ds(pl.multiple_of(chunk * weights.width + part * half, half), half)]
            grads.append((e * gelu_terms(u.astype(F32))[1]).astype(BF16))
        for part in range(2):
            total[...] += lax.dot_general(grads[part], wi[:, pl.ds(part * half, half)], COL, preferred_element_type=F32)

    sweep = weights.sweep(layer, base, following, body)
    middle = weights.steps // 2

    def first_piece():
        total[...] = jnp.zeros_like(total)
        sweep(0, middle)

    def second_piece():
        sweep(middle, weights.steps)
        out[...] = (grad[...].astype(F32) + total[...]).astype(BF16)

    return first_piece, second_piece


class ShardWork:
    def __init__(self, layer, w_in, w_out, shard, take):
        self.group, self.shard = GROUPS[layer], shard
        self.wi, self.wo, self.wi_t, self.act, self.slope, w_sems = take(6)
        self.buffers = [take(4), take(4)]
        width = self.wi.shape[1]
        start = pl.multiple_of((lax.axis_index(self.group) * 2 + lax.axis_index('c')) * width, width)
        self.loads = [
            pltpu.make_async_copy(w_in.at[layer, :, pl.ds(start, width)], self.wi, w_sems.at[0]),
            pltpu.make_async_copy(w_out.at[layer, pl.ds(start, width), :], self.wo, w_sems.at[1]),
        ]

    def load(self):
        for load in self.loads:
            load.start()

    def ready(self):
        self.loads[0].wait()
        self.wi_t[...] = self.wi[...].T
        self.loads[1].wait()

    def rows(self, hg, gg, slot):
        n = hg.shape[1]
        at = pl.ds(pl.multiple_of(slot * n, n), n)
        u = lax.dot_general(self.wi_t[...], hg[slot], COL, preferred_element_type=F32).astype(BF16)
        e = lax.dot_general(self.wo[...], gg[slot], COL, preferred_element_type=F32)
        post, slope = gelu_terms(u.astype(F32))
        self.act[:, at] = post.astype(BF16)
        self.slope[:, at] = (e * slope).astype(BF16)

    def fill(self, color, which, hg, gg):
        parts = self.buffers[color][0]
        cols = parts.shape[2]
        at = pl.ds(pl.multiple_of(which * cols, cols), cols)
        left, right = (self.slope, hg) if color == 0 else (self.act, gg)
        parts[which] = jnp.dot(left[...], right[:, :, at].reshape(-1, cols), preferred_element_type=F32)

    def plan(self, plan, hg, gg, ready, priority):
        for color in range(2):
            parts, got_one, mid, got_two = self.buffers[color]
            one, two = OTHERS[self.group][color], OTHERS[self.group][1 - color]
            at = around(one)
            filled = {}
            for rank, which in enumerate('onpm'):
                filled[which] = [('fill', color, which)]
                plan.work(filled[which][0], 0.7, functools.partial(self.fill, color, at[which], hg, gg), ready, (10, 21, 22, 40)[rank] + 0.5 * color)
            sums = plan_sums(plan, ('sum', 1, color), parts, filled, got_one, functools.partial(put_blocks, mid), one, [], (0.12, 0.15), priority)
            filled = dict.fromkeys('mpno', sums)
            put = functools.partial(put_rows, self.shard, color * mid.shape[1])
            plan_sums(plan, ('sum', 2, color), mid, filled, got_two, put, two, [], (0.05, 0.05), priority - 4)


def shard_scratch(tokens, d, width):
    cols, n = d // RING, width // RING
    scratch = [pltpu.VMEM((d, width), BF16), pltpu.VMEM((width, d), BF16), pltpu.VMEM((width, d), BF16)]
    scratch += [pltpu.VMEM((width, tokens), BF16)] * 2 + [pltpu.SemaphoreType.DMA((2,))]
    for _ in range(2):
        scratch += [pltpu.VMEM((RING, width, cols), F32), pltpu.VMEM((6, width // 2, cols), F32)]
        scratch += [pltpu.VMEM((RING, n, cols), F32), pltpu.VMEM((6, n // 2, cols), F32)]
    return scratch


def send_sems(count):
    return [pltpu.SemaphoreType.DMA((count,))] * 2


def stream_scratch(d, full):
    width = min(CHUNK, full // 4)
    return [pltpu.VMEM((SLOTS, d, width), BF16), pltpu.VMEM((SLOTS, width, d), BF16), pltpu.SemaphoreType.DMA((2, SLOTS))]


def first_kernel(scale, tok, tgt, w_in, w_out, *refs):
    refs = list(refs)
    take = lambda count: [refs.pop(0) for _ in range(count)]
    (shard,) = take(1)
    hg_out, gg_out = take(3), take(3)
    buf_in, buf_out, w_sems, pre, total, mine, keep_sems, h3, g4 = take(9)
    sems = take(2)
    meet = greet()
    layers = w_in.shape[0]
    top = layers - 1
    weights = Weights(w_in, w_out, buf_in, buf_out, w_sems)
    work = ShardWork(top, w_in, w_out, shard, take)
    for chunk in range(SLOTS - 1):
        weights.start(0, chunk, chunk)
    work.load()
    meet()
    plan = Plan(sems, 3.0)
    hiddens = [tok, mine.at[0], mine.at[1], h3.at[0]]
    grads = [g4.at[0], mine.at[2], mine.at[3], mine.at[4]]

    def to(ref):
        def out(value):
            ref[...] = value

        return out

    def last(value):
        g4[0] = ((value.astype(F32) - tgt[...].astype(F32)) * scale).astype(BF16)

    steps = weights.steps
    outs = [to(hiddens[1]), to(hiddens[2]), to(hiddens[3]), last]
    for l in range(layers):
        run = forward_layer(weights, l, l * steps, min(l + 1, top), hiddens[l], pre.at[l - 1] if l else None, total, outs[l])
        plan.work(('forward', l), 6.5, run, [('forward', l - 1)] if l else [], 1)
    plan.work('ready', 2.0, work.ready, [('forward', 1)], 3)
    done = ('forward', top)
    for i in range(layers - 1):
        l = top - i
        pieces = backward_layer(weights, l, (layers + i) * steps, l - 1 if l > 1 else None, grads[i], pre.at[l - 1], total, grads[i + 1])
        for k, piece in enumerate(pieces):
            plan.work(('backward', l, k), 3.5, piece, [done], 6 + i)
            done = ('backward', l, k)
    stores = []

    def keep(name, own, out, axis, after, priority):
        plan_rows(plan, name, own, out, axis, after, priority)
        stores.append(pltpu.make_async_copy(own, out.at[0], keep_sems.at[len(stores)]))
        plan.work((name, 'store'), 0.02, stores[-1].start, after, 50)

    for l in range(top):
        keep(('h', l), hiddens[l], hg_out[l], GROUPS[l], [('forward', l - 1)] if l else [], (22, 22, 10)[l])
    for l in range(top):
        keep(('g', l), grads[top - l], gg_out[l], GROUPS[l], [('backward', l + 1, 1)], (32, 31, 10)[l])
    h3_slots = plan_rows(plan, 'h3', hiddens[top], h3, GROUPS[top], [('forward', top - 1)], 0)
    g4_slots = plan_rows(plan, 'g4', grads[0], g4, GROUPS[top], [('forward', top)], 5)
    rows = []
    for slots in ((0,), (4,), (1, 2), (5, 6), (3,), (7,)):
        if len(slots) == 1:
            run = functools.partial(work.rows, h3, g4, slots[0])
        else:
            run = functools.partial(pl.loop(slots[0], slots[-1] + 1), functools.partial(work.rows, h3, g4))
        rows.append(('rows', slots))
        plan.work(rows[-1], 0.85 * len(slots), run, sum([h3_slots[slot] + g4_slots[slot] for slot in slots], ['ready']), 5)
    work.plan(plan, h3, g4, rows, -10)
    plan.run(5.0)
    for store in stores:
        store.wait()


def first(tok, tgt, w_in, w_out, total_rows, collective_id):
    vmem, anywhere = pl.BlockSpec(memory_space=pltpu.VMEM), pl.BlockSpec(memory_space=pl.ANY)
    n, d = tok.shape
    layers, _, full = w_in.shape
    group = (2 * RING, n, d)
    kept = 2 * (layers - 1)
    scratch = stream_scratch(d, full)
    scratch += [pltpu.VMEM((layers - 1, n, full), BF16), pltpu.VMEM((n, d), F32), pltpu.VMEM((5, n, d), BF16)]
    scratch += [pltpu.SemaphoreType.DMA((kept,))] + [pltpu.VMEM(group, BF16)] * 2 + send_sems((kept + 2) * ROW_SENDS + SUM_SENDS)
    scratch += shard_scratch(2 * RING * n, d, full // (2 * RING))
    return pl.pallas_call(
        functools.partial(first_kernel, 1.0 / total_rows),
        out_shape=[pltpu.VMEM((full // (4 * RING), d // RING), F32)] + [jax.ShapeDtypeStruct(group, BF16)] * kept,
        in_specs=[vmem, vmem, anywhere, anywhere],
        out_specs=[vmem] + [anywhere] * kept,
        scratch_shapes=scratch,
        compiler_params=pltpu.CompilerParams(collective_id=collective_id, has_side_effects=True, vmem_limit_bytes=60 * MIB),
        cost_estimate=pl.CostEstimate(flops=60_000_000_000, bytes_accessed=96 * MIB, transcendentals=0),
        name='first',
    )(tok, tgt, w_in, w_out)


def layer_kernel(layer, hg_in, gg_in, w_in, w_out, above, shard, blocks, hg, gg, row_sems, *refs):
    refs = list(refs)
    take = lambda count: [refs.pop(0) for _ in range(count)]
    sems = take(2)
    meet = greet()
    work = ShardWork(layer, w_in, w_out, shard, take)
    work.load()

    def row_copies(i):
        return [pltpu.make_async_copy(src.at[i], dst.at[i], row_sems.at[k, i]) for k, (src, dst) in enumerate(((hg_in, hg), (gg_in, gg)))]

    for i in range(2 * RING):
        for copy in row_copies(i):
            copy.start()
    hold_block(above, blocks)
    meet()
    plan = Plan(sems, 3.0)
    plan.work('ready', 2.0, work.ready, [], 5)

    def quarter(first):
        @pl.loop(first, first + 2)
        def _(i):
            for copy in row_copies(i):
                copy.wait()
            work.rows(hg, gg, i)

    for i in range(RING):
        plan.work(('rows', i), 1.7, functools.partial(quarter, 2 * i), ['ready'], 6)
    turn = dict(zip('zyx', (GROUPS[layer],) + OTHERS[GROUPS[layer]]))
    plan_all_blocks(plan, blocks, [([turn[axis] for axis in order], share) for order, share in COLORS])
    work.plan(plan, hg, gg, [('rows', i) for i in range(RING)], 45)
    plan.run(4.0)


def layer_grads(layer, hg, gg, w_in, w_out, above):
    vmem, anywhere = pl.BlockSpec(memory_space=pltpu.VMEM), pl.BlockSpec(memory_space=pl.ANY)
    _, m, d = hg.shape
    scratch = [pltpu.VMEM(hg.shape, BF16)] * 2 + [pltpu.SemaphoreType.DMA((2, 2 * RING))]
    scratch += send_sems(len(COLORS) * BLOCK_SENDS + SUM_SENDS)
    scratch += shard_scratch(2 * RING * m, d, w_in.shape[2] // (2 * RING))
    return pl.pallas_call(
        functools.partial(layer_kernel, layer),
        out_shape=[pltpu.VMEM(above.shape, F32), pltpu.VMEM((2, RING, RING, RING) + above.shape, F32)],
        in_specs=[anywhere] * 4 + [vmem],
        out_specs=[vmem, vmem],
        scratch_shapes=scratch,
        compiler_params=pltpu.CompilerParams(collective_id=layer, has_side_effects=True, vmem_limit_bytes=31_000_000),
        cost_estimate=pl.CostEstimate(flops=30_000_000_000, bytes_accessed=16 * MIB, transcendentals=0),
        name='layer_grads',
    )(hg, gg, w_in, w_out, in_vmem(above))


def in_vmem(value):
    return pltpu.with_memory_space_constraint(value, pltpu.VMEM)


def hold_block(shard, out):
    out[(0,) + tuple(lax.axis_index(axis) for axis in ('z', 'y', 'x'))] = shard[...]


def plan_all_blocks(plan, out, colors):
    unit, start = out.shape[-2] // sum(share for _, share in colors), 0
    for k, (order, share) in enumerate(colors):
        plan_blocks(plan, ('blocks', k), out, order, (unit * start, unit * share), [])
        start += share


def block_gather_kernel(shard, out, send, recv):
    meet = greet()
    hold_block(shard, out)
    meet()
    plan = Plan((send, recv), 2.0)
    plan_all_blocks(plan, out, LAST_COLORS)
    plan.run(3.0)


def block_gather(shard, collective_id):
    vmem = pl.BlockSpec(memory_space=pltpu.VMEM)
    return pl.pallas_call(
        block_gather_kernel,
        out_shape=pltpu.VMEM((2, RING, RING, RING) + shard.shape, F32),
        in_specs=[vmem],
        out_specs=vmem,
        scratch_shapes=send_sems(len(LAST_COLORS) * BLOCK_SENDS),
        compiler_params=pltpu.CompilerParams(collective_id=collective_id, has_side_effects=True, vmem_limit_bytes=16 * MIB),
        cost_estimate=pl.CostEstimate(flops=60_000_000_000, bytes_accessed=32 * MIB, transcendentals=0),
        name='block_gather',
    )(in_vmem(shard))


def place_kernel(along, _, blocks, *refs):
    out_in, out_out = refs[-2:]
    i, k = pl.program_id(0), pl.program_id(1)
    n, cols = blocks.shape[-2] // 2, blocks.shape[-1]
    for a in range(RING):
        for b in range(RING):
            at = [a, b]
            at.insert(along, i)
            block = blocks[(k,) + tuple(at)]
            out_in[a * cols : (a + 1) * cols, b * n : (b + 1) * n] = block[:n].T
            out_out[a * n : (a + 1) * n, b * cols : (b + 1) * cols] = block[n:]


def place_blocks(core, blocks, outs, layer, layers):
    cols = blocks.shape[-1]
    n = cols // 2
    width, d = n * RING, cols * RING
    return pl.pallas_call(
        functools.partial(place_kernel, AXES.index(GROUPS[layer])),
        grid_spec=pltpu.PrefetchScalarGridSpec(
            num_scalar_prefetch=1,
            grid=(RING, 2),
            in_specs=[pl.BlockSpec(memory_space=pltpu.VMEM)] + [pl.BlockSpec(memory_space=pl.ANY)] * len(outs),
            out_specs=[
                pl.BlockSpec((None, d, width), lambda i, k, s: (layer, 0, i * 2 + (s[0] + k) % 2)),
                pl.BlockSpec((None, width, d), lambda i, k, s: (layer, i * 2 + (s[0] + k) % 2, 0)),
            ],
        ),
        out_shape=[jax.ShapeDtypeStruct((layers, d, width * 2 * RING), F32), jax.ShapeDtypeStruct((layers, width * 2 * RING, d), F32)],
        input_output_aliases={2 + k: k for k in range(len(outs))},
        compiler_params=pltpu.CompilerParams(vmem_limit_bytes=24 * MIB),
        cost_estimate=pl.CostEstimate(flops=10_000_000_000, bytes_accessed=32 * MIB, transcendentals=0),
        name='place_blocks',
    )(core, in_vmem(blocks), *outs)


def solution(mesh):
    mesh4 = Mesh(mesh.devices.reshape(RING, RING, RING, 2), AXES)

    def local_step(tok, tgt, w_in, w_out):
        layers = w_in.shape[0]
        core = lax.axis_index('c').astype(jnp.int32).reshape(1)
        above, *rows = first(tok, tgt, w_in, w_out, tok.shape[0] * mesh4.size, 2 * layers)
        hg, gg = rows[: layers - 1], rows[layers - 1 :]
        outs = []
        for l in reversed(range(layers - 1)):
            if outs:
                above, *outs = lax.optimization_barrier((above, *outs))
            shard, blocks = layer_grads(l, hg[l], gg[l], w_in, w_out, above)
            outs = place_blocks(core, blocks, outs, l + 1, layers)
            above = shard
        above, *outs = lax.optimization_barrier((above, *outs))
        outs = place_blocks(core, block_gather(above, layers + 1), outs, 0, layers)
        return outs[0], outs[1]

    spec = P(AXES, None)
    return jax.shard_map(local_step, mesh=mesh4, in_specs=(spec, spec, P(), P()), out_specs=(P(), P()), check_vma=False)
```

```python
import functools
import math

import jax
import jax.numpy as jnp
from jax import lax
from jax.experimental import pallas as pl
from jax.experimental.pallas import tpu as pltpu
from jax.sharding import Mesh
from jax.sharding import PartitionSpec as P

AXES = ('z', 'y', 'x', 'c')
RING = 4
GROUPS = ('x', 'z', 'y', 'x')
OTHERS = {'x': ('z', 'y'), 'y': ('z', 'x'), 'z': ('y', 'x')}
CHUNK = 1024
PART = 256
SLOTS = 3
ORDERS = (('x', 'y', 'z'), ('y', 'z', 'x'), ('z', 'x', 'y'))
SHARES = {3: (10, 8, 14), 2: (14, 10, 8), 1: (8, 14, 10), 0: (10, 11, 11)}
F32, BF16 = jnp.float32, jnp.bfloat16
COL = (((1,), (1,)), ((), ()))
GELU_S = 0.7978845608028654
GELU_C = 0.044715
MESH_ID = pl.DeviceIdType.MESH
MIB = 1 << 20
HOP_US, CHIP_US = 2.0, 1.1
LINK_RATE, CHIP_RATE = 45.7e3, 600e3
ROW_SENDS, SUM_SENDS, BLOCK_SENDS = 10, 24, 123


def place(axis, step):
    coords = [lax.axis_index(name) for name in AXES]
    which = AXES.index(axis)
    size = 2 if axis == 'c' else RING
    coords[which] = lax.rem(coords[which] + (step + size), size)
    return tuple(coords)


def greet():
    barrier = pltpu.get_barrier_semaphore()
    neighbours = [(axis, step) for axis in 'xyz' for step in (1, -1)] + [('c', 1)]
    for axis, step in neighbours:
        pl.semaphore_signal(barrier, inc=1, device_id=place(axis, step), device_id_type=MESH_ID)
    return lambda: pl.semaphore_wait(barrier, len(neighbours))


def around(axis):
    me = lax.axis_index(axis)
    return {'m': me, 'p': lax.rem(me + 3, RING), 'n': lax.rem(me + 1, RING), 'o': lax.rem(me + 2, RING)}


class Plan:
    def __init__(self, sems, backlog):
        self.sems, self.backlog, self.items, self.copies = sems, backlog, {}, {}

    def send(self, name, axis, step, src, dst, needs, priority):
        index = len(self.copies)
        self.copies[name] = pltpu.make_async_remote_copy(
            src_ref=src, dst_ref=dst, send_sem=self.sems[0].at[index], recv_sem=self.sems[1].at[index], device_id=place(axis, step), device_id_type=MESH_ID
        )
        size = math.prod(src.shape) * jnp.dtype(src.dtype).itemsize
        self.items[name] = ((axis, step), size, tuple(needs), priority)

    def work(self, name, cost, run, needs, priority):
        self.items[name] = (run, cost, tuple(needs), priority)

    def order(self, now):
        free, done, todo, order = {}, {}, dict(self.items), []
        while todo:
            due, soonest = None, math.inf
            for name, (what, size, needs, priority) in todo.items():
                if any(need not in done for need in needs):
                    continue
                when = max([done[need] for need in needs], default=0.0)
                if name in self.copies:
                    when = max(when, free.get(what, 0.0) - self.backlog)
                if when <= now + 1e-9:
                    key = (name not in self.copies, priority)
                    due = min(due, (key, len(order), name), key=lambda d: d[0]) if due else (key, len(order), name)
                soonest = min(soonest, when)
            if due is None:
                now = max(now, soonest)
                continue
            name = due[2]
            what, size, _, _ = todo.pop(name)
            order.append(name)
            if name in self.copies:
                inside = what[0] == 'c'
                free[what] = max(now, free.get(what, 0.0)) + size / (CHIP_RATE if inside else LINK_RATE)
                done[name] = free[what] + (CHIP_US if inside else HOP_US)
                now += 0.03
            else:
                now += size
                done[name] = now
        return order

    def run(self, start):
        landed = set()

        def arrive(name):
            if name in self.copies and name not in landed:
                landed.add(name)
                self.copies[name].wait_recv()

        for name in self.order(start):
            what, _, needs, _ = self.items[name]
            for need in needs:
                arrive(need)
            if name in self.copies:
                self.copies[name].start()
            else:
                what()
        for name, copy in self.copies.items():
            arrive(name)
            copy.wait_send()


def plan_rows(plan, key, own, out, axis, after, priority):
    half = out.shape[1] // 2
    top, bottom = pl.ds(0, half), pl.ds(half, half)

    def send(name, axis, step, src, dst, needs, late=0):
        plan.send((key,) + name, axis, step, src, out.at[dst], needs, priority + late)
        return (key,) + name

    right_top = send(('own', 'right', 'top'), axis, 1, own.at[top], (1, top), after)
    left_bottom = send(('own', 'left', 'bottom'), axis, -1, own.at[bottom], (2, bottom), after)
    right_bottom = send(('own', 'right', 'bottom'), axis, 1, own.at[bottom], (1, bottom), after, 2)
    left_top = send(('own', 'left', 'top'), axis, -1, own.at[top], (2, top), after, 2)
    ahead = send(('on', 'right'), axis, 1, out.at[1, top], (3, top), [right_top], 1)
    behind = send(('on', 'left'), axis, -1, out.at[2, bottom], (3, bottom), [left_bottom], 1)
    slots = [list(after), [right_top, right_bottom], [left_top, left_bottom], [ahead, behind]]
    return slots + [[send(('core', slot), 'c', 1, out.at[slot] if slot else own, (4 + slot,), slots[slot])] for slot in range(4)]


def plan_sums(plan, key, parts, filled, got, put, axis, after, costs, priority):
    at = around(axis)
    half = parts.shape[1] // 2
    top, bottom = pl.ds(0, half), pl.ds(half, half)
    send = lambda name, step, src, dst, needs, late: plan.send((key, name), axis, step, src, got.at[dst], list(after) + needs, priority + late)
    send('far right', 1, parts.at[at['o'], top], 0, filled['o'], 0)
    send('far left', -1, parts.at[at['o'], bottom], 3, filled['o'], 0)
    send('near right', 1, parts.at[at['n'], bottom], 1, filled['n'], 3)
    send('near left', -1, parts.at[at['p'], top], 4, filled['p'], 3)

    def add(slot, which, rows):
        got[slot] = got[slot] + parts[at[which], rows]

    plan.work((key, 'add right'), costs[0], lambda: add(0, 'n', top), [(key, 'far right')] + filled['n'], 1)
    plan.work((key, 'add left'), costs[0], lambda: add(3, 'p', bottom), [(key, 'far left')] + filled['p'], 1)
    send('on right', 1, got.at[0], 2, [(key, 'add right')], 1)
    send('on left', -1, got.at[3], 5, [(key, 'add left')], 1)

    def total(which, rows, one, two):
        put(which, parts[at['m'], rows] + got[one] + got[two])

    plan.work((key, 'sum 0'), costs[1], lambda: total(0, top, 4, 2), [(key, 'near left'), (key, 'on right')] + filled['m'], 2)
    plan.work((key, 'sum 1'), costs[1], lambda: total(1, bottom, 1, 5), [(key, 'near right'), (key, 'on left')] + filled['m'], 2)
    return [(key, 'sum 0'), (key, 'sum 1')]


def put_blocks(total, which, value):
    total[pl.ds(which * 2, 2)] = value.reshape((2,) + total.shape[1:])


def put_rows(total, offset, which, value):
    total[pl.ds(offset + which * value.shape[0], value.shape[0])] = value


def plan_blocks(plan, key, out, order, rows, after):
    near, far = out.at[0], out.at[1]
    at = {axis: around(axis) for axis in order}
    every = pl.ds(0, RING)
    onward = {'m': 1, 'o': 1, 'p': -1, 'n': -1}

    def where(picks, part=rows):
        chosen = dict(zip(order, picks))
        return tuple(every if chosen[axis] == 'all' else at[axis][chosen[axis]] for axis in ('z', 'y', 'x')) + (pl.ds(*part),)

    def send(name, axis, step, picks, needs, priority, part=rows, dst=near):
        spot = where(picks, part)
        plan.send((key,) + name, axis, step, near.at[spot], dst.at[spot], needs, priority)
        return [(key,) + name]

    cut = (rows[1] // 16) * 8
    halves = (rows[0], cut), (rows[0] + cut, rows[1] - cut)
    ready = {'m': list(after)}
    for side, step, half in (('p', 1, 0), ('n', -1, 1)):
        ready[side] = send((1, 'own', side), order[0], step, 'mmm', after, 10)
    ready['o'] = []
    for side, step, half in (('p', 1, 0), ('n', -1, 1)):
        ready['o'] = ready['o'] + send((1, 'on', side), order[0], step, (side, 'm', 'm'), ready[side], 9, halves[half])
    for phase in (2, 3):
        spread = {'m': sum([ready[i] for i in 'mpno'], []), 'p': [], 'n': [], 'o': []}
        arrived = {}
        for i in 'mpno':
            picks = {side: (i, side, 'm') if phase == 2 else ('all', i, side) for side in 'mpno'}
            for side, step in (('p', 1), ('n', -1)):
                first = onward[i] == step
                arrived[i, side] = send((phase, 'own', side, i), order[phase - 1], step, picks['m'], ready[i], (12 if first else 14) if phase == 2 else (30 if first else 50))
            side = 'p' if onward[i] == 1 else 'n'
            arrived[i, 'o'] = send((phase, 'on', side, i), order[phase - 1], onward[i], picks[side], arrived[i, side], 11 if phase == 2 else 40)
            for side in 'pno':
                spread[side] = spread[side] + arrived[i, side]
                if phase == 3:
                    send(('core', side, i), 'c', 1, picks[side], arrived[i, side], 60, dst=far)
        if phase == 2:
            ready = spread
            send(('core', 'm'), 'c', 1, ('all', 'all', 'm'), sum([ready[i] for i in 'mpno'], []), 60, dst=far)


def gelu_terms(x):
    square = x * x
    t = jnp.tanh(x * (GELU_S + GELU_S * GELU_C * square))
    cdf = 0.5 + 0.5 * t
    slope = cdf + (0.5 * x) * (1.0 - t * t) * (GELU_S + 3.0 * GELU_S * GELU_C * square)
    return x * cdf, slope


class Weights:
    def __init__(self, w_in, w_out, buf_in, buf_out, sems):
        self.w_in, self.w_out, self.buf_in, self.buf_out, self.sems = w_in, w_out, buf_in, buf_out, sems
        self.width = buf_in.shape[2]
        self.steps = w_in.shape[2] // self.width

    def copies(self, layer, chunk, slot):
        at = pl.ds(pl.multiple_of(chunk * self.width, self.width), self.width)
        return (
            pltpu.make_async_copy(self.w_in.at[layer, :, at], self.buf_in.at[slot], self.sems.at[0, slot]),
            pltpu.make_async_copy(self.w_out.at[layer, at, :], self.buf_out.at[slot], self.sems.at[1, slot]),
        )

    def start(self, layer, chunk, slot):
        for copy in self.copies(layer, chunk, slot):
            copy.start()

    def sweep(self, layer, base, following, body):
        def step(chunk):
            slot = lax.rem(base + chunk, SLOTS)
            for copy in self.copies(layer, chunk, slot):
                copy.wait()
            ahead = chunk + SLOTS - 1
            over = lax.div(ahead, self.steps)

            def load():
                self.start(layer + over * ((layer if following is None else following) - layer), ahead - over * self.steps, lax.rem(base + ahead, SLOTS))

            if following is None:
                pl.when(ahead < self.steps)(load)
            else:
                load()
            body(chunk, self.buf_in.at[slot], self.buf_out.at[slot])

        return lambda first, last: pl.loop(first, last)(step)


def forward_layer(weights, layer, base, following, hidden, pre, total, out):
    half = min(PART, weights.width // 2)
    parts = weights.width // half

    def body(chunk, wi, wo):
        posts = []
        for part in range(parts):
            at = pl.ds(part * half, half)
            u = jnp.dot(hidden[...], wi[:, at], preferred_element_type=F32).astype(BF16)
            if pre is not None:
                pre[:, pl.ds(pl.multiple_of(chunk * weights.width + part * half, half), half)] = u
            posts.append(gelu_terms(u.astype(F32))[0].astype(BF16))
        for part in range(parts):
            total[...] += jnp.dot(posts[part], wo[pl.ds(part * half, half)], preferred_element_type=F32)

    sweep = weights.sweep(layer, base, following, body)

    def run():
        total[...] = jnp.zeros_like(total)
        sweep(0, weights.steps)
        out((hidden[...].astype(F32) + total[...]).astype(BF16))

    return run


def backward_layer(weights, layer, base, following, grad, pre, total, out):
    half = min(PART, weights.width // 2)
    parts = weights.width // half

    def body(chunk, wi, wo):
        grads = []
        for part in range(parts):
            e = lax.dot_general(grad[...], wo[pl.ds(part * half, half)], COL, preferred_element_type=F32)
            u = pre[:, pl.ds(pl.multiple_of(chunk * weights.width + part * half, half), half)]
            grads.append((e * gelu_terms(u.astype(F32))[1]).astype(BF16))
        for part in range(parts):
            total[...] += lax.dot_general(grads[part], wi[:, pl.ds(part * half, half)], COL, preferred_element_type=F32)

    sweep = weights.sweep(layer, base, following, body)
    middle = weights.steps // 2

    def first_piece():
        total[...] = jnp.zeros_like(total)
        sweep(0, middle)

    def second_piece():
        sweep(middle, weights.steps)
        out[...] = (grad[...].astype(F32) + total[...]).astype(BF16)

    return first_piece, second_piece


class ShardWork:
    def __init__(self, layer, w_in, w_out, shard, take):
        self.group, self.shard = GROUPS[layer], shard
        self.wi, self.wo, self.wi_t, self.act, self.slope, w_sems = take(6)
        self.buffers = [take(4), take(4)]
        width = self.wi.shape[1]
        start = pl.multiple_of((lax.axis_index(self.group) * 2 + lax.axis_index('c')) * width, width)
        self.loads = [
            pltpu.make_async_copy(w_in.at[layer, :, pl.ds(start, width)], self.wi, w_sems.at[0]),
            pltpu.make_async_copy(w_out.at[layer, pl.ds(start, width), :], self.wo, w_sems.at[1]),
        ]

    def load(self):
        for load in self.loads:
            load.start()

    def ready(self):
        self.loads[0].wait()
        self.wi_t[...] = self.wi[...].T
        self.loads[1].wait()

    def rows(self, hg, gg, slot):
        n = hg.shape[1]
        at = pl.ds(pl.multiple_of(slot * n, n), n)
        u = lax.dot_general(self.wi_t[...], hg[slot], COL, preferred_element_type=F32).astype(BF16)
        e = lax.dot_general(self.wo[...], gg[slot], COL, preferred_element_type=F32)
        post, slope = gelu_terms(u.astype(F32))
        self.act[:, at] = post.astype(BF16)
        self.slope[:, at] = (e * slope).astype(BF16)

    def fill(self, color, which, hg, gg):
        parts = self.buffers[color][0]
        cols = parts.shape[2]
        at = pl.ds(pl.multiple_of(which * cols, cols), cols)
        left, right = (self.slope, hg) if color == 0 else (self.act, gg)
        parts[which] = jnp.dot(left[...], right[:, :, at].reshape(-1, cols), preferred_element_type=F32)

    def plan(self, plan, hg, gg, ready, priority):
        for color in range(2):
            parts, got_one, mid, got_two = self.buffers[color]
            one, two = OTHERS[self.group][color], OTHERS[self.group][1 - color]
            at = around(one)
            filled = {}
            for rank, which in enumerate('onpm'):
                filled[which] = [('fill', color, which)]
                plan.work(filled[which][0], 0.7, functools.partial(self.fill, color, at[which], hg, gg), ready, (10, 21, 22, 40)[rank] + 0.5 * color)
            sums = plan_sums(plan, ('sum', 1, color), parts, filled, got_one, functools.partial(put_blocks, mid), one, [], (0.12, 0.15), priority)
            filled = dict.fromkeys('mpno', sums)
            put = functools.partial(put_rows, self.shard, color * mid.shape[1])
            plan_sums(plan, ('sum', 2, color), mid, filled, got_two, put, two, [], (0.05, 0.05), priority - 4)


def shard_scratch(tokens, d, width):
    cols, n = d // RING, width // RING
    scratch = [pltpu.VMEM((d, width), BF16), pltpu.VMEM((width, d), BF16), pltpu.VMEM((width, d), BF16)]
    scratch += [pltpu.VMEM((width, tokens), BF16)] * 2 + [pltpu.SemaphoreType.DMA((2,))]
    for _ in range(2):
        scratch += [pltpu.VMEM((RING, width, cols), F32), pltpu.VMEM((6, width // 2, cols), F32)]
        scratch += [pltpu.VMEM((RING, n, cols), F32), pltpu.VMEM((6, n // 2, cols), F32)]
    return scratch


def send_sems(count):
    return [pltpu.SemaphoreType.DMA((count,))] * 2


def stream_scratch(d, full):
    width = min(CHUNK, full // 4)
    return [pltpu.VMEM((SLOTS, d, width), BF16), pltpu.VMEM((SLOTS, width, d), BF16), pltpu.SemaphoreType.DMA((2, SLOTS))]


def first_kernel(scale, tok, tgt, w_in, w_out, *refs):
    refs = list(refs)
    take = lambda count: [refs.pop(0) for _ in range(count)]
    (shard,) = take(1)
    hg_out, gg_out = take(3), take(3)
    buf_in, buf_out, w_sems, pre, total, mine, keep_sems, h3, g4 = take(9)
    sems = take(2)
    meet = greet()
    layers = w_in.shape[0]
    top = layers - 1
    weights = Weights(w_in, w_out, buf_in, buf_out, w_sems)
    work = ShardWork(top, w_in, w_out, shard, take)
    for chunk in range(SLOTS - 1):
        weights.start(0, chunk, chunk)
    work.load()
    meet()
    plan = Plan(sems, 3.0)
    hiddens = [tok, mine.at[0], mine.at[1], h3.at[0]]
    grads = [g4.at[0], mine.at[2], mine.at[3], mine.at[4]]

    def to(ref):
        def out(value):
            ref[...] = value

        return out

    def last(value):
        g4[0] = ((value.astype(F32) - tgt[...].astype(F32)) * scale).astype(BF16)

    steps = weights.steps
    outs = [to(hiddens[1]), to(hiddens[2]), to(hiddens[3]), last]
    for l in range(layers):
        run = forward_layer(weights, l, l * steps, min(l + 1, top), hiddens[l], pre.at[l - 1] if l else None, total, outs[l])
        plan.work(('forward', l), 6.5, run, [('forward', l - 1)] if l else [], 1)
    plan.work('ready', 2.0, work.ready, [('forward', 1)], 3)
    done = ('forward', top)
    for i in range(layers - 1):
        l = top - i
        pieces = backward_layer(weights, l, (layers + i) * steps, l - 1 if l > 1 else None, grads[i], pre.at[l - 1], total, grads[i + 1])
        for k, piece in enumerate(pieces):
            plan.work(('backward', l, k), 3.5, piece, [done], 6 + i)
            done = ('backward', l, k)
    stores = []

    def keep(name, own, out, axis, after, priority):
        plan_rows(plan, name, own, out, axis, after, priority)
        stores.append(pltpu.make_async_copy(own, out.at[0], keep_sems.at[len(stores)]))
        plan.work((name, 'store'), 0.02, stores[-1].start, after, 50)

    for l in range(top):
        keep(('h', l), hiddens[l], hg_out[l], GROUPS[l], [('forward', l - 1)] if l else [], (22, 22, 10)[l])
    for l in range(top):
        keep(('g', l), grads[top - l], gg_out[l], GROUPS[l], [('backward', l + 1, 1)], (32, 31, 10)[l])
    h3_slots = plan_rows(plan, 'h3', hiddens[top], h3, GROUPS[top], [('forward', top - 1)], 0)
    g4_slots = plan_rows(plan, 'g4', grads[0], g4, GROUPS[top], [('forward', top)], 5)
    rows = []
    for slots in ((0,), (4,), (1, 2), (5, 6), (3,), (7,)):
        if len(slots) == 1:
            run = functools.partial(work.rows, h3, g4, slots[0])
        else:
            run = functools.partial(pl.loop(slots[0], slots[-1] + 1), functools.partial(work.rows, h3, g4))
        rows.append(('rows', slots))
        plan.work(rows[-1], 0.85 * len(slots), run, sum([h3_slots[slot] + g4_slots[slot] for slot in slots], ['ready']), 5)
    work.plan(plan, h3, g4, rows, -10)
    plan.run(5.0)
    for store in stores:
        store.wait()


def first(tok, tgt, w_in, w_out, total_rows, collective_id):
    vmem, anywhere = pl.BlockSpec(memory_space=pltpu.VMEM), pl.BlockSpec(memory_space=pl.ANY)
    n, d = tok.shape
    layers, _, full = w_in.shape
    group = (2 * RING, n, d)
    kept = 2 * (layers - 1)
    scratch = stream_scratch(d, full)
    scratch += [pltpu.VMEM((layers - 1, n, full), BF16), pltpu.VMEM((n, d), F32), pltpu.VMEM((5, n, d), BF16)]
    scratch += [pltpu.SemaphoreType.DMA((kept,))] + [pltpu.VMEM(group, BF16)] * 2 + send_sems((kept + 2) * ROW_SENDS + SUM_SENDS)
    scratch += shard_scratch(2 * RING * n, d, full // (2 * RING))
    return pl.pallas_call(
        functools.partial(first_kernel, 1.0 / total_rows),
        out_shape=[pltpu.VMEM((full // (4 * RING), d // RING), F32)] + [jax.ShapeDtypeStruct(group, BF16)] * kept,
        in_specs=[vmem, vmem, anywhere, anywhere],
        out_specs=[vmem] + [anywhere] * kept,
        scratch_shapes=scratch,
        compiler_params=pltpu.CompilerParams(collective_id=collective_id, has_side_effects=True, vmem_limit_bytes=60 * MIB),
        cost_estimate=pl.CostEstimate(flops=60_000_000_000, bytes_accessed=96 * MIB, transcendentals=0),
        name='first',
    )(tok, tgt, w_in, w_out)


def layer_kernel(layer, hg_in, gg_in, w_in, w_out, above, shard, blocks, hg, gg, row_sems, *refs):
    refs = list(refs)
    take = lambda count: [refs.pop(0) for _ in range(count)]
    sems = take(2)
    meet = greet()
    work = ShardWork(layer, w_in, w_out, shard, take)
    work.load()

    def row_copies(i):
        return [pltpu.make_async_copy(src.at[i], dst.at[i], row_sems.at[k, i]) for k, (src, dst) in enumerate(((hg_in, hg), (gg_in, gg)))]

    def load_rows():
        for i in range(2 * RING):
            for copy in row_copies(i):
                copy.start()

    hold_block(above, blocks)
    meet()
    plan = Plan(sems, 2.0)
    plan.work('load', 0.5, load_rows, [], 4)
    plan.work('ready', 2.0, work.ready, ['load'], 5)

    def quarter(first):
        @pl.loop(first, first + 2)
        def _(i):
            for copy in row_copies(i):
                copy.wait()
            work.rows(hg, gg, i)

    for i in range(RING):
        plan.work(('rows', i), 1.7, functools.partial(quarter, 2 * i), ['ready'], 6)
    plan_all_blocks(plan, blocks, SHARES[layer + 1])
    work.plan(plan, hg, gg, [('rows', i) for i in range(RING)], 45)
    plan.run(4.0)


def layer_grads(layer, hg, gg, w_in, w_out, above):
    vmem, anywhere = pl.BlockSpec(memory_space=pltpu.VMEM), pl.BlockSpec(memory_space=pl.ANY)
    _, m, d = hg.shape
    scratch = [pltpu.VMEM(hg.shape, BF16)] * 2 + [pltpu.SemaphoreType.DMA((2, 2 * RING))]
    scratch += send_sems(BLOCK_SENDS + SUM_SENDS)
    scratch += shard_scratch(2 * RING * m, d, w_in.shape[2] // (2 * RING))
    return pl.pallas_call(
        functools.partial(layer_kernel, layer),
        out_shape=[pltpu.VMEM(above.shape, F32), pltpu.VMEM((2, RING, RING, RING) + above.shape, F32)],
        in_specs=[anywhere] * 4 + [vmem],
        out_specs=[vmem, vmem],
        scratch_shapes=scratch,
        compiler_params=pltpu.CompilerParams(collective_id=layer, has_side_effects=True, vmem_limit_bytes=31_000_000),
        cost_estimate=pl.CostEstimate(flops=30_000_000_000, bytes_accessed=16 * MIB, transcendentals=0),
        name='layer_grads',
    )(hg, gg, w_in, w_out, in_vmem(above))


def in_vmem(value):
    return pltpu.with_memory_space_constraint(value, pltpu.VMEM)


def hold_block(shard, out):
    out[(0,) + tuple(lax.axis_index(axis) for axis in ('z', 'y', 'x'))] = shard[...]


def plan_all_blocks(plan, out, shares):
    unit = out.shape[-2] // sum(shares)
    for k, order in enumerate(ORDERS):
        plan_blocks(plan, ('blocks', k), out, order, (unit * sum(shares[:k]), unit * shares[k]), [])


def block_gather_kernel(shard, out, send, recv):
    meet = greet()
    hold_block(shard, out)
    meet()
    plan = Plan((send, recv), 2.0)
    plan_all_blocks(plan, out, SHARES[0])
    plan.run(3.0)


def block_gather(shard, collective_id):
    vmem = pl.BlockSpec(memory_space=pltpu.VMEM)
    return pl.pallas_call(
        block_gather_kernel,
        out_shape=pltpu.VMEM((2, RING, RING, RING) + shard.shape, F32),
        in_specs=[vmem],
        out_specs=vmem,
        scratch_shapes=send_sems(BLOCK_SENDS),
        compiler_params=pltpu.CompilerParams(collective_id=collective_id, has_side_effects=True, vmem_limit_bytes=16 * MIB),
        cost_estimate=pl.CostEstimate(flops=60_000_000_000, bytes_accessed=32 * MIB, transcendentals=0),
        name='block_gather',
    )(in_vmem(shard))


def place_kernel(along, _, blocks, *refs):
    out_in, out_out = refs[-2:]
    i, k = pl.program_id(0), pl.program_id(1)
    n, cols = blocks.shape[-2] // 2, blocks.shape[-1]
    for a in range(RING):
        for b in range(RING):
            at = [a, b]
            at.insert(along, i)
            block = blocks[(k,) + tuple(at)]
            out_in[a * cols : (a + 1) * cols, b * n : (b + 1) * n] = block[:n].T
            out_out[a * n : (a + 1) * n, b * cols : (b + 1) * cols] = block[n:]


def place_blocks(core, blocks, outs, layer, layers):
    cols = blocks.shape[-1]
    n = cols // 2
    width, d = n * RING, cols * RING
    return pl.pallas_call(
        functools.partial(place_kernel, AXES.index(GROUPS[layer])),
        grid_spec=pltpu.PrefetchScalarGridSpec(
            num_scalar_prefetch=1,
            grid=(RING, 2),
            in_specs=[pl.BlockSpec(memory_space=pltpu.VMEM)] + [pl.BlockSpec(memory_space=pl.ANY)] * len(outs),
            out_specs=[
                pl.BlockSpec((None, d, width), lambda i, k, s: (layer, 0, i * 2 + (s[0] + k) % 2)),
                pl.BlockSpec((None, width, d), lambda i, k, s: (layer, i * 2 + (s[0] + k) % 2, 0)),
            ],
        ),
        out_shape=[jax.ShapeDtypeStruct((layers, d, width * 2 * RING), F32), jax.ShapeDtypeStruct((layers, width * 2 * RING, d), F32)],
        input_output_aliases={2 + k: k for k in range(len(outs))},
        compiler_params=pltpu.CompilerParams(vmem_limit_bytes=24 * MIB),
        cost_estimate=pl.CostEstimate(flops=10_000_000_000, bytes_accessed=32 * MIB, transcendentals=0),
        name='place_blocks',
    )(core, in_vmem(blocks), *outs)


def solution(mesh):
    mesh4 = Mesh(mesh.devices.reshape(RING, RING, RING, 2), AXES)

    def local_step(tok, tgt, w_in, w_out):
        layers = w_in.shape[0]
        core = lax.axis_index('c').astype(jnp.int32).reshape(1)
        above, *rows = first(tok, tgt, w_in, w_out, tok.shape[0] * mesh4.size, 2 * layers)
        hg, gg = rows[: layers - 1], rows[layers - 1 :]
        outs = []
        for l in reversed(range(layers - 1)):
            if outs:
                above, *outs = lax.optimization_barrier((above, *outs))
            shard, blocks = layer_grads(l, hg[l], gg[l], w_in, w_out, above)
            outs = place_blocks(core, blocks, outs, l + 1, layers)
            above = shard
        above, *outs = lax.optimization_barrier((above, *outs))
        outs = place_blocks(core, block_gather(above, layers + 1), outs, 0, layers)
        return outs[0], outs[1]

    spec = P(AXES, None)
    return jax.shard_map(local_step, mesh=mesh4, in_specs=(spec, spec, P(), P()), out_specs=(P(), P()), check_vma=False)
```

```python
import functools
import math

import jax
import jax.numpy as jnp
from jax import lax
from jax.experimental import pallas as pl
from jax.experimental.pallas import tpu as pltpu
from jax.sharding import Mesh
from jax.sharding import PartitionSpec as P

AXES = ('z', 'y', 'x', 'c')
RING = 4
GROUPS = ('x', 'z', 'y', 'x')
OTHERS = {'x': ('z', 'y'), 'y': ('z', 'x'), 'z': ('y', 'x')}
CHUNK = 1024
PART = 256
SLOTS = 3
ORDERS = (('x', 'y', 'z'), ('y', 'z', 'x'), ('z', 'x', 'y'))
SHARES = {3: (10, 8, 14), 2: (14, 10, 8), 1: (8, 14, 10), 0: (10, 11, 11)}
F32, BF16 = jnp.float32, jnp.bfloat16
COL = (((1,), (1,)), ((), ()))
GELU_S = 0.7978845608028654
GELU_C = 0.044715
MESH_ID = pl.DeviceIdType.MESH
MIB = 1 << 20
HOP_US, CHIP_US = 2.0, 1.1
LINK_RATE, CHIP_RATE = 45.7e3, 600e3
ROW_SENDS, SUM_SENDS, BLOCK_SENDS = 10, 24, 123


def place(axis, step):
    coords = [lax.axis_index(name) for name in AXES]
    which = AXES.index(axis)
    size = 2 if axis == 'c' else RING
    coords[which] = lax.rem(coords[which] + (step + size), size)
    return tuple(coords)


def greet():
    barrier = pltpu.get_barrier_semaphore()
    neighbours = [(axis, step) for axis in 'xyz' for step in (1, -1)] + [('c', 1)]
    for axis, step in neighbours:
        pl.semaphore_signal(barrier, inc=1, device_id=place(axis, step), device_id_type=MESH_ID)
    return lambda: pl.semaphore_wait(barrier, len(neighbours))


def around(axis):
    me = lax.axis_index(axis)
    return {'m': me, 'p': lax.rem(me + 3, RING), 'n': lax.rem(me + 1, RING), 'o': lax.rem(me + 2, RING)}


class Plan:
    def __init__(self, sems, backlog):
        self.sems, self.backlog, self.items, self.copies = sems, backlog, {}, {}

    def send(self, name, axis, step, src, dst, needs, priority):
        index = len(self.copies)
        self.copies[name] = pltpu.make_async_remote_copy(
            src_ref=src, dst_ref=dst, send_sem=self.sems[0].at[index], recv_sem=self.sems[1].at[index], device_id=place(axis, step), device_id_type=MESH_ID
        )
        size = math.prod(src.shape) * jnp.dtype(src.dtype).itemsize
        self.items[name] = ((axis, step), size, tuple(needs), priority)

    def work(self, name, cost, run, needs, priority):
        self.items[name] = (run, cost, tuple(needs), priority)

    def order(self, now):
        free, done, todo, order = {}, {}, dict(self.items), []
        while todo:
            due, soonest = None, math.inf
            for name, (what, size, needs, priority) in todo.items():
                if any(need not in done for need in needs):
                    continue
                when = max([done[need] for need in needs], default=0.0)
                if name in self.copies:
                    when = max(when, free.get(what, 0.0) - self.backlog)
                if when <= now + 1e-9:
                    key = (name not in self.copies, priority)
                    due = min(due, (key, len(order), name), key=lambda d: d[0]) if due else (key, len(order), name)
                soonest = min(soonest, when)
            if due is None:
                now = max(now, soonest)
                continue
            name = due[2]
            what, size, _, _ = todo.pop(name)
            order.append(name)
            if name in self.copies:
                inside = what[0] == 'c'
                free[what] = max(now, free.get(what, 0.0)) + size / (CHIP_RATE if inside else LINK_RATE)
                done[name] = free[what] + (CHIP_US if inside else HOP_US)
                now += 0.03
            else:
                now += size
                done[name] = now
        return order

    def run(self, start):
        landed = set()

        def arrive(name):
            if name in self.copies and name not in landed:
                landed.add(name)
                self.copies[name].wait_recv()

        for name in self.order(start):
            what, _, needs, _ = self.items[name]
            for need in needs:
                arrive(need)
            if name in self.copies:
                self.copies[name].start()
            else:
                what()
        for name, copy in self.copies.items():
            arrive(name)
            copy.wait_send()


def plan_rows(plan, key, own, out, axis, after, priority):
    half = out.shape[1] // 2
    top, bottom = pl.ds(0, half), pl.ds(half, half)

    def send(name, axis, step, src, dst, needs, late=0):
        plan.send((key,) + name, axis, step, src, out.at[dst], needs, priority + late)
        return (key,) + name

    right_top = send(('own', 'right', 'top'), axis, 1, own.at[top], (1, top), after)
    left_bottom = send(('own', 'left', 'bottom'), axis, -1, own.at[bottom], (2, bottom), after)
    right_bottom = send(('own', 'right', 'bottom'), axis, 1, own.at[bottom], (1, bottom), after, 2)
    left_top = send(('own', 'left', 'top'), axis, -1, own.at[top], (2, top), after, 2)
    ahead = send(('on', 'right'), axis, 1, out.at[1, top], (3, top), [right_top], 1)
    behind = send(('on', 'left'), axis, -1, out.at[2, bottom], (3, bottom), [left_bottom], 1)
    slots = [list(after), [right_top, right_bottom], [left_top, left_bottom], [ahead, behind]]
    return slots + [[send(('core', slot), 'c', 1, out.at[slot] if slot else own, (4 + slot,), slots[slot])] for slot in range(4)]


def plan_sums(plan, key, parts, filled, got, put, axis, after, costs, priority):
    at = around(axis)
    half = parts.shape[1] // 2
    top, bottom = pl.ds(0, half), pl.ds(half, half)
    send = lambda name, step, src, dst, needs, late: plan.send((key, name), axis, step, src, got.at[dst], list(after) + needs, priority + late)
    send('far right', 1, parts.at[at['o'], top], 0, filled['o'], 0)
    send('far left', -1, parts.at[at['o'], bottom], 3, filled['o'], 0)
    send('near right', 1, parts.at[at['n'], bottom], 1, filled['n'], 3)
    send('near left', -1, parts.at[at['p'], top], 4, filled['p'], 3)

    def add(slot, which, rows):
        got[slot] = got[slot] + parts[at[which], rows]

    plan.work((key, 'add right'), costs[0], lambda: add(0, 'n', top), [(key, 'far right')] + filled['n'], 1)
    plan.work((key, 'add left'), costs[0], lambda: add(3, 'p', bottom), [(key, 'far left')] + filled['p'], 1)
    send('on right', 1, got.at[0], 2, [(key, 'add right')], 1)
    send('on left', -1, got.at[3], 5, [(key, 'add left')], 1)

    def total(which, rows, one, two):
        put(which, parts[at['m'], rows] + got[one] + got[two])

    plan.work((key, 'sum 0'), costs[1], lambda: total(0, top, 4, 2), [(key, 'near left'), (key, 'on right')] + filled['m'], 2)
    plan.work((key, 'sum 1'), costs[1], lambda: total(1, bottom, 1, 5), [(key, 'near right'), (key, 'on left')] + filled['m'], 2)
    return [(key, 'sum 0'), (key, 'sum 1')]


def put_blocks(total, which, value):
    total[pl.ds(which * 2, 2)] = value.reshape((2,) + total.shape[1:])


def put_rows(total, offset, which, value):
    total[pl.ds(offset + which * value.shape[0], value.shape[0])] = value


def plan_blocks(plan, key, out, order, rows, after):
    near, far = out.at[0], out.at[1]
    at = {axis: around(axis) for axis in order}
    every = pl.ds(0, RING)
    onward = {'m': 1, 'o': 1, 'p': -1, 'n': -1}

    def where(picks, part=rows):
        chosen = dict(zip(order, picks))
        return tuple(every if chosen[axis] == 'all' else at[axis][chosen[axis]] for axis in ('z', 'y', 'x')) + (pl.ds(*part),)

    def send(name, axis, step, picks, needs, priority, part=rows, dst=near):
        spot = where(picks, part)
        plan.send((key,) + name, axis, step, near.at[spot], dst.at[spot], needs, priority)
        return [(key,) + name]

    cut = (rows[1] // 16) * 8
    halves = (rows[0], cut), (rows[0] + cut, rows[1] - cut)
    ready = {'m': list(after)}
    for side, step, half in (('p', 1, 0), ('n', -1, 1)):
        ready[side] = send((1, 'own', side), order[0], step, 'mmm', after, 10)
    ready['o'] = []
    for side, step, half in (('p', 1, 0), ('n', -1, 1)):
        ready['o'] = ready['o'] + send((1, 'on', side), order[0], step, (side, 'm', 'm'), ready[side], 9, halves[half])
    for phase in (2, 3):
        spread = {'m': sum([ready[i] for i in 'mpno'], []), 'p': [], 'n': [], 'o': []}
        arrived = {}
        for i in 'mpno':
            picks = {side: (i, side, 'm') if phase == 2 else ('all', i, side) for side in 'mpno'}
            for side, step in (('p', 1), ('n', -1)):
                first = onward[i] == step
                arrived[i, side] = send((phase, 'own', side, i), order[phase - 1], step, picks['m'], ready[i], (12 if first else 14) if phase == 2 else (30 if first else 50))
            side = 'p' if onward[i] == 1 else 'n'
            arrived[i, 'o'] = send((phase, 'on', side, i), order[phase - 1], onward[i], picks[side], arrived[i, side], 11 if phase == 2 else 40)
            for side in 'pno':
                spread[side] = spread[side] + arrived[i, side]
                if phase == 3:
                    send(('core', side, i), 'c', 1, picks[side], arrived[i, side], 60, dst=far)
        if phase == 2:
            ready = spread
            send(('core', 'm'), 'c', 1, ('all', 'all', 'm'), sum([ready[i] for i in 'mpno'], []), 60, dst=far)


def gelu_terms(x):
    square = x * x
    t = jnp.tanh(x * (GELU_S + GELU_S * GELU_C * square))
    cdf = 0.5 + 0.5 * t
    slope = cdf + (0.5 * x) * (1.0 - t * t) * (GELU_S + 3.0 * GELU_S * GELU_C * square)
    return x * cdf, slope


class Weights:
    def __init__(self, w_in, w_out, buf_in, buf_out, sems):
        self.w_in, self.w_out, self.buf_in, self.buf_out, self.sems = w_in, w_out, buf_in, buf_out, sems
        self.width = buf_in.shape[2]
        self.steps = w_in.shape[2] // self.width

    def copies(self, layer, chunk, slot):
        at = pl.ds(pl.multiple_of(chunk * self.width, self.width), self.width)
        return (
            pltpu.make_async_copy(self.w_in.at[layer, :, at], self.buf_in.at[slot], self.sems.at[0, slot]),
            pltpu.make_async_copy(self.w_out.at[layer, at, :], self.buf_out.at[slot], self.sems.at[1, slot]),
        )

    def start(self, layer, chunk, slot):
        for copy in self.copies(layer, chunk, slot):
            copy.start()

    def sweep(self, layer, base, following, body):
        def step(chunk):
            slot = lax.rem(base + chunk, SLOTS)
            for copy in self.copies(layer, chunk, slot):
                copy.wait()
            ahead = chunk + SLOTS - 1
            over = lax.div(ahead, self.steps)

            def load():
                self.start(layer + over * ((layer if following is None else following) - layer), ahead - over * self.steps, lax.rem(base + ahead, SLOTS))

            if following is None:
                pl.when(ahead < self.steps)(load)
            else:
                load()
            body(chunk, self.buf_in.at[slot], self.buf_out.at[slot])

        return lambda first, last: pl.loop(first, last)(step)


def forward_layer(weights, layer, base, following, hidden, pre, total, out):
    half = min(PART, weights.width // 2)
    parts = weights.width // half

    def body(chunk, wi, wo):
        posts = []
        for part in range(parts):
            at = pl.ds(part * half, half)
            u = jnp.dot(hidden[...], wi[:, at], preferred_element_type=F32).astype(BF16)
            if pre is not None:
                pre[:, pl.ds(pl.multiple_of(chunk * weights.width + part * half, half), half)] = u
            posts.append(gelu_terms(u.astype(F32))[0].astype(BF16))
        for part in range(parts):
            total[...] += jnp.dot(posts[part], wo[pl.ds(part * half, half)], preferred_element_type=F32)

    sweep = weights.sweep(layer, base, following, body)

    def run():
        total[...] = jnp.zeros_like(total)
        sweep(0, weights.steps)
        out((hidden[...].astype(F32) + total[...]).astype(BF16))

    return run


def backward_layer(weights, layer, base, following, grad, pre, total, out):
    half = min(PART, weights.width // 2)
    parts = weights.width // half

    def body(chunk, wi, wo):
        grads = []
        for part in range(parts):
            e = lax.dot_general(grad[...], wo[pl.ds(part * half, half)], COL, preferred_element_type=F32)
            u = pre[:, pl.ds(pl.multiple_of(chunk * weights.width + part * half, half), half)]
            grads.append((e * gelu_terms(u.astype(F32))[1]).astype(BF16))
        for part in range(parts):
            total[...] += lax.dot_general(grads[part], wi[:, pl.ds(part * half, half)], COL, preferred_element_type=F32)

    sweep = weights.sweep(layer, base, following, body)
    middle = weights.steps // 2

    def first_piece():
        total[...] = jnp.zeros_like(total)
        sweep(0, middle)

    def second_piece():
        sweep(middle, weights.steps)
        out[...] = (grad[...].astype(F32) + total[...]).astype(BF16)

    return first_piece, second_piece


class ShardWork:
    def __init__(self, layer, w_in, w_out, shard, take):
        self.group, self.shard = GROUPS[layer], shard
        self.wi, self.wo, self.wi_t, self.act, self.slope, w_sems = take(6)
        self.buffers = [take(4), take(4)]
        width = self.wi.shape[1]
        start = pl.multiple_of((lax.axis_index(self.group) * 2 + lax.axis_index('c')) * width, width)
        self.loads = [
            pltpu.make_async_copy(w_in.at[layer, :, pl.ds(start, width)], self.wi, w_sems.at[0]),
            pltpu.make_async_copy(w_out.at[layer, pl.ds(start, width), :], self.wo, w_sems.at[1]),
        ]

    def load(self):
        for load in self.loads:
            load.start()

    def ready(self):
        self.loads[0].wait()
        self.wi_t[...] = self.wi[...].T
        self.loads[1].wait()

    def rows(self, hg, gg, slot):
        n = hg.shape[1]
        at = pl.ds(pl.multiple_of(slot * n, n), n)
        u = lax.dot_general(self.wi_t[...], hg[slot], COL, preferred_element_type=F32).astype(BF16)
        e = lax.dot_general(self.wo[...], gg[slot], COL, preferred_element_type=F32)
        post, slope = gelu_terms(u.astype(F32))
        self.act[:, at] = post.astype(BF16)
        self.slope[:, at] = (e * slope).astype(BF16)

    def fill(self, color, which, hg, gg):
        parts = self.buffers[color][0]
        cols = parts.shape[2]
        at = pl.ds(pl.multiple_of(which * cols, cols), cols)
        left, right = (self.slope, hg) if color == 0 else (self.act, gg)
        parts[which] = jnp.dot(left[...], right[:, :, at].reshape(-1, cols), preferred_element_type=F32)

    def plan(self, plan, hg, gg, ready, priority):
        for color in range(2):
            parts, got_one, mid, got_two = self.buffers[color]
            one, two = OTHERS[self.group][color], OTHERS[self.group][1 - color]
            at = around(one)
            filled = {}
            for rank, which in enumerate('onpm'):
                filled[which] = [('fill', color, which)]
                plan.work(filled[which][0], 0.7, functools.partial(self.fill, color, at[which], hg, gg), ready, (10, 21, 22, 40)[rank] + 0.5 * color)
            sums = plan_sums(plan, ('sum', 1, color), parts, filled, got_one, functools.partial(put_blocks, mid), one, [], (0.12, 0.15), priority)
            filled = dict.fromkeys('mpno', sums)
            put = functools.partial(put_rows, self.shard, color * mid.shape[1])
            plan_sums(plan, ('sum', 2, color), mid, filled, got_two, put, two, [], (0.05, 0.05), priority - 4)


def shard_scratch(tokens, d, width):
    cols, n = d // RING, width // RING
    scratch = [pltpu.VMEM((d, width), BF16), pltpu.VMEM((width, d), BF16), pltpu.VMEM((width, d), BF16)]
    scratch += [pltpu.VMEM((width, tokens), BF16)] * 2 + [pltpu.SemaphoreType.DMA((2,))]
    for _ in range(2):
        scratch += [pltpu.VMEM((RING, width, cols), F32), pltpu.VMEM((6, width // 2, cols), F32)]
        scratch += [pltpu.VMEM((RING, n, cols), F32), pltpu.VMEM((6, n // 2, cols), F32)]
    return scratch


def send_sems(count):
    return [pltpu.SemaphoreType.DMA((count,))] * 2


def stream_scratch(d, full):
    width = min(CHUNK, full // 4)
    return [pltpu.VMEM((SLOTS, d, width), BF16), pltpu.VMEM((SLOTS, width, d), BF16), pltpu.SemaphoreType.DMA((2, SLOTS))]


def first_kernel(scale, tok_in, tgt_in, w_in, w_out, *refs):
    refs = list(refs)
    take = lambda count: [refs.pop(0) for _ in range(count)]
    (shard,) = take(1)
    hg_out, gg_out = take(3), take(3)
    buf_in, buf_out, w_sems, pre, total, mine, keep_sems, in_sems, h3, g4 = take(10)
    sems = take(2)
    meet = greet()
    layers = w_in.shape[0]
    top = layers - 1
    weights = Weights(w_in, w_out, buf_in, buf_out, w_sems)
    work = ShardWork(top, w_in, w_out, shard, take)
    for chunk in range(SLOTS - 1):
        weights.start(0, chunk, chunk)
    tok, tgt = mine.at[5], mine.at[6]
    inputs = [pltpu.make_async_copy(src, dst, in_sems.at[i]) for i, (src, dst) in enumerate(((tok_in, tok), (tgt_in, tgt)))]
    for copy in inputs:
        copy.start()
    work.load()
    inputs[0].wait()
    meet()
    plan = Plan(sems, 3.0)
    hiddens = [tok, mine.at[0], mine.at[1], h3.at[0]]
    grads = [g4.at[0], mine.at[2], mine.at[3], mine.at[4]]

    def to(ref):
        def out(value):
            ref[...] = value

        return out

    def last(value):
        inputs[1].wait()
        g4[0] = ((value.astype(F32) - tgt[...].astype(F32)) * scale).astype(BF16)

    steps = weights.steps
    outs = [to(hiddens[1]), to(hiddens[2]), to(hiddens[3]), last]
    for l in range(layers):
        run = forward_layer(weights, l, l * steps, min(l + 1, top), hiddens[l], pre.at[l - 1] if l else None, total, outs[l])
        plan.work(('forward', l), 6.5, run, [('forward', l - 1)] if l else [], 1)
    plan.work('ready', 2.0, work.ready, [('forward', 1)], 3)
    done = ('forward', top)
    for i in range(layers - 1):
        l = top - i
        pieces = backward_layer(weights, l, (layers + i) * steps, l - 1 if l > 1 else None, grads[i], pre.at[l - 1], total, grads[i + 1])
        for k, piece in enumerate(pieces):
            plan.work(('backward', l, k), 3.5, piece, [done], 6 + i)
            done = ('backward', l, k)
    stores = []

    def keep(name, own, out, axis, after, priority):
        plan_rows(plan, name, own, out, axis, after, priority)
        stores.append(pltpu.make_async_copy(own, out.at[0], keep_sems.at[len(stores)]))
        plan.work((name, 'store'), 0.02, stores[-1].start, after, 50)

    for l in range(top):
        keep(('h', l), hiddens[l], hg_out[l], GROUPS[l], [('forward', l - 1)] if l else [], (22, 22, 10)[l])
    for l in range(top):
        keep(('g', l), grads[top - l], gg_out[l], GROUPS[l], [('backward', l + 1, 1)], (32, 31, 10)[l])
    h3_slots = plan_rows(plan, 'h3', hiddens[top], h3, GROUPS[top], [('forward', top - 1)], 0)
    g4_slots = plan_rows(plan, 'g4', grads[0], g4, GROUPS[top], [('forward', top)], 5)
    rows = []
    for slots in ((0,), (4,), (1, 2), (5, 6), (3,), (7,)):
        if len(slots) == 1:
            run = functools.partial(work.rows, h3, g4, slots[0])
        else:
            run = functools.partial(pl.loop(slots[0], slots[-1] + 1), functools.partial(work.rows, h3, g4))
        rows.append(('rows', slots))
        plan.work(rows[-1], 0.85 * len(slots), run, sum([h3_slots[slot] + g4_slots[slot] for slot in slots], ['ready']), 5)
    work.plan(plan, h3, g4, rows, -10)
    plan.run(5.0)
    for store in stores:
        store.wait()


def first(tok, tgt, w_in, w_out, total_rows, collective_id):
    vmem, anywhere = pl.BlockSpec(memory_space=pltpu.VMEM), pl.BlockSpec(memory_space=pl.ANY)
    n, d = tok.shape
    layers, _, full = w_in.shape
    group = (2 * RING, n, d)
    kept = 2 * (layers - 1)
    scratch = stream_scratch(d, full)
    scratch += [pltpu.VMEM((layers - 1, n, full), BF16), pltpu.VMEM((n, d), F32), pltpu.VMEM((7, n, d), BF16)]
    scratch += [pltpu.SemaphoreType.DMA((kept,)), pltpu.SemaphoreType.DMA((2,))] + [pltpu.VMEM(group, BF16)] * 2 + send_sems((kept + 2) * ROW_SENDS + SUM_SENDS)
    scratch += shard_scratch(2 * RING * n, d, full // (2 * RING))
    return pl.pallas_call(
        functools.partial(first_kernel, 1.0 / total_rows),
        out_shape=[pltpu.VMEM((full // (4 * RING), d // RING), F32)] + [jax.ShapeDtypeStruct(group, BF16)] * kept,
        in_specs=[anywhere] * 4,
        out_specs=[vmem] + [anywhere] * kept,
        scratch_shapes=scratch,
        compiler_params=pltpu.CompilerParams(collective_id=collective_id, has_side_effects=True, vmem_limit_bytes=60 * MIB),
        cost_estimate=pl.CostEstimate(flops=60_000_000_000, bytes_accessed=96 * MIB, transcendentals=0),
        name='first',
    )(tok, tgt, w_in, w_out)


def layer_kernel(layer, hg_in, gg_in, w_in, w_out, above, shard, blocks, hg, gg, row_sems, *refs):
    refs = list(refs)
    take = lambda count: [refs.pop(0) for _ in range(count)]
    sems = take(2)
    meet = greet()
    work = ShardWork(layer, w_in, w_out, shard, take)
    work.load()

    def row_copies(i):
        return [pltpu.make_async_copy(src.at[i], dst.at[i], row_sems.at[k, i]) for k, (src, dst) in enumerate(((hg_in, hg), (gg_in, gg)))]

    def load_rows():
        for i in range(2 * RING):
            for copy in row_copies(i):
                copy.start()

    hold_block(above, blocks)
    meet()
    plan = Plan(sems, 2.0)
    plan.work('load', 0.5, load_rows, [], 4)
    plan.work('ready', 2.0, work.ready, ['load'], 5)

    def quarter(first):
        @pl.loop(first, first + 2)
        def _(i):
            for copy in row_copies(i):
                copy.wait()
            work.rows(hg, gg, i)

    for i in range(RING):
        plan.work(('rows', i), 1.7, functools.partial(quarter, 2 * i), ['ready'], 6)
    plan_all_blocks(plan, blocks, SHARES[layer + 1])
    work.plan(plan, hg, gg, [('rows', i) for i in range(RING)], 45)
    plan.run(4.0)


def layer_grads(layer, hg, gg, w_in, w_out, above):
    vmem, anywhere = pl.BlockSpec(memory_space=pltpu.VMEM), pl.BlockSpec(memory_space=pl.ANY)
    _, m, d = hg.shape
    scratch = [pltpu.VMEM(hg.shape, BF16)] * 2 + [pltpu.SemaphoreType.DMA((2, 2 * RING))]
    scratch += send_sems(BLOCK_SENDS + SUM_SENDS)
    scratch += shard_scratch(2 * RING * m, d, w_in.shape[2] // (2 * RING))
    return pl.pallas_call(
        functools.partial(layer_kernel, layer),
        out_shape=[pltpu.VMEM(above.shape, F32), pltpu.VMEM((2, RING, RING, RING) + above.shape, F32)],
        in_specs=[anywhere] * 4 + [vmem],
        out_specs=[vmem, vmem],
        scratch_shapes=scratch,
        compiler_params=pltpu.CompilerParams(collective_id=layer, has_side_effects=True, vmem_limit_bytes=31_000_000),
        cost_estimate=pl.CostEstimate(flops=30_000_000_000, bytes_accessed=16 * MIB, transcendentals=0),
        name='layer_grads',
    )(hg, gg, w_in, w_out, in_vmem(above))


def in_vmem(value):
    return pltpu.with_memory_space_constraint(value, pltpu.VMEM)


def hold_block(shard, out):
    out[(0,) + tuple(lax.axis_index(axis) for axis in ('z', 'y', 'x'))] = shard[...]


def plan_all_blocks(plan, out, shares):
    unit = out.shape[-2] // sum(shares)
    for k, order in enumerate(ORDERS):
        plan_blocks(plan, ('blocks', k), out, order, (unit * sum(shares[:k]), unit * shares[k]), [])


def block_gather_kernel(shard, out, send, recv):
    meet = greet()
    hold_block(shard, out)
    meet()
    plan = Plan((send, recv), 2.0)
    plan_all_blocks(plan, out, SHARES[0])
    plan.run(3.0)


def block_gather(shard, collective_id):
    vmem = pl.BlockSpec(memory_space=pltpu.VMEM)
    return pl.pallas_call(
        block_gather_kernel,
        out_shape=pltpu.VMEM((2, RING, RING, RING) + shard.shape, F32),
        in_specs=[vmem],
        out_specs=vmem,
        scratch_shapes=send_sems(BLOCK_SENDS),
        compiler_params=pltpu.CompilerParams(collective_id=collective_id, has_side_effects=True, vmem_limit_bytes=16 * MIB),
        cost_estimate=pl.CostEstimate(flops=60_000_000_000, bytes_accessed=32 * MIB, transcendentals=0),
        name='block_gather',
    )(in_vmem(shard))


def place_kernel(along, core, blocks, *refs):
    out_in, out_out = refs[-2:]
    i, part = pl.program_id(0), pl.program_id(1)
    n, cols = blocks.shape[-2] // 2, blocks.shape[-1]

    def block(which, a, b):
        at = [a, b]
        at.insert(along, i)
        return (lax.rem(core[0] + which, 2),) + tuple(at)

    for b in range(RING):
        for a in range(RING // 2):
            for c in range(2):
                columns = slice((c * RING + b) * n, (c * RING + b + 1) * n)
                out_in[a * cols : (a + 1) * cols, columns] = blocks[block(c, part * (RING // 2) + a, b)][:n].T
        for a in range(RING):
            out_out[a * n : (a + 1) * n, b * cols : (b + 1) * cols] = blocks[block(part, a, b)][n:]


def place_blocks(core, blocks, outs, layer, layers):
    cols = blocks.shape[-1]
    n = cols // 2
    width, d = n * RING, cols * RING
    return pl.pallas_call(
        functools.partial(place_kernel, AXES.index(GROUPS[layer])),
        grid_spec=pltpu.PrefetchScalarGridSpec(
            num_scalar_prefetch=1,
            grid=(RING, 2),
            in_specs=[pl.BlockSpec(memory_space=pltpu.VMEM)] + [pl.BlockSpec(memory_space=pl.ANY)] * len(outs),
            out_specs=[
                pl.BlockSpec((None, d // 2, 2 * width), lambda i, part, s: (layer, part, i)),
                pl.BlockSpec((None, width, d), lambda i, part, s: (layer, i * 2 + part, 0)),
            ],
        ),
        out_shape=[jax.ShapeDtypeStruct((layers, d, width * 2 * RING), F32), jax.ShapeDtypeStruct((layers, width * 2 * RING, d), F32)],
        input_output_aliases={2 + k: k for k in range(len(outs))},
        compiler_params=pltpu.CompilerParams(vmem_limit_bytes=24 * MIB),
        cost_estimate=pl.CostEstimate(flops=10_000_000_000, bytes_accessed=32 * MIB, transcendentals=0),
        name='place_blocks',
    )(core, in_vmem(blocks), *outs)


def solution(mesh):
    mesh4 = Mesh(mesh.devices.reshape(RING, RING, RING, 2), AXES)

    def local_step(tok, tgt, w_in, w_out):
        layers = w_in.shape[0]
        core = lax.axis_index('c').astype(jnp.int32).reshape(1)
        above, *rows = first(tok, tgt, w_in, w_out, tok.shape[0] * mesh4.size, 2 * layers)
        hg, gg = rows[: layers - 1], rows[layers - 1 :]
        outs = []
        for l in reversed(range(layers - 1)):
            if outs:
                above, *outs = lax.optimization_barrier((above, *outs))
            shard, blocks = layer_grads(l, hg[l], gg[l], w_in, w_out, above)
            outs = place_blocks(core, blocks, outs, l + 1, layers)
            above = shard
        above, *outs = lax.optimization_barrier((above, *outs))
        outs = place_blocks(core, block_gather(above, layers + 1), outs, 0, layers)
        return outs[0], outs[1]

    spec = P(AXES, None)
    return jax.shard_map(local_step, mesh=mesh4, in_specs=(spec, spec, P(), P()), out_specs=(P(), P()), check_vma=False)
```
